8 devices in a mesh: hp: 1 (over z), cp: 8 (over y, x, core).
Axes of the slice: x: 2, y: 2, z: 1, core: 2. Of those that a mesh axis runs over, the one named last changes fastest.
Arguments:
- q_heads: bfloat16 [2048, 16, 256], P('cp', 'hp')
- k_heads: bfloat16 [2048, 16, 256], P('cp', 'hp')
- v_heads: bfloat16 [2048, 16, 256], P('cp', 'hp')
- o_heads: bfloat16 [2048, 16, 256], P('cp', 'hp')
- do_heads: bfloat16 [2048, 16, 256], P('cp', 'hp')
- lse_rows: float32 [2048, 16], P('cp', 'hp')
- cu_seqlens: int32 [67], replicated
Outputs:
- output 1: bfloat16 [2048, 16, 256], P('cp', 'hp')
- output 2: bfloat16 [2048, 16, 256], P('cp', 'hp')
- output 3: bfloat16 [2048, 16, 256], P('cp', 'hp')
All inputs are finite; a program needn't handle non-finite values.
Results may differ from the reference program's by a relative error of at most 0.001.
Values are sent between devices in bfloat16 or wider.
A program may use at most 1 GiB of HBM per device.

```python
import jax
import jax.numpy as jnp
from jax import lax

CHUNK_LEN = 256
CP_SIZE = 8
HEADS_LOCAL = 16
HEAD_DIM = 256
REACH_CHUNKS = 3
QBLOCK = 256

SEQ_LEN = CHUNK_LEN * CP_SIZE
DOC_SLOTS = 8 * CP_SIZE + 2
WINDOW = REACH_CHUNKS * CHUNK_LEN
SOFTMAX_SCALE = HEAD_DIM ** -0.5
N_BLOCKS = SEQ_LEN // QBLOCK


def draw_cu_seqlens(doc_key):
    key_first, key_base, key_tier, key_long = jax.random.split(doc_key, 4)
    first_len = CHUNK_LEN // 4 + jax.random.randint(key_first, (1,), 0, CHUNK_LEN // 2)
    base_len = jax.random.randint(key_base, (DOC_SLOTS - 2,), CHUNK_LEN // 8, CHUNK_LEN + 1)
    long_len = WINDOW - jax.random.randint(key_long, (DOC_SLOTS - 2,), 0, CHUNK_LEN)
    tier_draw = jax.random.randint(key_tier, (DOC_SLOTS - 2,), 0, 4)
    rest_len = jnp.where(tier_draw == 3, long_len, base_len * jnp.where(tier_draw == 2, 2, 1))
    lengths = jnp.concatenate([first_len, jnp.full((1,), WINDOW, jnp.int32), rest_len]).astype(jnp.int32)
    doc_ends = jnp.minimum(jnp.cumsum(lengths), SEQ_LEN).astype(jnp.int32)
    return jnp.concatenate([jnp.zeros((1,), jnp.int32), doc_ends])


def doc_index(cu_seqlens):
    positions = jnp.arange(SEQ_LEN, dtype=jnp.int32)
    return (jnp.searchsorted(cu_seqlens, positions, side="right") - 1).astype(jnp.int32)


def window_mask(q_doc, q_pos, k_doc, k_pos):
    return (q_doc[:, None] == k_doc[None, :]) & (k_pos[None, :] <= q_pos[:, None])


def attention_forward(q_heads, k_heads, v_heads, doc_ids):
    front_pad = jnp.zeros((WINDOW, HEADS_LOCAL, HEAD_DIM), jnp.float32)
    k_pad = jnp.concatenate([front_pad, k_heads.astype(jnp.float32)])
    v_pad = jnp.concatenate([front_pad, v_heads.astype(jnp.float32)])
    doc_pad = jnp.concatenate([jnp.full((WINDOW,), -1, jnp.int32), doc_ids])
    q_full = q_heads.astype(jnp.float32)

    def forward_block(blk_idx):
        q_start = blk_idx * QBLOCK
        q_pos = q_start + jnp.arange(QBLOCK, dtype=jnp.int32)
        k_pos = q_start - WINDOW + jnp.arange(WINDOW + QBLOCK, dtype=jnp.int32)
        keep_mask = window_mask(lax.dynamic_slice_in_dim(doc_ids, q_start, QBLOCK), q_pos, lax.dynamic_slice_in_dim(doc_pad, q_start, WINDOW + QBLOCK), k_pos)
        q_blk = lax.dynamic_slice_in_dim(q_full, q_start, QBLOCK)
        k_win = lax.dynamic_slice_in_dim(k_pad, q_start, WINDOW + QBLOCK)
        v_win = lax.dynamic_slice_in_dim(v_pad, q_start, WINDOW + QBLOCK)
        scores = jnp.einsum("qhd,khd->hqk", q_blk, k_win) * SOFTMAX_SCALE
        scores = jnp.where(keep_mask[None], scores, -jnp.inf)
        row_max = jnp.max(scores, axis=-1, keepdims=True)
        weights = jnp.exp(scores - row_max)
        row_sum = jnp.sum(weights, axis=-1, keepdims=True)
        out_blk = jnp.einsum("hqk,khd->qhd", weights / row_sum, v_win)
        lse_blk = jnp.transpose((row_max + jnp.log(row_sum))[:, :, 0])
        return out_blk.astype(jnp.bfloat16), lse_blk

    out_blocks, lse_blocks = lax.map(forward_block, jnp.arange(N_BLOCKS))
    return out_blocks.reshape(SEQ_LEN, HEADS_LOCAL, HEAD_DIM), lse_blocks.reshape(SEQ_LEN, HEADS_LOCAL)


def setup_inputs(seed: int = 0, part: int = 0) -> dict:
    doc_key, data_key = jax.random.split(jax.random.key(seed))
    cu_seqlens = draw_cu_seqlens(doc_key)
    doc_ids = doc_index(cu_seqlens)
    key_q, key_k, key_v, key_do = jax.random.split(jax.random.fold_in(data_key, part), 4)
    head_shape = (SEQ_LEN, HEADS_LOCAL, HEAD_DIM)
    q_heads = jax.random.normal(key_q, head_shape, jnp.float32).astype(jnp.bfloat16)
    k_heads = jax.random.normal(key_k, head_shape, jnp.float32).astype(jnp.bfloat16)
    v_heads = jax.random.normal(key_v, head_shape, jnp.float32).astype(jnp.bfloat16)
    do_heads = (jax.random.normal(key_do, head_shape, jnp.float32) * (0.5 * CHUNK_LEN ** 0.5)).astype(jnp.bfloat16)
    o_heads, lse_rows = attention_forward(q_heads, k_heads, v_heads, doc_ids)
    return {"q_heads": q_heads, "k_heads": k_heads, "v_heads": v_heads, "o_heads": o_heads, "do_heads": do_heads, "lse_rows": lse_rows, "cu_seqlens": cu_seqlens}


def reference(q_heads, k_heads, v_heads, o_heads, do_heads, lse_rows, cu_seqlens):
    doc_ids = doc_index(cu_seqlens)
    q_full = q_heads.astype(jnp.float32)
    k_full = k_heads.astype(jnp.float32)
    v_full = v_heads.astype(jnp.float32)
    do_full = do_heads.astype(jnp.float32)
    delta_rows = jnp.sum(do_full * o_heads.astype(jnp.float32), axis=-1)
    zero_rows = jnp.zeros((WINDOW, HEADS_LOCAL, HEAD_DIM), jnp.float32)
    zero_stats = jnp.zeros((WINDOW, HEADS_LOCAL), jnp.float32)
    no_doc = jnp.full((WINDOW,), -1, jnp.int32)
    k_front = jnp.concatenate([zero_rows, k_full])
    v_front = jnp.concatenate([zero_rows, v_full])
    doc_front = jnp.concatenate([no_doc, doc_ids])
    q_back = jnp.concatenate([q_full, zero_rows])
    do_back = jnp.concatenate([do_full, zero_rows])
    lse_back = jnp.concatenate([lse_rows, zero_stats])
    delta_back = jnp.concatenate([delta_rows, zero_stats])
    doc_back = jnp.concatenate([doc_ids, no_doc])

    def dq_block(blk_idx):
        q_start = blk_idx * QBLOCK
        q_pos = q_start + jnp.arange(QBLOCK, dtype=jnp.int32)
        k_pos = q_start - WINDOW + jnp.arange(WINDOW + QBLOCK, dtype=jnp.int32)
        keep_mask = window_mask(lax.dynamic_slice_in_dim(doc_ids, q_start, QBLOCK), q_pos, lax.dynamic_slice_in_dim(doc_front, q_start, WINDOW + QBLOCK), k_pos)
        q_blk = lax.dynamic_slice_in_dim(q_full, q_start, QBLOCK)
        do_blk = lax.dynamic_slice_in_dim(do_full, q_start, QBLOCK)
        lse_blk = lax.dynamic_slice_in_dim(lse_rows, q_start, QBLOCK)
        delta_blk = lax.dynamic_slice_in_dim(delta_rows, q_start, QBLOCK)
        k_win = lax.dynamic_slice_in_dim(k_front, q_start, WINDOW + QBLOCK)
        v_win = lax.dynamic_slice_in_dim(v_front, q_start, WINDOW + QBLOCK)
        scores = jnp.einsum("qhd,khd->hqk", q_blk, k_win)
        p_matrix = jnp.exp(jnp.where(keep_mask[None], scores * SOFTMAX_SCALE - lse_blk.T[:, :, None], -jnp.inf))
        dprobs = jnp.einsum("qhd,khd->hqk", do_blk, v_win)
        dscores = (p_matrix * (dprobs - delta_blk.T[:, :, None])).astype(jnp.bfloat16).astype(jnp.float32)
        return jnp.einsum("hqk,khd->qhd", dscores, k_win) * SOFTMAX_SCALE

    def dkv_block(blk_idx):
        k_start = blk_idx * QBLOCK
        k_pos = k_start + jnp.arange(QBLOCK, dtype=jnp.int32)
        q_pos = k_start + jnp.arange(QBLOCK + WINDOW, dtype=jnp.int32)
        keep_mask = window_mask(lax.dynamic_slice_in_dim(doc_back, k_start, QBLOCK + WINDOW), q_pos, lax.dynamic_slice_in_dim(doc_ids, k_start, QBLOCK), k_pos)
        q_win = lax.dynamic_slice_in_dim(q_back, k_start, QBLOCK + WINDOW)
        do_win = lax.dynamic_slice_in_dim(do_back, k_start, QBLOCK + WINDOW)
        lse_win = lax.dynamic_slice_in_dim(lse_back, k_start, QBLOCK + WINDOW)
        delta_win = lax.dynamic_slice_in_dim(delta_back, k_start, QBLOCK + WINDOW)
        k_blk = lax.dynamic_slice_in_dim(k_full, k_start, QBLOCK)
        v_blk = lax.dynamic_slice_in_dim(v_full, k_start, QBLOCK)
        scores = jnp.einsum("qhd,khd->hqk", q_win, k_blk)
        p_matrix = jnp.exp(jnp.where(keep_mask[None], scores * SOFTMAX_SCALE - lse_win.T[:, :, None], -jnp.inf))
        dv_blk = jnp.einsum("hqk,qhd->khd", p_matrix.astype(jnp.bfloat16).astype(jnp.float32), do_win)
        dprobs = jnp.einsum("qhd,khd->hqk", do_win, v_blk)
        dscores = (p_matrix * (dprobs - delta_win.T[:, :, None])).astype(jnp.bfloat16).astype(jnp.float32)
        dk_blk = jnp.einsum("hqk,qhd->khd", dscores, q_win) * SOFTMAX_SCALE
        return dk_blk, dv_blk

    full_shape = (SEQ_LEN, HEADS_LOCAL, HEAD_DIM)
    dq_blocks = lax.map(dq_block, jnp.arange(N_BLOCKS))
    dk_blocks, dv_blocks = lax.map(dkv_block, jnp.arange(N_BLOCKS))
    return (dq_blocks.reshape(full_shape).astype(jnp.bfloat16), dk_blocks.reshape(full_shape).astype(jnp.bfloat16), dv_blocks.reshape(full_shape).astype(jnp.bfloat16))
```

```python
import functools

import jax
import jax.numpy as jnp
from jax import lax
from jax.experimental import pallas as pl
from jax.experimental.pallas import tpu as pltpu
from jax.sharding import PartitionSpec as P

REACH = 3
HEADS_PER_COPY = 2
LOG2E = 1.4426950408889634
MESH_ID = pl.DeviceIdType.MESH


def to_dev(idx):
    return {"cp": idx}


def greet_all(n_dev, me):
    barrier = pltpu.get_barrier_semaphore()
    for step in range(1, n_dev):
        pl.semaphore_signal(barrier, inc=1, device_id=to_dev(lax.rem(me + step, n_dev)), device_id_type=MESH_ID)
    pl.semaphore_wait(barrier, n_dev - 1)


def stat_copies(me, n_dev, stat_ref, swin_ref, send_sem, recv_sem):
    out = []
    for dist in range(1, REACH + 1):
        copy = pltpu.make_async_remote_copy(src_ref=stat_ref, dst_ref=swin_ref.at[dist - 1], send_sem=send_sem.at[dist - 1], recv_sem=recv_sem.at[dist - 1], device_id=to_dev(lax.rem(me + n_dev - dist, n_dev)), device_id_type=MESH_ID)
        out.append((dist, copy))
    return out


def near_kernel(n_dev, pk_ref, kv_ref, qd_ref, stat_ref, win_ref, swin_ref, st_s, st_r, own_s, own_r, x_s, x_r, y_s, y_r, fx_s, fx_r, fy_s, fy_r):
    me = lax.axis_index("cp")
    core = lax.rem(me, 2)
    chip = me // 2
    chip_odd = lax.rem(chip, 2)
    n_heads = pk_ref.shape[1]
    n_ch = n_heads // HEADS_PER_COPY
    relays = (chip == 0) | (chip == 3)
    x_dev, y_dev, mate = me + 2 - 4 * chip_odd, lax.rem(me + 4, n_dev), me + 1 - 2 * core
    x_dst = 1 + 3 * chip_odd
    x_slot = 4 - 3 * chip_odd
    y_slot = 5 - x_slot

    def heads(j):
        return pl.ds(j * HEADS_PER_COPY, HEADS_PER_COPY)

    def remote(src, dst, s_sem, r_sem, dev):
        return pltpu.make_async_remote_copy(src_ref=src, dst_ref=dst, send_sem=s_sem, recv_sem=r_sem, device_id=to_dev(dev), device_id_type=MESH_ID)

    def x_copy(j):
        return remote(pk_ref.at[:, heads(j)], win_ref.at[x_dst, :, heads(j)], x_s.at[j], x_r.at[j], x_dev)

    def y_copy(j):
        return remote(win_ref.at[x_slot, :, heads(j)], win_ref.at[5 - x_slot, :, heads(j)], y_s.at[j], y_r.at[j], y_dev)

    def mate_dst(slot_is_q):
        return 2 * (1 - core) + slot_is_q * (1 + 4 * core)

    def fx_copy(j):
        return remote(win_ref.at[x_slot, :, heads(j)], win_ref.at[mate_dst(1 - chip_odd), :, heads(j)], fx_s.at[j], fx_r.at[j], mate)

    def fy_copy(j):
        return remote(win_ref.at[y_slot, :, heads(j)], win_ref.at[mate_dst(chip_odd), :, heads(j)], fy_s.at[j], fy_r.at[j], mate)

    greet_all(n_dev, me)
    for j in range(n_ch):
        x_copy(j).start()
    own_kv = remote(kv_ref, win_ref.at[0], own_s, own_r, mate)
    own_qd = remote(qd_ref, win_ref.at[3], own_s, own_r, mate)
    pl.when(core == 0)(own_kv.start)
    pl.when(core == 1)(own_qd.start)
    stats = stat_copies(me, n_dev, stat_ref, swin_ref, st_s, st_r)
    for dist, copy in stats:
        pl.when(me >= dist)(copy.start)

    def step(j, carry):
        x_copy(j).wait_recv()
        pl.when(relays)(lambda: y_copy(j).start())
        fx_copy(j).start()

        def take_y():
            y_copy(j).wait_recv()
            fy_copy(j).start()

        pl.when(jnp.logical_not(relays))(take_y)
        return carry

    lax.fori_loop(0, n_ch, step, 0)
    own_kv.wait_send()
    own_qd.wait_recv()
    for dist, copy in stats:
        pl.when(me >= dist)(copy.wait_send)
        pl.when(me + dist < n_dev)(copy.wait_recv)

    def drain(j, carry):
        x_copy(j).wait_send()
        fx_copy(j).wait()
        pl.when(relays)(lambda: y_copy(j).wait_send())
        pl.when(jnp.logical_not(relays))(lambda: fy_copy(j).wait())
        return carry

    lax.fori_loop(0, n_ch, drain, 0)


def far_kernel(n_dev, kv_ref, qd_ref, stat_ref, win_ref, swin_ref, st_s, st_r, kv_s, kv_r, qd_s, qd_r):
    me = lax.axis_index("cp")
    greet_all(n_dev, me)
    stats = stat_copies(me, n_dev, stat_ref, swin_ref, st_s, st_r)
    for dist, copy in stats:
        up = pltpu.make_async_remote_copy(src_ref=kv_ref, dst_ref=win_ref.at[dist - 1], send_sem=kv_s.at[dist - 1], recv_sem=kv_r.at[dist - 1], device_id=to_dev(lax.rem(me + dist, n_dev)), device_id_type=MESH_ID)
        down = pltpu.make_async_remote_copy(src_ref=qd_ref, dst_ref=win_ref.at[REACH + dist - 1], send_sem=qd_s.at[dist - 1], recv_sem=qd_r.at[dist - 1], device_id=to_dev(lax.rem(me + n_dev - dist, n_dev)), device_id_type=MESH_ID)
        pl.when(me + dist < n_dev)(up.start)
        pl.when(me >= dist)(down.start)
        pl.when(me >= dist)(copy.start)
    for dist, copy in stats:
        up = pltpu.make_async_remote_copy(src_ref=kv_ref, dst_ref=win_ref.at[dist - 1], send_sem=kv_s.at[dist - 1], recv_sem=kv_r.at[dist - 1], device_id=to_dev(lax.rem(me + dist, n_dev)), device_id_type=MESH_ID)
        down = pltpu.make_async_remote_copy(src_ref=qd_ref, dst_ref=win_ref.at[REACH + dist - 1], send_sem=qd_s.at[dist - 1], recv_sem=qd_r.at[dist - 1], device_id=to_dev(lax.rem(me + n_dev - dist, n_dev)), device_id_type=MESH_ID)
        pl.when(me + dist < n_dev)(up.wait_send)
        pl.when(me >= dist)(up.wait_recv)
        pl.when(me >= dist)(down.wait_send)
        pl.when(me + dist < n_dev)(down.wait_recv)
        pl.when(me >= dist)(copy.wait_send)
        pl.when(me + dist < n_dev)(copy.wait_recv)


def nt_dot(a, b):
    return lax.dot_general(a, b, (((1,), (1,)), ((), ())), preferred_element_type=jnp.float32)


def nn_dot(a, b):
    return lax.dot_general(a, b, (((1,), (0,)), ((), ())), preferred_element_type=jnp.float32)


def tn_dot(a, b):
    return lax.dot_general(a, b, (((0,), (0,)), ((), ())), preferred_element_type=jnp.float32)


def grad_kernel(score_scale, flag_ref, qd_ref, kv_ref, win_ref, stat_ref, swin_ref, start_ref, dq_ref, dk_ref, dv_ref, dq_acc, dk_acc, dv_acc):
    head = pl.program_id(0)
    n_heads = pl.num_programs(0)
    base = flag_ref[2 * REACH]
    n_tok = qd_ref.shape[2]

    def terms(k_blk, v_blk, q_blk, do_blk, lse_row, delta_row, start_row, k_base, q_base):
        s_t = nt_dot(k_blk, q_blk)
        dp_t = nt_dot(v_blk, do_blk)
        k_pos = k_base + lax.broadcasted_iota(jnp.int32, s_t.shape, 0)
        q_pos = q_base + lax.broadcasted_iota(jnp.int32, s_t.shape, 1)
        keep = (k_pos >= start_row) & (k_pos <= q_pos)
        p_t = jnp.where(keep, jnp.exp2(s_t * (score_scale * LOG2E) - lse_row * LOG2E), 0.0)
        ds_t = (p_t * (dp_t - delta_row)).astype(jnp.bfloat16)
        return p_t.astype(jnp.bfloat16), ds_t

    q_blk, do_blk = qd_ref[0, 0], qd_ref[1, 0]
    k_blk, v_blk = kv_ref[0, 0], kv_ref[1, 0]
    lse_own, delta_own = stat_ref[pl.ds(head, 1), :], stat_ref[pl.ds(n_heads + head, 1), :]
    p_t, ds_t = terms(k_blk, v_blk, q_blk, do_blk, lse_own, delta_own, start_ref[0:1, :], base, base)
    dv_acc[...] = nn_dot(p_t, do_blk)
    dk_acc[...] = nn_dot(ds_t, q_blk)
    dq_acc[...] = tn_dot(ds_t, k_blk)
    for dist in range(1, REACH + 1):
        @pl.when(flag_ref[dist - 1] == 1)
        def _():
            k_far, v_far = win_ref[dist - 1, 0, 0], win_ref[dist - 1, 1, 0]
            _, ds_far = terms(k_far, v_far, q_blk, do_blk, lse_own, delta_own, start_ref[0:1, :], base - dist * n_tok, base)
            dq_acc[...] += tn_dot(ds_far, k_far)

        @pl.when(flag_ref[REACH + dist - 1] == 1)
        def _():
            q_far, do_far = win_ref[REACH + dist - 1, 0, 0], win_ref[REACH + dist - 1, 1, 0]
            lse_far = swin_ref[dist - 1, pl.ds(head, 1), :]
            delta_far = swin_ref[dist - 1, pl.ds(n_heads + head, 1), :]
            p_far, ds_far = terms(k_blk, v_blk, q_far, do_far, lse_far, delta_far, start_ref[dist:dist + 1, :], base, base + dist * n_tok)
            dv_acc[...] += nn_dot(p_far, do_far)
            dk_acc[...] += nn_dot(ds_far, q_far)

    dq_ref[0] = (dq_acc[...] * score_scale).astype(dq_ref.dtype)
    dk_ref[0] = (dk_acc[...] * score_scale).astype(dk_ref.dtype)
    dv_ref[0] = dv_acc[...].astype(dv_ref.dtype)


def solution(mesh):
    n_dev = mesh.shape["cp"]
    head_spec = P("cp", "hp", None)
    row_spec = P("cp", "hp")

    def device_fn(q_loc, k_loc, v_loc, o_loc, do_loc, lse_loc, cu_seqlens):
        n_tok, n_heads, head_dim = q_loc.shape
        seq_len = n_tok * n_dev
        score_scale = head_dim ** -0.5
        n_ch = n_heads // HEADS_PER_COPY
        me = lax.axis_index("cp")
        chip = me // 2

        def doc_start(pos):
            found = jnp.max(jnp.where(cu_seqlens <= pos[..., None], cu_seqlens, 0), axis=-1)
            return jnp.where(pos < seq_len, found, seq_len).astype(jnp.int32)

        base = me * n_tok
        start_rows = doc_start(base + jnp.arange((REACH + 1) * n_tok, dtype=jnp.int32)).reshape(REACH + 1, n_tok)
        dists = jnp.arange(1, REACH + 1, dtype=jnp.int32)
        kv_on = start_rows[0, 0] < base - (dists - 1) * n_tok
        qd_on = start_rows[1:, 0] < base + n_tok
        flags = jnp.concatenate([kv_on.astype(jnp.int32), qd_on.astype(jnp.int32), base[None]]).astype(jnp.int32)
        chip_pos = jnp.arange(2, n_dev // 2, dtype=jnp.int32) * 2 * n_tok
        far = jnp.any(doc_start(chip_pos) < chip_pos - 2 * n_tok)

        delta_loc = jnp.einsum("shd,shd->sh", do_loc, o_loc, preferred_element_type=jnp.float32)
        stat = jnp.concatenate([lse_loc.T, delta_loc.T])
        qd = jnp.stack([q_loc, do_loc]).transpose(0, 2, 1, 3)
        kv = jnp.stack([k_loc, v_loc]).transpose(0, 2, 1, 3)
        send_qd = start_rows[0] < 2 * n_tok * chip
        pk = jnp.where(send_qd[None, None, :, None], qd, kv)

        any_spec = pl.BlockSpec(memory_space=pl.ANY)
        dma = pltpu.SemaphoreType.DMA
        win_shapes = (jax.ShapeDtypeStruct((2 * REACH,) + qd.shape, qd.dtype), jax.ShapeDtypeStruct((REACH,) + stat.shape, stat.dtype))

        def near(pk, kv, qd, stat):
            return pl.pallas_call(functools.partial(near_kernel, n_dev), out_shape=win_shapes, in_specs=[any_spec] * 4, out_specs=(any_spec, any_spec),
                                  scratch_shapes=[dma((REACH,)), dma((REACH,)), dma, dma] + [dma((n_ch,))] * 8,
                                  compiler_params=pltpu.CompilerParams(collective_id=0, has_side_effects=True), name="near_exchange")(pk, kv, qd, stat)

        def wide(pk, kv, qd, stat):
            return pl.pallas_call(functools.partial(far_kernel, n_dev), out_shape=win_shapes, in_specs=[any_spec] * 3, out_specs=(any_spec, any_spec),
                                  scratch_shapes=[dma((REACH,))] * 6,
                                  compiler_params=pltpu.CompilerParams(collective_id=1, has_side_effects=True), name="wide_exchange")(kv, qd, stat)

        win, swin = lax.cond(far, wide, near, pk, kv, qd, stat)

        head_blk = lambda h, flag: (0, h, 0, 0)
        full2 = lambda h, flag: (0, 0)
        out_blk = pl.BlockSpec((1, n_tok, head_dim), lambda h, flag: (h, 0, 0))
        out_one = jax.ShapeDtypeStruct((n_heads, n_tok, head_dim), jnp.bfloat16)
        dq, dk, dv = pl.pallas_call(
            functools.partial(grad_kernel, score_scale),
            grid_spec=pltpu.PrefetchScalarGridSpec(
                num_scalar_prefetch=1, grid=(n_heads,),
                in_specs=[pl.BlockSpec((2, 1, n_tok, head_dim), head_blk), pl.BlockSpec((2, 1, n_tok, head_dim), head_blk),
                          pl.BlockSpec((2 * REACH, 2, 1, n_tok, head_dim), lambda h, flag: (0, 0, h, 0, 0)),
                          pl.BlockSpec(stat.shape, full2), pl.BlockSpec((REACH,) + stat.shape, lambda h, flag: (0, 0, 0)),
                          pl.BlockSpec((REACH + 1, n_tok), full2)],
                out_specs=[out_blk] * 3,
                scratch_shapes=[pltpu.VMEM((n_tok, head_dim), jnp.float32)] * 3),
            out_shape=(out_one, out_one, out_one), name="grads",
        )(flags, qd, kv, win, stat, swin, start_rows)
        return tuple(item.transpose(1, 0, 2) for item in (dq, dk, dv))

    return jax.shard_map(device_fn, mesh=mesh, in_specs=(head_spec, head_spec, head_spec, head_spec, head_spec, row_spec, P()), out_specs=(head_spec, head_spec, head_spec), check_vma=False)
```

```python
import functools

import jax
import jax.numpy as jnp
from jax import lax
from jax.experimental import pallas as pl
from jax.experimental.pallas import tpu as pltpu
from jax.sharding import PartitionSpec as P

REACH = 3
TILE_HEADS = 8
ROW_PARTS = 2
LOG2E = 1.4426950408889634
MESH_ID = pl.DeviceIdType.MESH


def to_dev(idx):
    return {"cp": idx}


def greet_all(n_dev, me):
    barrier = pltpu.get_barrier_semaphore()
    for step in range(1, n_dev):
        pl.semaphore_signal(barrier, inc=1, device_id=to_dev(lax.rem(me + step, n_dev)), device_id_type=MESH_ID)
    pl.semaphore_wait(barrier, n_dev - 1)


def stat_copies(me, n_dev, stat_ref, swin_ref, send_sem, recv_sem):
    out = []
    for dist in range(1, REACH + 1):
        copy = pltpu.make_async_remote_copy(src_ref=stat_ref, dst_ref=swin_ref.at[dist - 1], send_sem=send_sem.at[dist - 1], recv_sem=recv_sem.at[dist - 1], device_id=to_dev(lax.rem(me + n_dev - dist, n_dev)), device_id_type=MESH_ID)
        out.append((dist, copy))
    return out


def far_kernel(n_dev, kv_ref, qd_ref, stat_ref, win_ref, swin_ref, st_s, st_r, kv_s, kv_r, qd_s, qd_r):
    me = lax.axis_index("cp")
    greet_all(n_dev, me)
    stats = stat_copies(me, n_dev, stat_ref, swin_ref, st_s, st_r)
    for dist, copy in stats:
        up = pltpu.make_async_remote_copy(src_ref=kv_ref, dst_ref=win_ref.at[dist - 1], send_sem=kv_s.at[dist - 1], recv_sem=kv_r.at[dist - 1], device_id=to_dev(lax.rem(me + dist, n_dev)), device_id_type=MESH_ID)
        down = pltpu.make_async_remote_copy(src_ref=qd_ref, dst_ref=win_ref.at[REACH + dist - 1], send_sem=qd_s.at[dist - 1], recv_sem=qd_r.at[dist - 1], device_id=to_dev(lax.rem(me + n_dev - dist, n_dev)), device_id_type=MESH_ID)
        pl.when(me + dist < n_dev)(up.start)
        pl.when(me >= dist)(down.start)
        pl.when(me >= dist)(copy.start)
    for dist, copy in stats:
        up = pltpu.make_async_remote_copy(src_ref=kv_ref, dst_ref=win_ref.at[dist - 1], send_sem=kv_s.at[dist - 1], recv_sem=kv_r.at[dist - 1], device_id=to_dev(lax.rem(me + dist, n_dev)), device_id_type=MESH_ID)
        down = pltpu.make_async_remote_copy(src_ref=qd_ref, dst_ref=win_ref.at[REACH + dist - 1], send_sem=qd_s.at[dist - 1], recv_sem=qd_r.at[dist - 1], device_id=to_dev(lax.rem(me + n_dev - dist, n_dev)), device_id_type=MESH_ID)
        pl.when(me + dist < n_dev)(up.wait_send)
        pl.when(me >= dist)(up.wait_recv)
        pl.when(me >= dist)(down.wait_send)
        pl.when(me + dist < n_dev)(down.wait_recv)
        pl.when(me >= dist)(copy.wait_send)
        pl.when(me + dist < n_dev)(copy.wait_recv)


def nt_dot(a, b):
    return lax.dot_general(a, b, (((1,), (1,)), ((), ())), preferred_element_type=jnp.float32)


def nn_dot(a, b):
    return lax.dot_general(a, b, (((1,), (0,)), ((), ())), preferred_element_type=jnp.float32)


def tn_dot(a, b):
    return lax.dot_general(a, b, (((0,), (0,)), ((), ())), preferred_element_type=jnp.float32)


def block_terms(score_scale, k_blk, v_blk, q_blk, do_blk, lse_row, delta_row, start_row, k_base, q_base):
    s_t = nt_dot(k_blk, q_blk)
    dp_t = nt_dot(v_blk, do_blk)
    k_pos = k_base + lax.broadcasted_iota(jnp.int32, s_t.shape, 0)
    q_pos = q_base + lax.broadcasted_iota(jnp.int32, s_t.shape, 1)
    keep = (k_pos >= start_row) & (k_pos <= q_pos)
    p_t = jnp.where(keep, jnp.exp2(s_t * (score_scale * LOG2E) - lse_row * LOG2E), 0.0)
    ds_t = (p_t * (dp_t - delta_row)).astype(jnp.bfloat16)
    return p_t.astype(jnp.bfloat16), ds_t


def grad_kernel(score_scale, flag_ref, qd_ref, kv_ref, win_ref, stat_ref, swin_ref, start_ref, dq_ref, dk_ref, dv_ref, dq_acc, dk_acc, dv_acc):
    head = pl.program_id(0)
    n_heads = pl.num_programs(0)
    base = flag_ref[2 * REACH]
    n_tok = qd_ref.shape[2]

    terms = functools.partial(block_terms, score_scale)

    q_blk, do_blk = qd_ref[0, 0], qd_ref[1, 0]
    k_blk, v_blk = kv_ref[0, 0], kv_ref[1, 0]
    lse_own, delta_own = stat_ref[pl.ds(head, 1), :], stat_ref[pl.ds(n_heads + head, 1), :]
    p_t, ds_t = terms(k_blk, v_blk, q_blk, do_blk, lse_own, delta_own, start_ref[0:1, :], base, base)
    dv_acc[...] = nn_dot(p_t, do_blk)
    dk_acc[...] = nn_dot(ds_t, q_blk)
    dq_acc[...] = tn_dot(ds_t, k_blk)
    for dist in range(1, REACH + 1):
        @pl.when(flag_ref[dist - 1] == 1)
        def _():
            k_far, v_far = win_ref[dist - 1, 0, 0], win_ref[dist - 1, 1, 0]
            _, ds_far = terms(k_far, v_far, q_blk, do_blk, lse_own, delta_own, start_ref[0:1, :], base - dist * n_tok, base)
            dq_acc[...] += tn_dot(ds_far, k_far)

        @pl.when(flag_ref[REACH + dist - 1] == 1)
        def _():
            q_far, do_far = win_ref[REACH + dist - 1, 0, 0], win_ref[REACH + dist - 1, 1, 0]
            lse_far = swin_ref[dist - 1, pl.ds(head, 1), :]
            delta_far = swin_ref[dist - 1, pl.ds(n_heads + head, 1), :]
            p_far, ds_far = terms(k_blk, v_blk, q_far, do_far, lse_far, delta_far, start_ref[dist:dist + 1, :], base, base + dist * n_tok)
            dv_acc[...] += nn_dot(p_far, do_far)
            dk_acc[...] += nn_dot(ds_far, q_far)

    dq_ref[0] = (dq_acc[...] * score_scale).astype(dq_ref.dtype)
    dk_ref[0] = (dk_acc[...] * score_scale).astype(dk_ref.dtype)
    dv_ref[0] = dv_acc[...].astype(dv_ref.dtype)


def near_kernel(n_dev, score_scale, cu_ref, q_ref, k_ref, v_ref, o_ref, do_ref, lse_ref, dq_ref, dk_ref, dv_ref,
                raw, raw_o, qd, kv, pk, win, stat, swin, starts, out_hm, dq_acc, dk_acc, dv_acc,
                ld_sem, o_sem, out_sem, st_s, st_r, own_s, own_r, x_s, x_r, y_s, y_r, fx_s, fx_r, fy_s, fy_r):
    me = lax.axis_index("cp")
    core = lax.rem(me, 2)
    chip = me // 2
    chip_odd = lax.rem(chip, 2)
    n_tok, n_heads, _ = q_ref.shape
    part = n_tok // ROW_PARTS
    base = me * n_tok
    first_chip, last_chip = chip == 0, chip == n_dev // 2 - 1
    not_first, not_last = jnp.logical_not(first_chip), jnp.logical_not(last_chip)
    relays = first_chip | last_chip
    middle = jnp.logical_not(relays)
    x_dev, y_dev, mate = me + 2 - 4 * chip_odd, lax.rem(me + 4, n_dev), me + 1 - 2 * core
    x_dst = 1 + 2 * chip_odd
    x_slot = 3 - 2 * chip_odd
    y_slot = 4 - x_slot

    def remote(src, dst, s_sem, r_sem, dev):
        return pltpu.make_async_remote_copy(src_ref=src, dst_ref=dst, send_sem=s_sem, recv_sem=r_sem, device_id=to_dev(dev), device_id_type=MESH_ID)

    def block(slot, h, r):
        return win.at[slot, :, h, pl.ds(r * part, part)]

    def x_copy(h, r):
        return remote(pk.at[:, h, pl.ds(r * part, part)], block(x_dst, h, r), x_s.at[h, r], x_r.at[h, r], x_dev)

    def y_copy(h, r):
        return remote(block(x_slot, h, r), block(y_slot, h, r), y_s.at[h, r], y_r.at[h, r], y_dev)

    def fx_copy(h, r):
        return remote(block(x_slot, h, r), block(4 - 2 * core - 2 * chip_odd, h, r), fx_s.at[h, r], fx_r.at[h, r], mate)

    def fy_copy(h, r):
        return remote(block(y_slot, h, r), block(2 - 2 * core + 2 * chip_odd, h, r), fy_s.at[h, r], fy_r.at[h, r], mate)

    def own_kv(h):
        return remote(kv.at[:, h], win.at[0, :, h], own_s.at[h], own_r.at[h], mate)

    def own_qd(h):
        return remote(qd.at[:, h], win.at[4, :, h], own_s.at[h], own_r.at[h], mate)

    def load(half, which):
        src = (q_ref, k_ref, do_ref, v_ref)[which]
        return pltpu.make_async_copy(src.at[:, pl.ds(half * TILE_HEADS, TILE_HEADS)], raw.at[half, which], ld_sem.at[half, which])

    halves = n_heads // TILE_HEADS
    for half in range(halves):
        for which in range(4):
            load(half, which).start()
    load_o = pltpu.make_async_copy(o_ref, raw_o, o_sem)
    load_o.start()

    chip_pos = chip * 2 * n_tok
    pos = base + n_tok * lax.broadcasted_iota(jnp.int32, starts.shape, 0) + lax.broadcasted_iota(jnp.int32, starts.shape, 1)

    def scan_docs(n, carry):
        found, cross_end = carry
        first, last = cu_ref[n], cu_ref[n + 1]
        crosses = (first < chip_pos) & (last > chip_pos)
        return jnp.where(first <= pos, jnp.maximum(found, first), found), jnp.where(crosses, last, cross_end)

    found, cross_end = lax.fori_loop(0, cu_ref.shape[0] - 1, scan_docs, (jnp.zeros(starts.shape, jnp.int32), 0))
    starts[...] = jnp.where(pos < n_dev * n_tok, found, n_dev * n_tok)
    send_rows = jnp.clip(cross_end - base, 0, n_tok)
    send_qd = lax.broadcasted_iota(jnp.int32, (TILE_HEADS, n_tok, q_ref.shape[2]), 1) < send_rows

    greet_all(n_dev, me)
    stats = stat_copies(me, n_dev, stat, swin, st_s, st_r)

    def send_heads(half):
        for h in range(half * TILE_HEADS, (half + 1) * TILE_HEADS):
            for r in range(ROW_PARTS):
                x_copy(h, r).start()
        for h in range(half * TILE_HEADS, (half + 1) * TILE_HEADS):
            pl.when(core == 0)(own_kv(h).start)
            pl.when(core == 1)(own_qd(h).start)

    for half in range(halves):
        rows = pl.ds(half * TILE_HEADS, TILE_HEADS)
        for pair in range(2):
            load(half, 2 * pair).wait()
            load(half, 2 * pair + 1).wait()
            q_side = jnp.swapaxes(raw[half, 2 * pair], 0, 1)
            k_side = jnp.swapaxes(raw[half, 2 * pair + 1], 0, 1)
            pk[pair, rows] = jnp.where(send_qd, q_side, k_side)
            qd[pair, rows] = q_side
            kv[pair, rows] = k_side
        if half == 0:
            load_o.wait()
            stat[0:n_heads, :] = lse_ref[...]
        delta = jnp.sum(raw[half, 2].astype(jnp.float32) * raw_o[:, half * TILE_HEADS:(half + 1) * TILE_HEADS, :].astype(jnp.float32), axis=-1)
        stat[n_heads + half * TILE_HEADS:n_heads + (half + 1) * TILE_HEADS, :] = delta.T
        send_heads(half)
    for dist, copy in stats:
        pl.when(me >= dist)(copy.start)
    for dist, copy in stats:
        pl.when(me + dist < n_dev)(copy.wait_recv)

    terms = functools.partial(block_terms, score_scale)

    def arrive(h):
        for r in range(ROW_PARTS):
            x_copy(h, r).wait_recv()
            pl.when(relays)(lambda: y_copy(h, r).start())
            fx_copy(h, r).start()

    def arrive_y(h):
        for r in range(ROW_PARTS):
            y_copy(h, r).wait_recv()
            fy_copy(h, r).start()

    def compute(h):
        own_qd(h).wait_recv()
        for r in range(ROW_PARTS):
            fx_copy(h, r).wait_recv()

        @pl.when(middle)
        def _():
            for r in range(ROW_PARTS):
                fy_copy(h, r).wait_recv()

        q_blk, do_blk, k_blk, v_blk = qd[0, h], qd[1, h], kv[0, h], kv[1, h]
        lse_own, delta_own = stat[pl.ds(h, 1), :], stat[pl.ds(n_heads + h, 1), :]
        p_t, ds_t = terms(k_blk, v_blk, q_blk, do_blk, lse_own, delta_own, starts[0:1, :], base, base)
        dv_acc[...] = nn_dot(p_t, do_blk)
        dk_acc[...] = nn_dot(ds_t, q_blk)
        dq_acc[...] = tn_dot(ds_t, k_blk)
        for dist in range(1, REACH + 1):
            k_here = {1: (core == 1) | not_first, 2: not_first, 3: (core == 1) & not_first}[dist]
            q_here = {1: (core == 0) | not_last, 2: not_last, 3: (core == 0) & not_last}[dist]

            @pl.when(k_here)
            def _():
                k_far, v_far = win[dist - 1, 0, h], win[dist - 1, 1, h]
                _, ds_far = terms(k_far, v_far, q_blk, do_blk, lse_own, delta_own, starts[0:1, :], base - dist * n_tok, base)
                dq_acc[...] += tn_dot(ds_far, k_far)

            @pl.when(q_here)
            def _():
                q_far, do_far = win[5 - dist, 0, h], win[5 - dist, 1, h]
                lse_far = swin[dist - 1, pl.ds(h, 1), :]
                delta_far = swin[dist - 1, pl.ds(n_heads + h, 1), :]
                p_far, ds_far = terms(k_blk, v_blk, q_far, do_far, lse_far, delta_far, starts[dist:dist + 1, :], base, base + dist * n_tok)
                dv_acc[...] += nn_dot(p_far, do_far)
                dk_acc[...] += nn_dot(ds_far, q_far)

        h_in = lax.rem(h, TILE_HEADS)
        out_hm[0, h_in] = (dq_acc[...] * score_scale).astype(out_hm.dtype)
        out_hm[1, h_in] = (dk_acc[...] * score_scale).astype(out_hm.dtype)
        out_hm[2, h_in] = dv_acc[...].astype(out_hm.dtype)

    def out_copy(half, which):
        dst = (dq_ref, dk_ref, dv_ref)[which]
        rows = pl.ds(half * TILE_HEADS, TILE_HEADS)
        return pltpu.make_async_copy(raw.at[half, which], dst.at[:, rows], out_sem.at[half, which])

    def step(t, carry):
        pl.when(t < n_heads)(lambda: arrive(t))
        pl.when(t >= 2)(lambda: compute(t - 2))
        for half in range(halves):
            @pl.when(t - 2 == (half + 1) * TILE_HEADS - 1)
            def _():
                for which in range(3):
                    raw[half, which] = jnp.swapaxes(out_hm[which], 0, 1)
                for which in range(3):
                    out_copy(half, which).start()
        pl.when((t >= 1) & (t <= n_heads) & middle)(lambda: arrive_y(t - 1))
        return carry

    lax.fori_loop(0, n_heads + 2, step, 0)

    def drain(h, carry):
        own_kv(h).wait_send()
        for r in range(ROW_PARTS):
            x_copy(h, r).wait_send()
            fx_copy(h, r).wait_send()
            pl.when(relays)(lambda: y_copy(h, r).wait_send())
            pl.when(middle)(lambda: fy_copy(h, r).wait_send())
        return carry

    lax.fori_loop(0, n_heads, drain, 0)
    for dist, copy in stats:
        pl.when(me >= dist)(copy.wait_send)
    for half in range(halves):
        for which in range(3):
            out_copy(half, which).wait()


def solution(mesh):
    n_dev = mesh.shape["cp"]
    head_spec = P("cp", "hp", None)
    row_spec = P("cp", "hp")
    any_spec = pl.BlockSpec(memory_space=pl.ANY)
    vmem_spec = pl.BlockSpec(memory_space=pltpu.VMEM)
    smem_spec = pl.BlockSpec(memory_space=pltpu.SMEM)
    dma = pltpu.SemaphoreType.DMA

    def device_fn(q_loc, k_loc, v_loc, o_loc, do_loc, lse_loc, cu_seqlens):
        n_tok, n_heads, head_dim = q_loc.shape
        seq_len = n_tok * n_dev
        score_scale = head_dim ** -0.5
        me = lax.axis_index("cp")
        pair_shape = (2, n_heads, n_tok, head_dim)

        def wide(q_loc, k_loc, v_loc, o_loc, do_loc, lse_loc, cu_seqlens):
            def doc_start(pos):
                found = jnp.max(jnp.where(cu_seqlens <= pos[..., None], cu_seqlens, 0), axis=-1)
                return jnp.where(pos < seq_len, found, seq_len).astype(jnp.int32)

            base = me * n_tok
            start_rows = doc_start(base + jnp.arange((REACH + 1) * n_tok, dtype=jnp.int32)).reshape(REACH + 1, n_tok)
            dists = jnp.arange(1, REACH + 1, dtype=jnp.int32)
            kv_on = start_rows[0, 0] < base - (dists - 1) * n_tok
            qd_on = start_rows[1:, 0] < base + n_tok
            flags = jnp.concatenate([kv_on.astype(jnp.int32), qd_on.astype(jnp.int32), base[None]]).astype(jnp.int32)
            delta_loc = jnp.einsum("shd,shd->sh", do_loc, o_loc, preferred_element_type=jnp.float32)
            stat = jnp.concatenate([lse_loc.T, delta_loc.T])
            qd = jnp.stack([q_loc, do_loc]).transpose(0, 2, 1, 3)
            kv = jnp.stack([k_loc, v_loc]).transpose(0, 2, 1, 3)
            win_shapes = (jax.ShapeDtypeStruct((2 * REACH,) + qd.shape, qd.dtype), jax.ShapeDtypeStruct((REACH,) + stat.shape, stat.dtype))
            win, swin = pl.pallas_call(functools.partial(far_kernel, n_dev), out_shape=win_shapes, in_specs=[any_spec] * 3, out_specs=(any_spec, any_spec),
                                       scratch_shapes=[dma((REACH,))] * 6,
                                       compiler_params=pltpu.CompilerParams(collective_id=1, has_side_effects=True), name="wide_exchange")(kv, qd, stat)
            head_blk = lambda h, flag: (0, h, 0, 0)
            full2 = lambda h, flag: (0, 0)
            out_blk = pl.BlockSpec((1, n_tok, head_dim), lambda h, flag: (h, 0, 0))
            out_one = jax.ShapeDtypeStruct((n_heads, n_tok, head_dim), jnp.bfloat16)
            dq, dk, dv = pl.pallas_call(
                functools.partial(grad_kernel, score_scale),
                grid_spec=pltpu.PrefetchScalarGridSpec(
                    num_scalar_prefetch=1, grid=(n_heads,),
                    in_specs=[pl.BlockSpec((2, 1, n_tok, head_dim), head_blk), pl.BlockSpec((2, 1, n_tok, head_dim), head_blk),
                              pl.BlockSpec((2 * REACH, 2, 1, n_tok, head_dim), lambda h, flag: (0, 0, h, 0, 0)),
                              pl.BlockSpec(stat.shape, full2), pl.BlockSpec((REACH,) + stat.shape, lambda h, flag: (0, 0, 0)),
                              pl.BlockSpec((REACH + 1, n_tok), full2)],
                    out_specs=[out_blk] * 3,
                    scratch_shapes=[pltpu.VMEM((n_tok, head_dim), jnp.float32)] * 3),
                out_shape=(out_one, out_one, out_one), name="grads",
            )(flags, qd, kv, win, stat, swin, start_rows)
            return tuple(item.transpose(1, 0, 2) for item in (dq, dk, dv))

        def near(q_loc, k_loc, v_loc, o_loc, do_loc, lse_loc, cu_seqlens):
            out_one = jax.ShapeDtypeStruct(q_loc.shape, q_loc.dtype)
            bf16, f32 = jnp.bfloat16, jnp.float32
            return pl.pallas_call(
                functools.partial(near_kernel, n_dev, score_scale),
                out_shape=(out_one, out_one, out_one),
                in_specs=[smem_spec] + [any_spec] * 5 + [vmem_spec], out_specs=(any_spec,) * 3,
                scratch_shapes=[pltpu.VMEM((n_heads // TILE_HEADS, 4, n_tok, TILE_HEADS, head_dim), bf16), pltpu.VMEM(q_loc.shape, bf16)]
                + [pltpu.VMEM(pair_shape, bf16)] * 3 + [pltpu.VMEM((5,) + pair_shape, bf16)]
                + [pltpu.VMEM((2 * n_heads, n_tok), f32), pltpu.VMEM((REACH, 2 * n_heads, n_tok), f32), pltpu.VMEM((8, n_tok), jnp.int32)]
                + [pltpu.VMEM((3, TILE_HEADS, n_tok, head_dim), bf16)] + [pltpu.VMEM((n_tok, head_dim), f32)] * 3
                + [dma((n_heads // TILE_HEADS, 4)), dma, dma((n_heads // TILE_HEADS, 3)), dma((REACH,)), dma((REACH,)), dma((n_heads,)), dma((n_heads,))]
                + [dma((n_heads, ROW_PARTS))] * 8,
                compiler_params=pltpu.CompilerParams(collective_id=0, has_side_effects=True), name="near_grads",
            )(cu_seqlens, q_loc, k_loc, v_loc, o_loc, do_loc, lse_loc.T)

        chip_pos = jnp.arange(1, n_dev // 2 - 1, dtype=jnp.int32)[:, None] * 2 * n_tok
        far = jnp.any((cu_seqlens[None, :-1] < chip_pos) & (cu_seqlens[None, 1:] > chip_pos + 2 * n_tok))
        return lax.cond(far, wide, near, q_loc, k_loc, v_loc, o_loc, do_loc, lse_loc, cu_seqlens)

    return jax.shard_map(device_fn, mesh=mesh, in_specs=(head_spec, head_spec, head_spec, head_spec, head_spec, row_spec, P()), out_specs=(head_spec, head_spec, head_spec), check_vma=False)
```

```python
import functools

import jax
import jax.numpy as jnp
from jax import lax
from jax.experimental import pallas as pl
from jax.experimental.pallas import tpu as pltpu
from jax.sharding import PartitionSpec as P

REACH = 3
TILE_HEADS = 8
ROW_PARTS = 2
HEADS_AHEAD = 1
LOG2E = 1.4426950408889634
MESH_ID = pl.DeviceIdType.MESH


def to_dev(idx):
    return {"cp": idx}


def greet_all(n_dev, me):
    barrier = pltpu.get_barrier_semaphore()
    for step in range(1, n_dev):
        pl.semaphore_signal(barrier, inc=1, device_id=to_dev(lax.rem(me + step, n_dev)), device_id_type=MESH_ID)


def await_all(n_dev):
    pl.semaphore_wait(pltpu.get_barrier_semaphore(), n_dev - 1)


def stat_copies(me, n_dev, stat_ref, swin_ref, send_sem, recv_sem):
    out = []
    for dist in range(1, REACH + 1):
        copy = pltpu.make_async_remote_copy(src_ref=stat_ref, dst_ref=swin_ref.at[dist - 1], send_sem=send_sem.at[dist - 1], recv_sem=recv_sem.at[dist - 1], device_id=to_dev(lax.rem(me + n_dev - dist, n_dev)), device_id_type=MESH_ID)
        out.append((dist, copy))
    return out


def far_kernel(n_dev, kv_ref, qd_ref, stat_ref, win_ref, swin_ref, st_s, st_r, kv_s, kv_r, qd_s, qd_r):
    me = lax.axis_index("cp")
    greet_all(n_dev, me)
    await_all(n_dev)
    stats = stat_copies(me, n_dev, stat_ref, swin_ref, st_s, st_r)
    for dist, copy in stats:
        up = pltpu.make_async_remote_copy(src_ref=kv_ref, dst_ref=win_ref.at[dist - 1], send_sem=kv_s.at[dist - 1], recv_sem=kv_r.at[dist - 1], device_id=to_dev(lax.rem(me + dist, n_dev)), device_id_type=MESH_ID)
        down = pltpu.make_async_remote_copy(src_ref=qd_ref, dst_ref=win_ref.at[REACH + dist - 1], send_sem=qd_s.at[dist - 1], recv_sem=qd_r.at[dist - 1], device_id=to_dev(lax.rem(me + n_dev - dist, n_dev)), device_id_type=MESH_ID)
        pl.when(me + dist < n_dev)(up.start)
        pl.when(me >= dist)(down.start)
        pl.when(me >= dist)(copy.start)
    for dist, copy in stats:
        up = pltpu.make_async_remote_copy(src_ref=kv_ref, dst_ref=win_ref.at[dist - 1], send_sem=kv_s.at[dist - 1], recv_sem=kv_r.at[dist - 1], device_id=to_dev(lax.rem(me + dist, n_dev)), device_id_type=MESH_ID)
        down = pltpu.make_async_remote_copy(src_ref=qd_ref, dst_ref=win_ref.at[REACH + dist - 1], send_sem=qd_s.at[dist - 1], recv_sem=qd_r.at[dist - 1], device_id=to_dev(lax.rem(me + n_dev - dist, n_dev)), device_id_type=MESH_ID)
        pl.when(me + dist < n_dev)(up.wait_send)
        pl.when(me >= dist)(up.wait_recv)
        pl.when(me >= dist)(down.wait_send)
        pl.when(me + dist < n_dev)(down.wait_recv)
        pl.when(me >= dist)(copy.wait_send)
        pl.when(me + dist < n_dev)(copy.wait_recv)


def nt_dot(a, b):
    return lax.dot_general(a, b, (((1,), (1,)), ((), ())), preferred_element_type=jnp.float32)


def nn_dot(a, b):
    return lax.dot_general(a, b, (((1,), (0,)), ((), ())), preferred_element_type=jnp.float32)


def tn_dot(a, b):
    return lax.dot_general(a, b, (((0,), (0,)), ((), ())), preferred_element_type=jnp.float32)


def block_terms(score_scale, k_blk, v_blk, q_blk, do_blk, lse_row, delta_row, start_row, k_base, q_base):
    s_t = nt_dot(k_blk, q_blk)
    dp_t = nt_dot(v_blk, do_blk)
    k_pos = k_base + lax.broadcasted_iota(jnp.int32, s_t.shape, 0)
    q_pos = q_base + lax.broadcasted_iota(jnp.int32, s_t.shape, 1)
    keep = (k_pos >= start_row) & (k_pos <= q_pos)
    p_t = jnp.where(keep, jnp.exp2(s_t * (score_scale * LOG2E) - lse_row * LOG2E), 0.0)
    ds_t = (p_t * (dp_t - delta_row)).astype(jnp.bfloat16)
    return p_t.astype(jnp.bfloat16), ds_t


def grad_kernel(score_scale, flag_ref, qd_ref, kv_ref, win_ref, stat_ref, swin_ref, start_ref, dq_ref, dk_ref, dv_ref, dq_acc, dk_acc, dv_acc):
    head = pl.program_id(0)
    n_heads = pl.num_programs(0)
    base = flag_ref[2 * REACH]
    n_tok = qd_ref.shape[2]

    terms = functools.partial(block_terms, score_scale)

    q_blk, do_blk = qd_ref[0, 0], qd_ref[1, 0]
    k_blk, v_blk = kv_ref[0, 0], kv_ref[1, 0]
    lse_own, delta_own = stat_ref[pl.ds(head, 1), :], stat_ref[pl.ds(n_heads + head, 1), :]
    p_t, ds_t = terms(k_blk, v_blk, q_blk, do_blk, lse_own, delta_own, start_ref[0:1, :], base, base)
    dv_acc[...] = nn_dot(p_t, do_blk)
    dk_acc[...] = nn_dot(ds_t, q_blk)
    dq_acc[...] = tn_dot(ds_t, k_blk)
    for dist in range(1, REACH + 1):
        @pl.when(flag_ref[dist - 1] == 1)
        def _():
            k_far, v_far = win_ref[dist - 1, 0, 0], win_ref[dist - 1, 1, 0]
            _, ds_far = terms(k_far, v_far, q_blk, do_blk, lse_own, delta_own, start_ref[0:1, :], base - dist * n_tok, base)
            dq_acc[...] += tn_dot(ds_far, k_far)

        @pl.when(flag_ref[REACH + dist - 1] == 1)
        def _():
            q_far, do_far = win_ref[REACH + dist - 1, 0, 0], win_ref[REACH + dist - 1, 1, 0]
            lse_far = swin_ref[dist - 1, pl.ds(head, 1), :]
            delta_far = swin_ref[dist - 1, pl.ds(n_heads + head, 1), :]
            p_far, ds_far = terms(k_blk, v_blk, q_far, do_far, lse_far, delta_far, start_ref[dist:dist + 1, :], base, base + dist * n_tok)
            dv_acc[...] += nn_dot(p_far, do_far)
            dk_acc[...] += nn_dot(ds_far, q_far)

    dq_ref[0] = (dq_acc[...] * score_scale).astype(dq_ref.dtype)
    dk_ref[0] = (dk_acc[...] * score_scale).astype(dk_ref.dtype)
    dv_ref[0] = dv_acc[...].astype(dv_ref.dtype)


def near_kernel(n_dev, score_scale, cu_ref, q_ref, k_ref, v_ref, o_ref, do_ref, lse_ref, dq_ref, dk_ref, dv_ref,
                raw, raw_o, qd, kv, pk, win, stat, swin, starts, out_hm, dq_acc, dk_acc, dv_acc,
                ld_sem, o_sem, out_sem, st_s, st_r, own_s, own_r, x_s, x_r, y_s, y_r, fx_s, fx_r, fy_s, fy_r):
    me = lax.axis_index("cp")
    core = lax.rem(me, 2)
    chip = me // 2
    chip_odd = lax.rem(chip, 2)
    n_tok, n_heads, _ = q_ref.shape
    part = n_tok // ROW_PARTS
    base = me * n_tok
    first_chip, last_chip = chip == 0, chip == n_dev // 2 - 1
    not_first, not_last = jnp.logical_not(first_chip), jnp.logical_not(last_chip)
    relays = first_chip | last_chip
    middle = jnp.logical_not(relays)
    x_dev, y_dev, mate = me + 2 - 4 * chip_odd, lax.rem(me + 4, n_dev), me + 1 - 2 * core
    x_dst = 1 + 2 * chip_odd
    x_slot = 3 - 2 * chip_odd
    y_slot = 4 - x_slot

    def remote(src, dst, s_sem, r_sem, dev):
        return pltpu.make_async_remote_copy(src_ref=src, dst_ref=dst, send_sem=s_sem, recv_sem=r_sem, device_id=to_dev(dev), device_id_type=MESH_ID)

    def block(slot, h, r):
        return win.at[slot, :, h, pl.ds(r * part, part)]

    def x_copy(h, r):
        return remote(pk.at[:, h, pl.ds(r * part, part)], block(x_dst, h, r), x_s.at[h, r], x_r.at[h, r], x_dev)

    def y_copy(h, r):
        return remote(block(x_slot, h, r), block(y_slot, h, r), y_s.at[h, r], y_r.at[h, r], y_dev)

    def fx_copy(h, r):
        return remote(block(x_slot, h, r), block(4 - 2 * core - 2 * chip_odd, h, r), fx_s.at[h, r], fx_r.at[h, r], mate)

    def fy_copy(h, r):
        return remote(block(y_slot, h, r), block(2 - 2 * core + 2 * chip_odd, h, r), fy_s.at[h, r], fy_r.at[h, r], mate)

    def own_kv(h):
        return remote(kv.at[:, h], win.at[0, :, h], own_s.at[h], own_r.at[h], mate)

    def own_qd(h):
        return remote(qd.at[:, h], win.at[4, :, h], own_s.at[h], own_r.at[h], mate)

    halves = n_heads // TILE_HEADS
    units = [(half, r) for half in range(halves) for r in range(ROW_PARTS)]

    def load(half, r, which):
        src = (q_ref, k_ref, do_ref, v_ref)[which]
        rows, heads = pl.ds(r * part, part), pl.ds(half * TILE_HEADS, TILE_HEADS)
        return pltpu.make_async_copy(src.at[rows, heads], raw.at[half, which, rows], ld_sem.at[half, r, which])

    greet_all(n_dev, me)
    for half, r in units:
        for which in range(4):
            load(half, r, which).start()
    load_o = pltpu.make_async_copy(o_ref, raw_o, o_sem)
    load_o.start()

    chip_pos = chip * 2 * n_tok
    pos = base + n_tok * lax.broadcasted_iota(jnp.int32, starts.shape, 0) + lax.broadcasted_iota(jnp.int32, starts.shape, 1)

    def scan_docs(n, carry):
        found, cross_end = carry
        first, last = cu_ref[n], cu_ref[n + 1]
        crosses = (first < chip_pos) & (last > chip_pos)
        return jnp.where(first <= pos, jnp.maximum(found, first), found), jnp.where(crosses, last, cross_end)

    found, cross_end = lax.fori_loop(0, cu_ref.shape[0] - 1, scan_docs, (jnp.zeros(starts.shape, jnp.int32), 0))
    starts[...] = jnp.where(pos < n_dev * n_tok, found, n_dev * n_tok)
    send_rows = jnp.clip(cross_end - base, 0, n_tok)
    row_ids = lax.broadcasted_iota(jnp.int32, (TILE_HEADS, part, q_ref.shape[2]), 1)
    stats = stat_copies(me, n_dev, stat, swin, st_s, st_r)

    def arrange(half, r):
        rows, heads = pl.ds(r * part, part), pl.ds(half * TILE_HEADS, TILE_HEADS)
        for pair in range(2):
            load(half, r, 2 * pair).wait()
            load(half, r, 2 * pair + 1).wait()
            q_side = jnp.swapaxes(raw[half, 2 * pair, rows], 0, 1)
            k_side = jnp.swapaxes(raw[half, 2 * pair + 1, rows], 0, 1)
            pk[pair, heads, rows] = jnp.where(row_ids < send_rows - r * part, q_side, k_side)
            qd[pair, heads, rows] = q_side
            kv[pair, heads, rows] = k_side

    def start_own(half):
        for h in range(half * TILE_HEADS, (half + 1) * TILE_HEADS):
            pl.when(core == 0)(own_kv(h).start)
            pl.when(core == 1)(own_qd(h).start)

    for r in range(ROW_PARTS):
        arrange(0, r)
        if r == 0:
            await_all(n_dev)
        x_copy(0, r).start()
    start_own(0)
    for half in range(1, halves):
        for r in range(ROW_PARTS):
            arrange(half, r)
        start_own(half)
    load_o.wait()
    stat[0:n_heads, :] = lse_ref[...]
    for half in range(halves):
        delta = jnp.sum(raw[half, 2].astype(jnp.float32) * raw_o[:, half * TILE_HEADS:(half + 1) * TILE_HEADS, :].astype(jnp.float32), axis=-1)
        stat[n_heads + half * TILE_HEADS:n_heads + (half + 1) * TILE_HEADS, :] = delta.T
    for dist, copy in stats:
        pl.when(me >= dist)(copy.start)

    terms = functools.partial(block_terms, score_scale)

    def arrive(h):
        for r in range(ROW_PARTS):
            pl.when(h + HEADS_AHEAD < n_heads)(lambda: x_copy(h + HEADS_AHEAD, r).start())
            x_copy(h, r).wait_recv()
            pl.when(relays)(lambda: y_copy(h, r).start())
            fx_copy(h, r).start()

    def arrive_y(h):
        for r in range(ROW_PARTS):
            y_copy(h, r).wait_recv()
            fy_copy(h, r).start()

    def compute(h):
        own_qd(h).wait_recv()
        for r in range(ROW_PARTS):
            fx_copy(h, r).wait_recv()

        @pl.when(middle)
        def _():
            for r in range(ROW_PARTS):
                fy_copy(h, r).wait_recv()

        q_blk, do_blk, k_blk, v_blk = qd[0, h], qd[1, h], kv[0, h], kv[1, h]
        lse_own, delta_own = stat[pl.ds(h, 1), :], stat[pl.ds(n_heads + h, 1), :]
        p_t, ds_t = terms(k_blk, v_blk, q_blk, do_blk, lse_own, delta_own, starts[0:1, :], base, base)
        dv_acc[...] = nn_dot(p_t, do_blk)
        dk_acc[...] = nn_dot(ds_t, q_blk)
        dq_acc[...] = tn_dot(ds_t, k_blk)
        for dist in range(1, REACH + 1):
            k_here = {1: (core == 1) | not_first, 2: not_first, 3: (core == 1) & not_first}[dist]
            q_here = {1: (core == 0) | not_last, 2: not_last, 3: (core == 0) & not_last}[dist]

            @pl.when(k_here)
            def _():
                k_far, v_far = win[dist - 1, 0, h], win[dist - 1, 1, h]
                _, ds_far = terms(k_far, v_far, q_blk, do_blk, lse_own, delta_own, starts[0:1, :], base - dist * n_tok, base)
                dq_acc[...] += tn_dot(ds_far, k_far)

            @pl.when(q_here)
            def _():
                q_far, do_far = win[5 - dist, 0, h], win[5 - dist, 1, h]
                lse_far = swin[dist - 1, pl.ds(h, 1), :]
                delta_far = swin[dist - 1, pl.ds(n_heads + h, 1), :]
                p_far, ds_far = terms(k_blk, v_blk, q_far, do_far, lse_far, delta_far, starts[dist:dist + 1, :], base, base + dist * n_tok)
                dv_acc[...] += nn_dot(p_far, do_far)
                dk_acc[...] += nn_dot(ds_far, q_far)

        h_in = lax.rem(h, TILE_HEADS)
        out_hm[0, h_in] = (dq_acc[...] * score_scale).astype(out_hm.dtype)
        out_hm[1, h_in] = (dk_acc[...] * score_scale).astype(out_hm.dtype)
        out_hm[2, h_in] = dv_acc[...].astype(out_hm.dtype)

    def out_copy(half, which):
        dst = (dq_ref, dk_ref, dv_ref)[which]
        rows = pl.ds(half * TILE_HEADS, TILE_HEADS)
        return pltpu.make_async_copy(raw.at[half, which], dst.at[:, rows], out_sem.at[half, which])

    def step(t, carry):
        pl.when(t < n_heads)(lambda: arrive(t))

        @pl.when(t == 2)
        def _():
            for dist, copy in stats:
                pl.when(me + dist < n_dev)(copy.wait_recv)

        pl.when(t >= 2)(lambda: compute(t - 2))
        for half in range(halves):
            @pl.when(t - 2 == (half + 1) * TILE_HEADS - 1)
            def _():
                for which in range(3):
                    raw[half, which] = jnp.swapaxes(out_hm[which], 0, 1)
                for which in range(3):
                    out_copy(half, which).start()
        pl.when((t >= 1) & (t <= n_heads) & middle)(lambda: arrive_y(t - 1))
        return carry

    lax.fori_loop(0, n_heads + 2, step, 0)

    def drain(h, carry):
        own_kv(h).wait_send()
        for r in range(ROW_PARTS):
            x_copy(h, r).wait_send()
            fx_copy(h, r).wait_send()
            pl.when(relays)(lambda: y_copy(h, r).wait_send())
            pl.when(middle)(lambda: fy_copy(h, r).wait_send())
        return carry

    lax.fori_loop(0, n_heads, drain, 0)
    for dist, copy in stats:
        pl.when(me >= dist)(copy.wait_send)
    for half in range(halves):
        for which in range(3):
            out_copy(half, which).wait()


def solution(mesh):
    n_dev = mesh.shape["cp"]
    head_spec = P("cp", "hp", None)
    row_spec = P("cp", "hp")
    any_spec = pl.BlockSpec(memory_space=pl.ANY)
    vmem_spec = pl.BlockSpec(memory_space=pltpu.VMEM)
    smem_spec = pl.BlockSpec(memory_space=pltpu.SMEM)
    dma = pltpu.SemaphoreType.DMA

    def device_fn(q_loc, k_loc, v_loc, o_loc, do_loc, lse_loc, cu_seqlens):
        n_tok, n_heads, head_dim = q_loc.shape
        seq_len = n_tok * n_dev
        score_scale = head_dim ** -0.5
        me = lax.axis_index("cp")
        pair_shape = (2, n_heads, n_tok, head_dim)

        def wide(q_loc, k_loc, v_loc, o_loc, do_loc, lse_loc, cu_seqlens):
            def doc_start(pos):
                found = jnp.max(jnp.where(cu_seqlens <= pos[..., None], cu_seqlens, 0), axis=-1)
                return jnp.where(pos < seq_len, found, seq_len).astype(jnp.int32)

            base = me * n_tok
            start_rows = doc_start(base + jnp.arange((REACH + 1) * n_tok, dtype=jnp.int32)).reshape(REACH + 1, n_tok)
            dists = jnp.arange(1, REACH + 1, dtype=jnp.int32)
            kv_on = start_rows[0, 0] < base - (dists - 1) * n_tok
            qd_on = start_rows[1:, 0] < base + n_tok
            flags = jnp.concatenate([kv_on.astype(jnp.int32), qd_on.astype(jnp.int32), base[None]]).astype(jnp.int32)
            delta_loc = jnp.einsum("shd,shd->sh", do_loc, o_loc, preferred_element_type=jnp.float32)
            stat = jnp.concatenate([lse_loc.T, delta_loc.T])
            qd = jnp.stack([q_loc, do_loc]).transpose(0, 2, 1, 3)
            kv = jnp.stack([k_loc, v_loc]).transpose(0, 2, 1, 3)
            win_shapes = (jax.ShapeDtypeStruct((2 * REACH,) + qd.shape, qd.dtype), jax.ShapeDtypeStruct((REACH,) + stat.shape, stat.dtype))
            win, swin = pl.pallas_call(functools.partial(far_kernel, n_dev), out_shape=win_shapes, in_specs=[any_spec] * 3, out_specs=(any_spec, any_spec),
                                       scratch_shapes=[dma((REACH,))] * 6,
                                       compiler_params=pltpu.CompilerParams(collective_id=1, has_side_effects=True), name="wide_exchange")(kv, qd, stat)
            head_blk = lambda h, flag: (0, h, 0, 0)
            full2 = lambda h, flag: (0, 0)
            out_blk = pl.BlockSpec((1, n_tok, head_dim), lambda h, flag: (h, 0, 0))
            out_one = jax.ShapeDtypeStruct((n_heads, n_tok, head_dim), jnp.bfloat16)
            dq, dk, dv = pl.pallas_call(
                functools.partial(grad_kernel, score_scale),
                grid_spec=pltpu.PrefetchScalarGridSpec(
                    num_scalar_prefetch=1, grid=(n_heads,),
                    in_specs=[pl.BlockSpec((2, 1, n_tok, head_dim), head_blk), pl.BlockSpec((2, 1, n_tok, head_dim), head_blk),
                              pl.BlockSpec((2 * REACH, 2, 1, n_tok, head_dim), lambda h, flag: (0, 0, h, 0, 0)),
                              pl.BlockSpec(stat.shape, full2), pl.BlockSpec((REACH,) + stat.shape, lambda h, flag: (0, 0, 0)),
                              pl.BlockSpec((REACH + 1, n_tok), full2)],
                    out_specs=[out_blk] * 3,
                    scratch_shapes=[pltpu.VMEM((n_tok, head_dim), jnp.float32)] * 3),
                out_shape=(out_one, out_one, out_one), name="grads",
            )(flags, qd, kv, win, stat, swin, start_rows)
            return tuple(item.transpose(1, 0, 2) for item in (dq, dk, dv))

        def near(q_loc, k_loc, v_loc, o_loc, do_loc, lse_loc, cu_seqlens):
            out_one = jax.ShapeDtypeStruct(q_loc.shape, q_loc.dtype)
            bf16, f32 = jnp.bfloat16, jnp.float32
            return pl.pallas_call(
                functools.partial(near_kernel, n_dev, score_scale),
                out_shape=(out_one, out_one, out_one),
                in_specs=[smem_spec] + [any_spec] * 5 + [vmem_spec], out_specs=(any_spec,) * 3,
                scratch_shapes=[pltpu.VMEM((n_heads // TILE_HEADS, 4, n_tok, TILE_HEADS, head_dim), bf16), pltpu.VMEM(q_loc.shape, bf16)]
                + [pltpu.VMEM(pair_shape, bf16)] * 3 + [pltpu.VMEM((5,) + pair_shape, bf16)]
                + [pltpu.VMEM((2 * n_heads, n_tok), f32), pltpu.VMEM((REACH, 2 * n_heads, n_tok), f32), pltpu.VMEM((8, n_tok), jnp.int32)]
                + [pltpu.VMEM((3, TILE_HEADS, n_tok, head_dim), bf16)] + [pltpu.VMEM((n_tok, head_dim), f32)] * 3
                + [dma((n_heads // TILE_HEADS, ROW_PARTS, 4)), dma, dma((n_heads // TILE_HEADS, 3)), dma((REACH,)), dma((REACH,)), dma((n_heads,)), dma((n_heads,))]
                + [dma((n_heads, ROW_PARTS))] * 8,
                compiler_params=pltpu.CompilerParams(collective_id=0, has_side_effects=True), name="near_grads",
            )(cu_seqlens, q_loc, k_loc, v_loc, o_loc, do_loc, lse_loc.T)

        chip_pos = jnp.arange(1, n_dev // 2 - 1, dtype=jnp.int32)[:, None] * 2 * n_tok
        far = jnp.any((cu_seqlens[None, :-1] < chip_pos) & (cu_seqlens[None, 1:] > chip_pos + 2 * n_tok))
        return lax.cond(far, wide, near, q_loc, k_loc, v_loc, o_loc, do_loc, lse_loc, cu_seqlens)

    return jax.shard_map(device_fn, mesh=mesh, in_specs=(head_spec, head_spec, head_spec, head_spec, head_spec, row_spec, P()), out_specs=(head_spec, head_spec, head_spec), check_vma=False)
```

```python
import functools

import jax
import jax.numpy as jnp
from jax import lax
from jax.experimental import pallas as pl
from jax.experimental.pallas import tpu as pltpu
from jax.sharding import PartitionSpec as P

REACH = 3
TILE_HEADS = 8
ROW_PARTS = 2
HEADS_AHEAD = 1
LOG2E = 1.4426950408889634
MESH_ID = pl.DeviceIdType.MESH


def to_dev(idx):
    return {"cp": idx}


def greet_all(n_dev, me):
    barrier = pltpu.get_barrier_semaphore()
    for step in range(1, n_dev):
        pl.semaphore_signal(barrier, inc=1, device_id=to_dev(lax.rem(me + step, n_dev)), device_id_type=MESH_ID)


def await_all(n_dev):
    pl.semaphore_wait(pltpu.get_barrier_semaphore(), n_dev - 1)


def stat_copies(me, n_dev, stat_ref, swin_ref, send_sem, recv_sem):
    out = []
    for dist in range(1, REACH + 1):
        copy = pltpu.make_async_remote_copy(src_ref=stat_ref, dst_ref=swin_ref.at[dist - 1], send_sem=send_sem.at[dist - 1], recv_sem=recv_sem.at[dist - 1], device_id=to_dev(lax.rem(me + n_dev - dist, n_dev)), device_id_type=MESH_ID)
        out.append((dist, copy))
    return out


def nt_dot(a, b):
    return lax.dot_general(a, b, (((1,), (1,)), ((), ())), preferred_element_type=jnp.float32)


def nn_dot(a, b):
    return lax.dot_general(a, b, (((1,), (0,)), ((), ())), preferred_element_type=jnp.float32)


def tn_dot(a, b):
    return lax.dot_general(a, b, (((0,), (0,)), ((), ())), preferred_element_type=jnp.float32)


def block_terms(score_scale, k_blk, v_blk, q_blk, do_blk, lse_row, delta_row, start_row, k_base, q_base):
    s_t = nt_dot(k_blk, q_blk)
    dp_t = nt_dot(v_blk, do_blk)
    k_pos = k_base + lax.broadcasted_iota(jnp.int32, s_t.shape, 0)
    q_pos = q_base + lax.broadcasted_iota(jnp.int32, s_t.shape, 1)
    keep = (k_pos >= start_row) & (k_pos <= q_pos)
    p_t = jnp.where(keep, jnp.exp2(s_t * (score_scale * LOG2E) - lse_row * LOG2E), 0.0)
    ds_t = (p_t * (dp_t - delta_row)).astype(jnp.bfloat16)
    return p_t.astype(jnp.bfloat16), ds_t


def swap_kernel(n_dev, pairs, *refs):
    me = lax.axis_index("cp")
    views = pairs(refs[:-3])
    s_sem, r_sem, l_sem = refs[-3:]
    greet_all(n_dev, me)
    await_all(n_dev)

    def copies(mask):
        peer = me ^ mask
        return [pltpu.make_async_remote_copy(src_ref=src(peer), dst_ref=dst(me), send_sem=s_sem.at[n, mask], recv_sem=r_sem.at[n, mask], device_id=to_dev(peer), device_id_type=MESH_ID)
                for n, (src, dst) in enumerate(views)]

    order = [2, 4, 6, 3, 5, 7, 1]
    for mask in order:
        for copy in copies(mask):
            copy.start()
    for n, (src, dst) in enumerate(views):
        pltpu.make_async_copy(src(me), dst(me), l_sem.at[n]).start()
    for n, (src, dst) in enumerate(views):
        pltpu.make_async_copy(src(me), dst(me), l_sem.at[n]).wait()
    for mask in order:
        for copy in copies(mask):
            copy.wait()


def head_kernel(score_scale, start_ref, got_ref, gstat_ref, rows_ref, out_ref, dq_acc, dk_acc, dv_acc):
    head = pl.program_id(0)
    n_dev, _, _, n_tok, _ = got_ref.shape
    terms = functools.partial(block_terms, score_scale)

    def shard(i, carry):
        q_blk, do_blk = got_ref[i, 0, 0], got_ref[i, 3, 0]
        lse_row, delta_row = gstat_ref[i, pl.ds(head, 1), :], gstat_ref[i, pl.ds(2 + head, 1), :]
        start_row = rows_ref[pl.ds(i, 1), :]

        def pair(j, first):
            k_blk, v_blk = got_ref[j, 1, 0], got_ref[j, 2, 0]
            p_t, ds_t = terms(k_blk, v_blk, q_blk, do_blk, lse_row, delta_row, start_row, j * n_tok, i * n_tok)
            dv, dk, dq = nn_dot(p_t, do_blk), nn_dot(ds_t, q_blk), tn_dot(ds_t, k_blk)
            if first:
                dv_acc[j], dk_acc[j], dq_acc[i] = dv, dk, dq
            else:
                dv_acc[j] += dv
                dk_acc[j] += dk
                dq_acc[i] += dq

        pair(i, True)
        lowest = start_ref[i] // n_tok
        lax.fori_loop(lowest, i, lambda j, c: (pair(j, False), c)[1], 0)
        return carry

    lax.fori_loop(0, n_dev, shard, 0)

    def write(i, carry):
        out_ref[i, 0, 0] = (dq_acc[i] * score_scale).astype(out_ref.dtype)
        out_ref[i, 1, 0] = (dk_acc[i] * score_scale).astype(out_ref.dtype)
        out_ref[i, 2, 0] = dv_acc[i].astype(out_ref.dtype)
        return carry

    lax.fori_loop(0, n_dev, write, 0)


def near_kernel(n_dev, score_scale, cu_ref, q_ref, k_ref, v_ref, o_ref, do_ref, lse_ref, dq_ref, dk_ref, dv_ref,
                raw, raw_o, qd, kv, pk, win, stat, swin, starts, out_hm, dq_acc, dk_acc, dv_acc,
                ld_sem, o_sem, out_sem, st_s, st_r, own_s, own_r, x_s, x_r, y_s, y_r, fx_s, fx_r, fy_s, fy_r):
    me = lax.axis_index("cp")
    core = lax.rem(me, 2)
    chip = me // 2
    chip_odd = lax.rem(chip, 2)
    n_tok, n_heads, _ = q_ref.shape
    part = n_tok // ROW_PARTS
    base = me * n_tok
    first_chip, last_chip = chip == 0, chip == n_dev // 2 - 1
    not_first, not_last = jnp.logical_not(first_chip), jnp.logical_not(last_chip)
    relays = first_chip | last_chip
    middle = jnp.logical_not(relays)
    x_dev, y_dev, mate = me + 2 - 4 * chip_odd, lax.rem(me + 4, n_dev), me + 1 - 2 * core
    x_dst = 1 + 2 * chip_odd
    x_slot = 3 - 2 * chip_odd
    y_slot = 4 - x_slot

    def remote(src, dst, s_sem, r_sem, dev):
        return pltpu.make_async_remote_copy(src_ref=src, dst_ref=dst, send_sem=s_sem, recv_sem=r_sem, device_id=to_dev(dev), device_id_type=MESH_ID)

    def block(slot, h, r):
        return win.at[slot, :, h, pl.ds(r * part, part)]

    def x_copy(h, r):
        return remote(pk.at[:, h, pl.ds(r * part, part)], block(x_dst, h, r), x_s.at[h, r], x_r.at[h, r], x_dev)

    def y_copy(h, r):
        return remote(block(x_slot, h, r), block(y_slot, h, r), y_s.at[h, r], y_r.at[h, r], y_dev)

    def fx_copy(h, r):
        return remote(block(x_slot, h, r), block(4 - 2 * core - 2 * chip_odd, h, r), fx_s.at[h, r], fx_r.at[h, r], mate)

    def fy_copy(h, r):
        return remote(block(y_slot, h, r), block(2 - 2 * core + 2 * chip_odd, h, r), fy_s.at[h, r], fy_r.at[h, r], mate)

    def own_kv(h):
        return remote(kv.at[:, h], win.at[0, :, h], own_s.at[h], own_r.at[h], mate)

    def own_qd(h):
        return remote(qd.at[:, h], win.at[4, :, h], own_s.at[h], own_r.at[h], mate)

    halves = n_heads // TILE_HEADS
    units = [(half, r) for half in range(halves) for r in range(ROW_PARTS)]

    def load(half, r, which):
        src = (q_ref, k_ref, do_ref, v_ref)[which]
        rows, heads = pl.ds(r * part, part), pl.ds(half * TILE_HEADS, TILE_HEADS)
        return pltpu.make_async_copy(src.at[rows, heads], raw.at[half, which, rows], ld_sem.at[half, r, which])

    greet_all(n_dev, me)
    for half, r in units:
        for which in range(4):
            load(half, r, which).start()
    load_o = pltpu.make_async_copy(o_ref, raw_o, o_sem)
    load_o.start()

    chip_pos = chip * 2 * n_tok
    pos = base + n_tok * lax.broadcasted_iota(jnp.int32, starts.shape, 0) + lax.broadcasted_iota(jnp.int32, starts.shape, 1)

    def scan_docs(n, carry):
        found, cross_end = carry
        first, last = cu_ref[n], cu_ref[n + 1]
        crosses = (first < chip_pos) & (last > chip_pos)
        return jnp.where(first <= pos, jnp.maximum(found, first), found), jnp.where(crosses, last, cross_end)

    found, cross_end = lax.fori_loop(0, cu_ref.shape[0] - 1, scan_docs, (jnp.zeros(starts.shape, jnp.int32), 0))
    starts[...] = jnp.where(pos < n_dev * n_tok, found, n_dev * n_tok)
    send_rows = jnp.clip(cross_end - base, 0, n_tok)
    row_ids = lax.broadcasted_iota(jnp.int32, (TILE_HEADS, part, q_ref.shape[2]), 1)
    stats = stat_copies(me, n_dev, stat, swin, st_s, st_r)

    def arrange(half, r):
        rows, heads = pl.ds(r * part, part), pl.ds(half * TILE_HEADS, TILE_HEADS)
        for pair in range(2):
            load(half, r, 2 * pair).wait()
            load(half, r, 2 * pair + 1).wait()
            q_side = jnp.swapaxes(raw[half, 2 * pair, rows], 0, 1)
            k_side = jnp.swapaxes(raw[half, 2 * pair + 1, rows], 0, 1)
            pk[pair, heads, rows] = jnp.where(row_ids < send_rows - r * part, q_side, k_side)
            qd[pair, heads, rows] = q_side
            kv[pair, heads, rows] = k_side

    def start_own(half):
        for h in range(half * TILE_HEADS, (half + 1) * TILE_HEADS):
            pl.when(core == 0)(own_kv(h).start)
            pl.when(core == 1)(own_qd(h).start)

    for r in range(ROW_PARTS):
        arrange(0, r)
        if r == 0:
            await_all(n_dev)
        x_copy(0, r).start()
    start_own(0)
    for half in range(1, halves):
        for r in range(ROW_PARTS):
            arrange(half, r)
        start_own(half)
    load_o.wait()
    stat[0:n_heads, :] = lse_ref[...]
    for half in range(halves):
        delta = jnp.sum(raw[half, 2].astype(jnp.float32) * raw_o[:, half * TILE_HEADS:(half + 1) * TILE_HEADS, :].astype(jnp.float32), axis=-1)
        stat[n_heads + half * TILE_HEADS:n_heads + (half + 1) * TILE_HEADS, :] = delta.T
    for dist, copy in stats:
        pl.when(me >= dist)(copy.start)

    terms = functools.partial(block_terms, score_scale)

    def arrive(h):
        for r in range(ROW_PARTS):
            pl.when(h + HEADS_AHEAD < n_heads)(lambda: x_copy(h + HEADS_AHEAD, r).start())
            x_copy(h, r).wait_recv()
            pl.when(relays)(lambda: y_copy(h, r).start())
            fx_copy(h, r).start()

    def arrive_y(h):
        for r in range(ROW_PARTS):
            y_copy(h, r).wait_recv()
            fy_copy(h, r).start()

    def compute(h):
        own_qd(h).wait_recv()
        for r in range(ROW_PARTS):
            fx_copy(h, r).wait_recv()

        @pl.when(middle)
        def _():
            for r in range(ROW_PARTS):
                fy_copy(h, r).wait_recv()

        q_blk, do_blk, k_blk, v_blk = qd[0, h], qd[1, h], kv[0, h], kv[1, h]
        lse_own, delta_own = stat[pl.ds(h, 1), :], stat[pl.ds(n_heads + h, 1), :]
        p_t, ds_t = terms(k_blk, v_blk, q_blk, do_blk, lse_own, delta_own, starts[0:1, :], base, base)
        dv_acc[...] = nn_dot(p_t, do_blk)
        dk_acc[...] = nn_dot(ds_t, q_blk)
        dq_acc[...] = tn_dot(ds_t, k_blk)
        for dist in range(1, REACH + 1):
            k_here = {1: (core == 1) | not_first, 2: not_first, 3: (core == 1) & not_first}[dist]
            q_here = {1: (core == 0) | not_last, 2: not_last, 3: (core == 0) & not_last}[dist]

            @pl.when(k_here)
            def _():
                k_far, v_far = win[dist - 1, 0, h], win[dist - 1, 1, h]
                _, ds_far = terms(k_far, v_far, q_blk, do_blk, lse_own, delta_own, starts[0:1, :], base - dist * n_tok, base)
                dq_acc[...] += tn_dot(ds_far, k_far)

            @pl.when(q_here)
            def _():
                q_far, do_far = win[5 - dist, 0, h], win[5 - dist, 1, h]
                lse_far = swin[dist - 1, pl.ds(h, 1), :]
                delta_far = swin[dist - 1, pl.ds(n_heads + h, 1), :]
                p_far, ds_far = terms(k_blk, v_blk, q_far, do_far, lse_far, delta_far, starts[dist:dist + 1, :], base, base + dist * n_tok)
                dv_acc[...] += nn_dot(p_far, do_far)
                dk_acc[...] += nn_dot(ds_far, q_far)

        h_in = lax.rem(h, TILE_HEADS)
        out_hm[0, h_in] = (dq_acc[...] * score_scale).astype(out_hm.dtype)
        out_hm[1, h_in] = (dk_acc[...] * score_scale).astype(out_hm.dtype)
        out_hm[2, h_in] = dv_acc[...].astype(out_hm.dtype)

    def out_copy(half, which):
        dst = (dq_ref, dk_ref, dv_ref)[which]
        rows = pl.ds(half * TILE_HEADS, TILE_HEADS)
        return pltpu.make_async_copy(raw.at[half, which], dst.at[:, rows], out_sem.at[half, which])

    def step(t, carry):
        pl.when(t < n_heads)(lambda: arrive(t))

        @pl.when(t == 2)
        def _():
            for dist, copy in stats:
                pl.when(me + dist < n_dev)(copy.wait_recv)

        pl.when(t >= 2)(lambda: compute(t - 2))
        for half in range(halves):
            @pl.when(t - 2 == (half + 1) * TILE_HEADS - 1)
            def _():
                for which in range(3):
                    raw[half, which] = jnp.swapaxes(out_hm[which], 0, 1)
                for which in range(3):
                    out_copy(half, which).start()
        pl.when((t >= 1) & (t <= n_heads) & middle)(lambda: arrive_y(t - 1))
        return carry

    lax.fori_loop(0, n_heads + 2, step, 0)

    def drain(h, carry):
        own_kv(h).wait_send()
        for r in range(ROW_PARTS):
            x_copy(h, r).wait_send()
            fx_copy(h, r).wait_send()
            pl.when(relays)(lambda: y_copy(h, r).wait_send())
            pl.when(middle)(lambda: fy_copy(h, r).wait_send())
        return carry

    lax.fori_loop(0, n_heads, drain, 0)
    for dist, copy in stats:
        pl.when(me >= dist)(copy.wait_send)
    for half in range(halves):
        for which in range(3):
            out_copy(half, which).wait()


def solution(mesh):
    n_dev = mesh.shape["cp"]
    head_spec = P("cp", "hp", None)
    row_spec = P("cp", "hp")
    any_spec = pl.BlockSpec(memory_space=pl.ANY)
    vmem_spec = pl.BlockSpec(memory_space=pltpu.VMEM)
    smem_spec = pl.BlockSpec(memory_space=pltpu.SMEM)
    dma = pltpu.SemaphoreType.DMA

    def device_fn(q_loc, k_loc, v_loc, o_loc, do_loc, lse_loc, cu_seqlens):
        n_tok, n_heads, head_dim = q_loc.shape
        seq_len = n_tok * n_dev
        score_scale = head_dim ** -0.5
        pair_shape = (2, n_heads, n_tok, head_dim)

        def wide(q_loc, k_loc, v_loc, o_loc, do_loc, lse_loc, cu_seqlens):
            bf16, f32 = jnp.bfloat16, jnp.float32
            per = n_heads // n_dev
            pos = jnp.arange(seq_len, dtype=jnp.int32).reshape(n_dev, n_tok)
            start_rows = jnp.max(jnp.where(cu_seqlens <= pos[..., None], cu_seqlens, 0), axis=-1)
            delta_loc = jnp.einsum("shd,shd->hs", do_loc, o_loc, preferred_element_type=f32)
            parts = [item.reshape(n_dev, per, n_tok) for item in (lse_loc.T, delta_loc)]
            stat = jnp.concatenate(parts + [jnp.zeros((n_dev, 8 - 2 * per, n_tok), f32)], axis=1)
            ops = jnp.stack([q_loc, k_loc, v_loc, do_loc]).transpose(0, 2, 1, 3)

            def heads_of(dev):
                return pl.ds(dev * per, per)

            def call(pairs, n_pairs, ident, out_shape, *args):
                return pl.pallas_call(functools.partial(swap_kernel, n_dev, pairs), out_shape=out_shape,
                                      in_specs=[any_spec] * len(args), out_specs=[any_spec] * len(out_shape),
                                      scratch_shapes=[dma((n_pairs, n_dev)), dma((n_pairs, n_dev)), dma((n_pairs,))],
                                      compiler_params=pltpu.CompilerParams(collective_id=ident, has_side_effects=True))(*args)

            def in_pairs(refs):
                ops_ref, stat_ref, got_ref, gstat_ref = refs
                return [(lambda d: ops_ref.at[:, heads_of(d)], lambda d: got_ref.at[d]), (lambda d: stat_ref.at[d], lambda d: gstat_ref.at[d])]

            def out_pairs(refs):
                grad_ref, back_ref = refs
                return [(lambda d: grad_ref.at[d], lambda d: back_ref.at[:, heads_of(d)])]

            got, gstat = call(in_pairs, 2, 1, (jax.ShapeDtypeStruct((n_dev, 4, per, n_tok, head_dim), bf16), jax.ShapeDtypeStruct((n_dev, 8, n_tok), f32)), ops, stat)
            grads = pl.pallas_call(
                functools.partial(head_kernel, score_scale),
                grid_spec=pltpu.PrefetchScalarGridSpec(
                    num_scalar_prefetch=1, grid=(per,),
                    in_specs=[pl.BlockSpec((n_dev, 4, 1, n_tok, head_dim), lambda h, s: (0, 0, h, 0, 0)), pl.BlockSpec((n_dev, 8, n_tok), lambda h, s: (0, 0, 0)), pl.BlockSpec((n_dev, n_tok), lambda h, s: (0, 0))],
                    out_specs=pl.BlockSpec((n_dev, 3, 1, n_tok, head_dim), lambda h, s: (0, 0, h, 0, 0)),
                    scratch_shapes=[pltpu.VMEM((n_dev, n_tok, head_dim), f32)] * 3),
                out_shape=jax.ShapeDtypeStruct((n_dev, 3, per, n_tok, head_dim), bf16), name="head_grads",
            )(start_rows[:, 0], got, gstat, start_rows)
            back, = call(out_pairs, 1, 2, (jax.ShapeDtypeStruct((3, n_heads, n_tok, head_dim), bf16),), grads)
            return tuple(back[n].transpose(1, 0, 2) for n in range(3))

        def near(q_loc, k_loc, v_loc, o_loc, do_loc, lse_loc, cu_seqlens):
            out_one = jax.ShapeDtypeStruct(q_loc.shape, q_loc.dtype)
            bf16, f32 = jnp.bfloat16, jnp.float32
            return pl.pallas_call(
                functools.partial(near_kernel, n_dev, score_scale),
                out_shape=(out_one, out_one, out_one),
                in_specs=[smem_spec] + [any_spec] * 5 + [vmem_spec], out_specs=(any_spec,) * 3,
                scratch_shapes=[pltpu.VMEM((n_heads // TILE_HEADS, 4, n_tok, TILE_HEADS, head_dim), bf16), pltpu.VMEM(q_loc.shape, bf16)]
                + [pltpu.VMEM(pair_shape, bf16)] * 3 + [pltpu.VMEM((5,) + pair_shape, bf16)]
                + [pltpu.VMEM((2 * n_heads, n_tok), f32), pltpu.VMEM((REACH, 2 * n_heads, n_tok), f32), pltpu.VMEM((8, n_tok), jnp.int32)]
                + [pltpu.VMEM((3, TILE_HEADS, n_tok, head_dim), bf16)] + [pltpu.VMEM((n_tok, head_dim), f32)] * 3
                + [dma((n_heads // TILE_HEADS, ROW_PARTS, 4)), dma, dma((n_heads // TILE_HEADS, 3)), dma((REACH,)), dma((REACH,)), dma((n_heads,)), dma((n_heads,))]
                + [dma((n_heads, ROW_PARTS))] * 8,
                compiler_params=pltpu.CompilerParams(collective_id=0, has_side_effects=True), name="near_grads",
            )(cu_seqlens, q_loc, k_loc, v_loc, o_loc, do_loc, lse_loc.T)

        chip_pos = jnp.arange(1, n_dev // 2 - 1, dtype=jnp.int32)[:, None] * 2 * n_tok
        cuts = (cu_seqlens[None] >= chip_pos) & (cu_seqlens[None] <= chip_pos + 2 * n_tok)
        far = jnp.logical_not(jnp.all(jnp.any(cuts, axis=1)))
        return lax.cond(far, wide, near, q_loc, k_loc, v_loc, o_loc, do_loc, lse_loc, cu_seqlens)

    return jax.shard_map(device_fn, mesh=mesh, in_specs=(head_spec, head_spec, head_spec, head_spec, head_spec, row_spec, P()), out_specs=(head_spec, head_spec, head_spec), check_vma=False)
```

```python
import functools

import jax
import jax.numpy as jnp
from jax import lax
from jax.experimental import pallas as pl
from jax.experimental.pallas import tpu as pltpu
from jax.sharding import PartitionSpec as P

REACH = 3
TILE_HEADS = 8
ROW_PARTS = 2
IN_FLIGHT = 4
OUT_STEPS = 2
LOG2E = 1.4426950408889634
MESH_ID = pl.DeviceIdType.MESH


def to_dev(idx):
    return {"cp": idx}


def greet_all(n_dev, me):
    barrier = pltpu.get_barrier_semaphore()
    for step in range(1, n_dev):
        pl.semaphore_signal(barrier, inc=1, device_id=to_dev(lax.rem(me + step, n_dev)), device_id_type=MESH_ID)


def await_all(n_dev):
    pl.semaphore_wait(pltpu.get_barrier_semaphore(), n_dev - 1)


def stat_copies(me, n_dev, stat_ref, swin_ref, send_sem, recv_sem):
    out = []
    for dist in range(1, REACH + 1):
        copy = pltpu.make_async_remote_copy(src_ref=stat_ref, dst_ref=swin_ref.at[dist - 1], send_sem=send_sem.at[dist - 1], recv_sem=recv_sem.at[dist - 1], device_id=to_dev(lax.rem(me + n_dev - dist, n_dev)), device_id_type=MESH_ID)
        out.append((dist, copy))
    return out


def nt_dot(a, b):
    return lax.dot_general(a, b, (((1,), (1,)), ((), ())), preferred_element_type=jnp.float32)


def nn_dot(a, b):
    return lax.dot_general(a, b, (((1,), (0,)), ((), ())), preferred_element_type=jnp.float32)


def tn_dot(a, b):
    return lax.dot_general(a, b, (((0,), (0,)), ((), ())), preferred_element_type=jnp.float32)


def block_terms(score_scale, k_blk, v_blk, q_blk, do_blk, lse_row, delta_row, start_row, k_base, q_base):
    s_t = nt_dot(k_blk, q_blk)
    dp_t = nt_dot(v_blk, do_blk)
    k_pos = k_base + lax.broadcasted_iota(jnp.int32, s_t.shape, 0)
    q_pos = q_base + lax.broadcasted_iota(jnp.int32, s_t.shape, 1)
    keep = (k_pos >= start_row) & (k_pos <= q_pos)
    p_t = jnp.where(keep, jnp.exp2(s_t * (score_scale * LOG2E) - lse_row * LOG2E), 0.0)
    ds_t = (p_t * (dp_t - delta_row)).astype(jnp.bfloat16)
    return p_t.astype(jnp.bfloat16), ds_t


def swap_kernel(n_dev, pairs, *refs):
    me = lax.axis_index("cp")
    views = pairs(refs[:-3])
    s_sem, r_sem, l_sem = refs[-3:]
    greet_all(n_dev, me)
    await_all(n_dev)

    def copies(mask):
        peer = me ^ mask
        return [pltpu.make_async_remote_copy(src_ref=src(peer), dst_ref=dst(me), send_sem=s_sem.at[n, mask], recv_sem=r_sem.at[n, mask], device_id=to_dev(peer), device_id_type=MESH_ID)
                for n, (src, dst) in enumerate(views)]

    order = [2, 4, 6, 3, 5, 7, 1]
    for mask in order:
        for copy in copies(mask):
            copy.start()
    for n, (src, dst) in enumerate(views):
        pltpu.make_async_copy(src(me), dst(me), l_sem.at[n]).start()
    for n, (src, dst) in enumerate(views):
        pltpu.make_async_copy(src(me), dst(me), l_sem.at[n]).wait()
    for mask in order:
        for copy in copies(mask):
            copy.wait()


def head_kernel(score_scale, start_ref, got_ref, gstat_ref, rows_ref, out_ref, dq_acc, dk_acc, dv_acc):
    head = pl.program_id(0)
    n_dev, _, _, n_tok, _ = got_ref.shape
    terms = functools.partial(block_terms, score_scale)

    def shard(i, carry):
        q_blk, do_blk = got_ref[i, 0, 0], got_ref[i, 3, 0]
        lse_row, delta_row = gstat_ref[i, pl.ds(head, 1), :], gstat_ref[i, pl.ds(2 + head, 1), :]
        start_row = rows_ref[pl.ds(i, 1), :]

        def pair(j, first):
            k_blk, v_blk = got_ref[j, 1, 0], got_ref[j, 2, 0]
            p_t, ds_t = terms(k_blk, v_blk, q_blk, do_blk, lse_row, delta_row, start_row, j * n_tok, i * n_tok)
            dv, dk, dq = nn_dot(p_t, do_blk), nn_dot(ds_t, q_blk), tn_dot(ds_t, k_blk)
            if first:
                dv_acc[j], dk_acc[j], dq_acc[i] = dv, dk, dq
            else:
                dv_acc[j] += dv
                dk_acc[j] += dk
                dq_acc[i] += dq

        pair(i, True)
        lowest = start_ref[i] // n_tok
        lax.fori_loop(lowest, i, lambda j, c: (pair(j, False), c)[1], 0)
        return carry

    lax.fori_loop(0, n_dev, shard, 0)

    def write(i, carry):
        out_ref[i, 0, 0] = (dq_acc[i] * score_scale).astype(out_ref.dtype)
        out_ref[i, 1, 0] = (dk_acc[i] * score_scale).astype(out_ref.dtype)
        out_ref[i, 2, 0] = dv_acc[i].astype(out_ref.dtype)
        return carry

    lax.fori_loop(0, n_dev, write, 0)


def near_kernel(n_dev, score_scale, cu_ref, q_ref, k_ref, v_ref, o_ref, do_ref, lse_ref, dq_ref, dk_ref, dv_ref,
                raw, raw_o, qd, kv, pk, win, stat, swin, starts, out_buf, dq_acc, dk_acc, dv_acc,
                ld_sem, o_sem, out_sem, st_s, st_r, own_s, own_r, x_s, x_r, y_s, y_r, fx_s, fx_r, fy_s, fy_r):
    me = lax.axis_index("cp")
    core = lax.rem(me, 2)
    chip = me // 2
    chip_odd = lax.rem(chip, 2)
    n_tok, n_heads, _ = q_ref.shape
    part = n_tok // ROW_PARTS
    base = me * n_tok
    first_chip, last_chip = chip == 0, chip == n_dev // 2 - 1
    not_first, not_last = jnp.logical_not(first_chip), jnp.logical_not(last_chip)
    relays = first_chip | last_chip
    middle = jnp.logical_not(relays)
    x_dev, y_dev, mate = me + 2 - 4 * chip_odd, lax.rem(me + 4, n_dev), me + 1 - 2 * core
    x_dst = 1 + 2 * chip_odd
    x_slot = 3 - 2 * chip_odd
    y_slot = 4 - x_slot

    def remote(src, dst, s_sem, r_sem, dev):
        return pltpu.make_async_remote_copy(src_ref=src, dst_ref=dst, send_sem=s_sem, recv_sem=r_sem, device_id=to_dev(dev), device_id_type=MESH_ID)

    def block(slot, h, r):
        return win.at[slot, :, h, pl.ds(r * part, part)]

    def x_copy(h, r):
        return remote(pk.at[:, h, pl.ds(r * part, part)], block(x_dst, h, r), x_s.at[h, r], x_r.at[h, r], x_dev)

    def y_copy(h, r):
        return remote(block(x_slot, h, r), block(y_slot, h, r), y_s.at[h, r], y_r.at[h, r], y_dev)

    def fx_copy(h):
        return remote(win.at[x_slot, :, h], win.at[4 - 2 * core - 2 * chip_odd, :, h], fx_s.at[h], fx_r.at[h], mate)

    def fy_copy(h):
        return remote(win.at[y_slot, :, h], win.at[2 - 2 * core + 2 * chip_odd, :, h], fy_s.at[h], fy_r.at[h], mate)

    def own_kv(h):
        return remote(kv.at[:, h], win.at[0, :, h], own_s.at[h], own_r.at[h], mate)

    def own_qd(h):
        return remote(qd.at[:, h], win.at[4, :, h], own_s.at[h], own_r.at[h], mate)

    halves = n_heads // TILE_HEADS
    units = [(half, r) for half in range(halves) for r in range(ROW_PARTS)]

    def load(half, r, which):
        src = (q_ref, k_ref, do_ref, v_ref)[which]
        rows, heads = pl.ds(r * part, part), pl.ds(half * TILE_HEADS, TILE_HEADS)
        return pltpu.make_async_copy(src.at[rows, heads], raw.at[half, which, rows], ld_sem.at[half, r, which])

    greet_all(n_dev, me)
    for half, r in units:
        for which in range(4):
            load(half, r, which).start()
    load_o = pltpu.make_async_copy(o_ref, raw_o, o_sem)
    load_o.start()

    chip_pos = chip * 2 * n_tok

    def scan_cross(n, cross_end):
        return jnp.where((cu_ref[n] < chip_pos) & (cu_ref[n + 1] > chip_pos), cu_ref[n + 1], cross_end)

    n_docs = cu_ref.shape[0] - 1
    send_rows = lax.fori_loop(0, n_docs, scan_cross, 0, unroll=True) - base

    def find_starts():
        pos = base + n_tok * lax.broadcasted_iota(jnp.int32, starts.shape, 0) + lax.broadcasted_iota(jnp.int32, starts.shape, 1)

        def scan_docs(n, found):
            return jnp.where(cu_ref[n] <= pos, jnp.maximum(found, cu_ref[n]), found)

        found = lax.fori_loop(0, n_docs, scan_docs, jnp.zeros(starts.shape, jnp.int32))
        starts[...] = jnp.where(pos < n_dev * n_tok, found, n_dev * n_tok)

    row_ids = lax.broadcasted_iota(jnp.int32, (TILE_HEADS, part, q_ref.shape[2]), 1)
    stats = stat_copies(me, n_dev, stat, swin, st_s, st_r)

    def arrange(half, r):
        rows, heads = pl.ds(r * part, part), pl.ds(half * TILE_HEADS, TILE_HEADS)
        for pair in range(2):
            load(half, r, 2 * pair).wait()
            load(half, r, 2 * pair + 1).wait()
            q_side = jnp.swapaxes(raw[half, 2 * pair, rows], 0, 1)
            k_side = jnp.swapaxes(raw[half, 2 * pair + 1, rows], 0, 1)
            pk[pair, heads, rows] = jnp.where(row_ids < send_rows - r * part, q_side, k_side)
            qd[pair, heads, rows] = q_side
            kv[pair, heads, rows] = k_side

    def start_own(half):
        for h in range(half * TILE_HEADS, (half + 1) * TILE_HEADS):
            pl.when(core == 0)(own_kv(h).start)
            pl.when(core == 1)(own_qd(h).start)

    for r in range(ROW_PARTS):
        arrange(0, r)
        if r == 0:
            await_all(n_dev)
        x_copy(0, r).start()
    start_own(0)
    for half in range(1, halves):
        for r in range(ROW_PARTS):
            arrange(half, r)
        start_own(half)
    find_starts()
    load_o.wait()
    stat[0:n_heads, :] = lse_ref[...]
    for half in range(halves):
        delta = jnp.sum(raw[half, 2].astype(jnp.float32) * raw_o[:, half * TILE_HEADS:(half + 1) * TILE_HEADS, :].astype(jnp.float32), axis=-1)
        stat[n_heads + half * TILE_HEADS:n_heads + (half + 1) * TILE_HEADS, :] = delta.T
    for dist, copy in stats:
        pl.when(me >= dist)(copy.start)

    terms = functools.partial(block_terms, score_scale)

    def arrive(h):
        for r in range(ROW_PARTS):
            x_copy(h, r).wait_recv()
            pl.when(relays)(lambda: y_copy(h, r).start())
            pl.when(h + 1 < n_heads)(lambda: x_copy(h + 1, r).start())
        fx_copy(h).start()

    def arrive_y(h):
        for r in range(ROW_PARTS):
            y_copy(h, r).wait_recv()
        fy_copy(h).start()

    def mine(h):
        return qd[0, h], qd[1, h], kv[0, h], kv[1, h]

    def key_block(h, slot):
        q_blk, do_blk, _, _ = mine(h)
        k_far, v_far = win[slot, 0, h], win[slot, 1, h]
        _, ds_far = terms(k_far, v_far, q_blk, do_blk, stat[pl.ds(h, 1), :], stat[pl.ds(n_heads + h, 1), :], starts[0:1, :], base - (slot + 1) * n_tok, base)
        return tn_dot(ds_far, k_far)

    def query_block(h, slot):
        _, _, k_blk, v_blk = mine(h)
        dist = 5 - slot
        q_far, do_far = win[slot, 0, h], win[slot, 1, h]
        p_far, ds_far = terms(k_blk, v_blk, q_far, do_far, swin[dist - 1, pl.ds(h, 1), :], swin[dist - 1, pl.ds(n_heads + h, 1), :], starts[pl.ds(dist, 1), :], base, base + dist * n_tok)
        return nn_dot(ds_far, q_far), nn_dot(p_far, do_far)

    def key_blocks(h, slots):
        dq_acc[h % IN_FLIGHT] += sum(key_block(h, slot) for slot in slots)

    def query_blocks(h, slots):
        found = [query_block(h, slot) for slot in slots]
        dk_acc[h % IN_FLIGHT] += sum(item[0] for item in found)
        dv_acc[h % IN_FLIGHT] += sum(item[1] for item in found)

    def chip_part(h):
        q_blk, do_blk, k_blk, v_blk = mine(h)
        p_t, ds_t = terms(k_blk, v_blk, q_blk, do_blk, stat[pl.ds(h, 1), :], stat[pl.ds(n_heads + h, 1), :], starts[0:1, :], base, base)
        dv_acc[h % IN_FLIGHT] = nn_dot(p_t, do_blk)
        dk_acc[h % IN_FLIGHT] = nn_dot(ds_t, q_blk)
        dq_acc[h % IN_FLIGHT] = tn_dot(ds_t, k_blk)
        own_qd(h).wait_recv()
        pl.when(core == 1)(lambda: key_blocks(h, [0]))
        pl.when(core == 0)(lambda: query_blocks(h, [4]))

    def far_part(h, keys):
        pl.when(keys)(lambda: key_blocks(h, [1, 2 * core]))
        pl.when(jnp.logical_not(keys))(lambda: query_blocks(h, [3, 2 + 2 * core]))

    def x_part(h):
        fx_copy(h).wait_recv()
        far_part(h, chip_odd == 1)

    def y_part(h):
        fy_copy(h).wait_recv()
        far_part(h, chip_odd == 0)

    def out_copy(h, which):
        dst = (dq_ref, dk_ref, dv_ref)[which]
        return pltpu.make_async_copy(out_buf.at[h % IN_FLIGHT, which], dst.at[h], out_sem.at[h % IN_FLIGHT, which])

    def finish(h):
        @pl.when(h >= IN_FLIGHT)
        def _():
            for which in range(3):
                out_copy(h - IN_FLIGHT, which).wait()

        at = h % IN_FLIGHT
        out_buf[at, 0] = (dq_acc[at] * score_scale).astype(out_buf.dtype)
        out_buf[at, 1] = (dk_acc[at] * score_scale).astype(out_buf.dtype)
        out_buf[at, 2] = dv_acc[at].astype(out_buf.dtype)
        for which in range(3):
            out_copy(h, which).start()

    for dist, copy in stats:
        pl.when(me + dist < n_dev)(copy.wait_recv)
    chip_part(0)

    def step(t, carry):
        pl.when(t < n_heads)(lambda: arrive(t))

        pl.when((t >= 1) & (t <= n_heads))(lambda: x_part(t - 1))
        pl.when((t >= 1) & (t <= n_heads) & middle)(lambda: arrive_y(t - 1))
        pl.when((t >= 2) & middle)(lambda: y_part(t - 2))
        pl.when(t >= 2)(lambda: finish(t - 2))
        pl.when(t < n_heads - 1)(lambda: chip_part(t + 1))
        return carry

    lax.fori_loop(0, n_heads + 2, step, 0)

    def drain(h, carry):
        own_kv(h).wait_send()
        fx_copy(h).wait_send()
        pl.when(middle)(lambda: fy_copy(h).wait_send())
        for r in range(ROW_PARTS):
            x_copy(h, r).wait_send()
            pl.when(relays)(lambda: y_copy(h, r).wait_send())
        return carry

    lax.fori_loop(0, n_heads, drain, 0)
    for dist, copy in stats:
        pl.when(me >= dist)(copy.wait_send)
    for h in range(n_heads - IN_FLIGHT, n_heads):
        for which in range(3):
            out_copy(h, which).wait()


def token_major_kernel(dq_ref, dk_ref, dv_ref, dq_out, dk_out, dv_out):
    for src, dst in ((dq_ref, dq_out), (dk_ref, dk_out), (dv_ref, dv_out)):
        dst[...] = jnp.swapaxes(src[...], 0, 1)


def solution(mesh):
    n_dev = mesh.shape["cp"]
    head_spec = P("cp", "hp", None)
    row_spec = P("cp", "hp")
    any_spec = pl.BlockSpec(memory_space=pl.ANY)
    vmem_spec = pl.BlockSpec(memory_space=pltpu.VMEM)
    smem_spec = pl.BlockSpec(memory_space=pltpu.SMEM)
    dma = pltpu.SemaphoreType.DMA

    def device_fn(q_loc, k_loc, v_loc, o_loc, do_loc, lse_loc, cu_seqlens):
        n_tok, n_heads, head_dim = q_loc.shape
        seq_len = n_tok * n_dev
        score_scale = head_dim ** -0.5
        pair_shape = (2, n_heads, n_tok, head_dim)

        def wide(q_loc, k_loc, v_loc, o_loc, do_loc, lse_loc, cu_seqlens):
            bf16, f32 = jnp.bfloat16, jnp.float32
            per = n_heads // n_dev
            pos = jnp.arange(seq_len, dtype=jnp.int32).reshape(n_dev, n_tok)
            start_rows = jnp.max(jnp.where(cu_seqlens <= pos[..., None], cu_seqlens, 0), axis=-1)
            delta_loc = jnp.einsum("shd,shd->hs", do_loc, o_loc, preferred_element_type=f32)
            parts = [item.reshape(n_dev, per, n_tok) for item in (lse_loc.T, delta_loc)]
            stat = jnp.concatenate(parts + [jnp.zeros((n_dev, 8 - 2 * per, n_tok), f32)], axis=1)
            ops = jnp.stack([q_loc, k_loc, v_loc, do_loc]).transpose(0, 2, 1, 3)

            def heads_of(dev):
                return pl.ds(dev * per, per)

            def call(pairs, n_pairs, ident, out_shape, *args):
                return pl.pallas_call(functools.partial(swap_kernel, n_dev, pairs), out_shape=out_shape,
                                      in_specs=[any_spec] * len(args), out_specs=[any_spec] * len(out_shape),
                                      scratch_shapes=[dma((n_pairs, n_dev)), dma((n_pairs, n_dev)), dma((n_pairs,))],
                                      compiler_params=pltpu.CompilerParams(collective_id=ident, has_side_effects=True))(*args)

            def in_pairs(refs):
                ops_ref, stat_ref, got_ref, gstat_ref = refs
                return [(lambda d: ops_ref.at[:, heads_of(d)], lambda d: got_ref.at[d]), (lambda d: stat_ref.at[d], lambda d: gstat_ref.at[d])]

            def out_pairs(refs):
                grad_ref, back_ref = refs
                return [(lambda d: grad_ref.at[d], lambda d: back_ref.at[:, heads_of(d)])]

            got, gstat = call(in_pairs, 2, 1, (jax.ShapeDtypeStruct((n_dev, 4, per, n_tok, head_dim), bf16), jax.ShapeDtypeStruct((n_dev, 8, n_tok), f32)), ops, stat)
            grads = pl.pallas_call(
                functools.partial(head_kernel, score_scale),
                grid_spec=pltpu.PrefetchScalarGridSpec(
                    num_scalar_prefetch=1, grid=(per,),
                    in_specs=[pl.BlockSpec((n_dev, 4, 1, n_tok, head_dim), lambda h, s: (0, 0, h, 0, 0)), pl.BlockSpec((n_dev, 8, n_tok), lambda h, s: (0, 0, 0)), pl.BlockSpec((n_dev, n_tok), lambda h, s: (0, 0))],
                    out_specs=pl.BlockSpec((n_dev, 3, 1, n_tok, head_dim), lambda h, s: (0, 0, h, 0, 0)),
                    scratch_shapes=[pltpu.VMEM((n_dev, n_tok, head_dim), f32)] * 3),
                out_shape=jax.ShapeDtypeStruct((n_dev, 3, per, n_tok, head_dim), bf16), name="head_grads",
            )(start_rows[:, 0], got, gstat, start_rows)
            back, = call(out_pairs, 1, 2, (jax.ShapeDtypeStruct((3, n_heads, n_tok, head_dim), bf16),), grads)
            return tuple(back[n].transpose(1, 0, 2) for n in range(3))

        def near(q_loc, k_loc, v_loc, o_loc, do_loc, lse_loc, cu_seqlens):
            out_one = jax.ShapeDtypeStruct((n_heads, n_tok, head_dim), q_loc.dtype)
            bf16, f32 = jnp.bfloat16, jnp.float32
            heads_out = pl.pallas_call(
                functools.partial(near_kernel, n_dev, score_scale),
                out_shape=(out_one, out_one, out_one),
                in_specs=[smem_spec] + [any_spec] * 5 + [vmem_spec], out_specs=(any_spec,) * 3,
                scratch_shapes=[pltpu.VMEM((n_heads // TILE_HEADS, 4, n_tok, TILE_HEADS, head_dim), bf16), pltpu.VMEM(q_loc.shape, bf16)]
                + [pltpu.VMEM(pair_shape, bf16)] * 3 + [pltpu.VMEM((5,) + pair_shape, bf16)]
                + [pltpu.VMEM((2 * n_heads, n_tok), f32), pltpu.VMEM((REACH, 2 * n_heads, n_tok), f32), pltpu.VMEM((8, n_tok), jnp.int32)]
                + [pltpu.VMEM((IN_FLIGHT, 3, n_tok, head_dim), bf16)] + [pltpu.VMEM((IN_FLIGHT, n_tok, head_dim), f32)] * 3
                + [dma((n_heads // TILE_HEADS, ROW_PARTS, 4)), dma, dma((IN_FLIGHT, 3)), dma((REACH,)), dma((REACH,)), dma((n_heads,)), dma((n_heads,))]
                + [dma((n_heads, ROW_PARTS))] * 4 + [dma((n_heads,))] * 4,
                compiler_params=pltpu.CompilerParams(collective_id=0, has_side_effects=True), name="near_grads",
            )(cu_seqlens, q_loc, k_loc, v_loc, o_loc, do_loc, lse_loc.T)
            rows = n_tok // OUT_STEPS
            return pl.pallas_call(
                token_major_kernel, grid=(OUT_STEPS,), out_shape=(jax.ShapeDtypeStruct(q_loc.shape, bf16),) * 3,
                in_specs=[pl.BlockSpec((n_heads, rows, head_dim), lambda i: (0, i, 0))] * 3,
                out_specs=[pl.BlockSpec((rows, n_heads, head_dim), lambda i: (i, 0, 0))] * 3, name="token_major", compiler_params=pltpu.CompilerParams(vmem_limit_bytes=67043328))(*heads_out)

        def branch_kernel(cu_ref, out_ref):
            first = 2 * n_tok

            def scan(n, seen):
                here = cu_ref[n]
                return tuple(jnp.where((here >= c * first) & (here <= (c + 1) * first), 1, flag) for c, flag in zip((1, 2), seen))

            seen = lax.fori_loop(0, cu_ref.shape[0], scan, (0, 0), unroll=True)
            out_ref[0] = 1 - seen[0] * seen[1]

        pick = pl.pallas_call(branch_kernel, out_shape=jax.ShapeDtypeStruct((1,), jnp.int32), in_specs=[smem_spec], out_specs=smem_spec, name="pick_branch")(cu_seqlens)[0]
        return lax.switch(pick, (near, wide), q_loc, k_loc, v_loc, o_loc, do_loc, lse_loc, cu_seqlens)

    return jax.shard_map(device_fn, mesh=mesh, in_specs=(head_spec, head_spec, head_spec, head_spec, head_spec, row_spec, P()), out_specs=(head_spec, head_spec, head_spec), check_vma=False)
```

```python
import functools

import jax
import jax.numpy as jnp
from jax import lax
from jax.experimental import pallas as pl
from jax.experimental.pallas import tpu as pltpu
from jax.sharding import PartitionSpec as P

REACH = 3
TILE_HEADS = 8
ROW_PARTS = 2
IN_FLIGHT = 4
OUT_STEPS = 2
LOG2E = 1.4426950408889634
MESH_ID = pl.DeviceIdType.MESH


def to_dev(idx):
    return {"cp": idx}


def greet_all(n_dev, me):
    barrier = pltpu.get_barrier_semaphore()
    for step in range(1, n_dev):
        pl.semaphore_signal(barrier, inc=1, device_id=to_dev(lax.rem(me + step, n_dev)), device_id_type=MESH_ID)


def await_all(n_dev):
    pl.semaphore_wait(pltpu.get_barrier_semaphore(), n_dev - 1)


def stat_copies(me, n_dev, stat_ref, swin_ref, send_sem, recv_sem):
    out = []
    for dist in range(1, REACH + 1):
        copy = pltpu.make_async_remote_copy(src_ref=stat_ref, dst_ref=swin_ref.at[dist - 1], send_sem=send_sem.at[dist - 1], recv_sem=recv_sem.at[dist - 1], device_id=to_dev(lax.rem(me + n_dev - dist, n_dev)), device_id_type=MESH_ID)
        out.append((dist, copy))
    return out


def nt_dot(a, b):
    return lax.dot_general(a, b, (((1,), (1,)), ((), ())), preferred_element_type=jnp.float32)


def nn_dot(a, b):
    return lax.dot_general(a, b, (((1,), (0,)), ((), ())), preferred_element_type=jnp.float32)


def tn_dot(a, b):
    return lax.dot_general(a, b, (((0,), (0,)), ((), ())), preferred_element_type=jnp.float32)


def block_terms(score_scale, k_blk, v_blk, q_blk, do_blk, lse_row, delta_row, start_row, k_base, q_base):
    s_t = nt_dot(k_blk, q_blk)
    dp_t = nt_dot(v_blk, do_blk)
    k_pos = k_base + lax.broadcasted_iota(jnp.int32, s_t.shape, 0)
    q_pos = q_base + lax.broadcasted_iota(jnp.int32, s_t.shape, 1)
    keep = (k_pos >= start_row) & (k_pos <= q_pos)
    p_t = jnp.where(keep, jnp.exp2(s_t * (score_scale * LOG2E) - lse_row * LOG2E), 0.0)
    ds_t = (p_t * (dp_t - delta_row)).astype(jnp.bfloat16)
    return p_t.astype(jnp.bfloat16), ds_t


def swap_kernel(n_dev, pairs, *refs):
    me = lax.axis_index("cp")
    views = pairs(refs[:-3])
    s_sem, r_sem, l_sem = refs[-3:]
    greet_all(n_dev, me)
    await_all(n_dev)

    def copies(mask):
        peer = me ^ mask
        return [pltpu.make_async_remote_copy(src_ref=src(peer), dst_ref=dst(me), send_sem=s_sem.at[n, mask], recv_sem=r_sem.at[n, mask], device_id=to_dev(peer), device_id_type=MESH_ID)
                for n, (src, dst) in enumerate(views)]

    order = [2, 4, 6, 3, 5, 7, 1]
    for mask in order:
        for copy in copies(mask):
            copy.start()
    for n, (src, dst) in enumerate(views):
        pltpu.make_async_copy(src(me), dst(me), l_sem.at[n]).start()
    for n, (src, dst) in enumerate(views):
        pltpu.make_async_copy(src(me), dst(me), l_sem.at[n]).wait()
    for mask in order:
        for copy in copies(mask):
            copy.wait()


def head_kernel(score_scale, start_ref, got_ref, gstat_ref, rows_ref, out_ref, dq_acc, dk_acc, dv_acc):
    head = pl.program_id(0)
    n_dev, _, _, n_tok, _ = got_ref.shape
    terms = functools.partial(block_terms, score_scale)

    def shard(i, carry):
        q_blk, do_blk = got_ref[i, 0, 0], got_ref[i, 3, 0]
        lse_row, delta_row = gstat_ref[i, pl.ds(head, 1), :], gstat_ref[i, pl.ds(2 + head, 1), :]
        start_row = rows_ref[pl.ds(i, 1), :]

        def pair(j, first):
            k_blk, v_blk = got_ref[j, 1, 0], got_ref[j, 2, 0]
            p_t, ds_t = terms(k_blk, v_blk, q_blk, do_blk, lse_row, delta_row, start_row, j * n_tok, i * n_tok)
            dv, dk, dq = nn_dot(p_t, do_blk), nn_dot(ds_t, q_blk), tn_dot(ds_t, k_blk)
            if first:
                dv_acc[j], dk_acc[j], dq_acc[i] = dv, dk, dq
            else:
                dv_acc[j] += dv
                dk_acc[j] += dk
                dq_acc[i] += dq

        pair(i, True)
        lowest = start_ref[i] // n_tok
        lax.fori_loop(lowest, i, lambda j, c: (pair(j, False), c)[1], 0)
        return carry

    lax.fori_loop(0, n_dev, shard, 0)

    def write(i, carry):
        out_ref[i, 0, 0] = (dq_acc[i] * score_scale).astype(out_ref.dtype)
        out_ref[i, 1, 0] = (dk_acc[i] * score_scale).astype(out_ref.dtype)
        out_ref[i, 2, 0] = dv_acc[i].astype(out_ref.dtype)
        return carry

    lax.fori_loop(0, n_dev, write, 0)


def near_kernel(n_dev, score_scale, cu_ref, q_ref, k_ref, v_ref, o_ref, do_ref, lse_ref, dq_ref, dk_ref, dv_ref,
                raw, raw_o, qd, kv, pk, win, stat, swin, starts, dq_acc, dk_acc, dv_acc,
                ld_sem, o_sem, st_s, st_r, own_s, own_r, x_s, x_r, y_s, y_r, fx_s, fx_r, fy_s, fy_r):
    me = lax.axis_index("cp")
    core = lax.rem(me, 2)
    chip = me // 2
    chip_odd = lax.rem(chip, 2)
    n_tok, n_heads, _ = q_ref.shape
    part = n_tok // ROW_PARTS
    base = me * n_tok
    first_chip, last_chip = chip == 0, chip == n_dev // 2 - 1
    not_first, not_last = jnp.logical_not(first_chip), jnp.logical_not(last_chip)
    relays = first_chip | last_chip
    middle = jnp.logical_not(relays)
    x_dev, y_dev, mate = me + 2 - 4 * chip_odd, lax.rem(me + 4, n_dev), me + 1 - 2 * core
    x_dst = 1 + 2 * chip_odd
    x_slot = 3 - 2 * chip_odd
    y_slot = 4 - x_slot

    def remote(src, dst, s_sem, r_sem, dev):
        return pltpu.make_async_remote_copy(src_ref=src, dst_ref=dst, send_sem=s_sem, recv_sem=r_sem, device_id=to_dev(dev), device_id_type=MESH_ID)

    def block(slot, h, r):
        return win.at[slot, :, h, pl.ds(r * part, part)]

    def x_copy(h, r):
        return remote(pk.at[:, h, pl.ds(r * part, part)], block(x_dst, h, r), x_s.at[h, r], x_r.at[h, r], x_dev)

    def y_copy(h, r):
        return remote(block(x_slot, h, r), block(y_slot, h, r), y_s.at[h, r], y_r.at[h, r], y_dev)

    def fx_copy(h):
        return remote(win.at[x_slot, :, h], win.at[4 - 2 * core - 2 * chip_odd, :, h], fx_s.at[h], fx_r.at[h], mate)

    def fy_copy(h):
        return remote(win.at[y_slot, :, h], win.at[2 - 2 * core + 2 * chip_odd, :, h], fy_s.at[h], fy_r.at[h], mate)

    def own_kv(h):
        return remote(kv.at[:, h], win.at[0, :, h], own_s.at[h], own_r.at[h], mate)

    def own_qd(h):
        return remote(qd.at[:, h], win.at[4, :, h], own_s.at[h], own_r.at[h], mate)

    halves = n_heads // TILE_HEADS
    units = [(half, r) for half in range(halves) for r in range(ROW_PARTS)]

    def load(half, r, which):
        src = (q_ref, k_ref, do_ref, v_ref)[which]
        rows, heads = pl.ds(r * part, part), pl.ds(half * TILE_HEADS, TILE_HEADS)
        return pltpu.make_async_copy(src.at[rows, heads], raw.at[half, which, rows], ld_sem.at[half, r, which])

    greet_all(n_dev, me)
    for half, r in units:
        for which in range(4):
            load(half, r, which).start()
    load_o = pltpu.make_async_copy(o_ref, raw_o, o_sem)
    load_o.start()

    chip_pos = chip * 2 * n_tok

    def scan_cross(n, cross_end):
        return jnp.where((cu_ref[n] < chip_pos) & (cu_ref[n + 1] > chip_pos), cu_ref[n + 1], cross_end)

    n_docs = cu_ref.shape[0] - 1
    send_rows = lax.fori_loop(0, n_docs, scan_cross, 0, unroll=True) - base

    def find_starts():
        pos = base + n_tok * lax.broadcasted_iota(jnp.int32, starts.shape, 0) + lax.broadcasted_iota(jnp.int32, starts.shape, 1)

        def scan_docs(n, found):
            return jnp.where(cu_ref[n] <= pos, jnp.maximum(found, cu_ref[n]), found)

        found = lax.fori_loop(0, n_docs, scan_docs, jnp.zeros(starts.shape, jnp.int32))
        starts[...] = jnp.where(pos < n_dev * n_tok, found, n_dev * n_tok)

    row_ids = lax.broadcasted_iota(jnp.int32, (TILE_HEADS, part, q_ref.shape[2]), 1)
    stats = stat_copies(me, n_dev, stat, swin, st_s, st_r)

    def arrange(half, r):
        rows, heads = pl.ds(r * part, part), pl.ds(half * TILE_HEADS, TILE_HEADS)
        for pair in range(2):
            load(half, r, 2 * pair).wait()
            load(half, r, 2 * pair + 1).wait()
            q_side = jnp.swapaxes(raw[half, 2 * pair, rows], 0, 1)
            k_side = jnp.swapaxes(raw[half, 2 * pair + 1, rows], 0, 1)
            pk[pair, heads, rows] = jnp.where(row_ids < send_rows - r * part, q_side, k_side)
            qd[pair, heads, rows] = q_side
            kv[pair, heads, rows] = k_side

    def start_own(half):
        for h in range(half * TILE_HEADS, (half + 1) * TILE_HEADS):
            pl.when(core == 0)(own_kv(h).start)
            pl.when(core == 1)(own_qd(h).start)

    for r in range(ROW_PARTS):
        arrange(0, r)
        if r == 0:
            await_all(n_dev)
        x_copy(0, r).start()
    start_own(0)
    for half in range(1, halves):
        for r in range(ROW_PARTS):
            arrange(half, r)
        start_own(half)
    find_starts()
    load_o.wait()
    stat[0:n_heads, :] = lse_ref[...]
    for half in range(halves):
        delta = jnp.sum(raw[half, 2].astype(jnp.float32) * raw_o[:, half * TILE_HEADS:(half + 1) * TILE_HEADS, :].astype(jnp.float32), axis=-1)
        stat[n_heads + half * TILE_HEADS:n_heads + (half + 1) * TILE_HEADS, :] = delta.T
    for dist, copy in stats:
        pl.when(me >= dist)(copy.start)

    terms = functools.partial(block_terms, score_scale)

    def arrive(h):
        for r in range(ROW_PARTS):
            x_copy(h, r).wait_recv()
            pl.when(relays)(lambda: y_copy(h, r).start())
            pl.when(h + 1 < n_heads)(lambda: x_copy(h + 1, r).start())
        fx_copy(h).start()

    def arrive_y(h):
        for r in range(ROW_PARTS):
            y_copy(h, r).wait_recv()
        fy_copy(h).start()

    def mine(h):
        return qd[0, h], qd[1, h], kv[0, h], kv[1, h]

    def key_block(h, slot):
        q_blk, do_blk, _, _ = mine(h)
        k_far, v_far = win[slot, 0, h], win[slot, 1, h]
        _, ds_far = terms(k_far, v_far, q_blk, do_blk, stat[pl.ds(h, 1), :], stat[pl.ds(n_heads + h, 1), :], starts[0:1, :], base - (slot + 1) * n_tok, base)
        return tn_dot(ds_far, k_far)

    def query_block(h, slot):
        _, _, k_blk, v_blk = mine(h)
        dist = 5 - slot
        q_far, do_far = win[slot, 0, h], win[slot, 1, h]
        p_far, ds_far = terms(k_blk, v_blk, q_far, do_far, swin[dist - 1, pl.ds(h, 1), :], swin[dist - 1, pl.ds(n_heads + h, 1), :], starts[pl.ds(dist, 1), :], base, base + dist * n_tok)
        return nn_dot(ds_far, q_far), nn_dot(p_far, do_far)

    def key_blocks(h, slots):
        dq_acc[h % IN_FLIGHT] += sum(key_block(h, slot) for slot in slots)

    def query_blocks(h, slots):
        found = [query_block(h, slot) for slot in slots]
        dk_acc[h % IN_FLIGHT] += sum(item[0] for item in found)
        dv_acc[h % IN_FLIGHT] += sum(item[1] for item in found)

    def chip_part(h):
        q_blk, do_blk, k_blk, v_blk = mine(h)
        p_t, ds_t = terms(k_blk, v_blk, q_blk, do_blk, stat[pl.ds(h, 1), :], stat[pl.ds(n_heads + h, 1), :], starts[0:1, :], base, base)
        dv_acc[h % IN_FLIGHT] = nn_dot(p_t, do_blk)
        dk_acc[h % IN_FLIGHT] = nn_dot(ds_t, q_blk)
        dq_acc[h % IN_FLIGHT] = tn_dot(ds_t, k_blk)
        own_qd(h).wait_recv()
        pl.when(core == 1)(lambda: key_blocks(h, [0]))
        pl.when(core == 0)(lambda: query_blocks(h, [4]))

    def far_part(h, keys):
        pl.when(keys)(lambda: key_blocks(h, [1, 2 * core]))
        pl.when(jnp.logical_not(keys))(lambda: query_blocks(h, [3, 2 + 2 * core]))

    def x_part(h):
        fx_copy(h).wait_recv()
        far_part(h, chip_odd == 1)

    def y_part(h):
        fy_copy(h).wait_recv()
        far_part(h, chip_odd == 0)

    def finish(h):
        at = h % IN_FLIGHT
        dq_ref[h] = (dq_acc[at] * score_scale).astype(dq_ref.dtype)
        dk_ref[h] = (dk_acc[at] * score_scale).astype(dk_ref.dtype)
        dv_ref[h] = dv_acc[at].astype(dv_ref.dtype)

    for dist, copy in stats:
        pl.when(me + dist < n_dev)(copy.wait_recv)
    chip_part(0)

    def step(t, carry):
        pl.when(t < n_heads)(lambda: arrive(t))

        pl.when((t >= 1) & (t <= n_heads))(lambda: x_part(t - 1))
        pl.when((t >= 1) & (t <= n_heads) & middle)(lambda: arrive_y(t - 1))
        pl.when((t >= 2) & middle)(lambda: y_part(t - 2))
        pl.when(t >= 2)(lambda: finish(t - 2))
        pl.when(t < n_heads - 1)(lambda: chip_part(t + 1))
        return carry

    lax.fori_loop(0, n_heads + 2, step, 0)

    def drain(h, carry):
        own_kv(h).wait_send()
        fx_copy(h).wait_send()
        pl.when(middle)(lambda: fy_copy(h).wait_send())
        for r in range(ROW_PARTS):
            x_copy(h, r).wait_send()
            pl.when(relays)(lambda: y_copy(h, r).wait_send())
        return carry

    lax.fori_loop(0, n_heads, drain, 0)
    for dist, copy in stats:
        pl.when(me >= dist)(copy.wait_send)


def token_major_kernel(dq_ref, dk_ref, dv_ref, dq_out, dk_out, dv_out, rows_buf, out_sem):
    part = dq_ref.shape[1] // OUT_STEPS
    copies = []
    for r in range(OUT_STEPS):
        for which, (src, dst) in enumerate(((dq_ref, dq_out), (dk_ref, dk_out), (dv_ref, dv_out))):
            rows = pl.ds(r * part, part)
            rows_buf[which, rows] = jnp.swapaxes(src[:, rows], 0, 1)
            copies.append(pltpu.make_async_copy(rows_buf.at[which, rows], dst.at[rows], out_sem.at[which, r]))
            copies[-1].start()
    for copy in copies:
        copy.wait()


def solution(mesh):
    n_dev = mesh.shape["cp"]
    head_spec = P("cp", "hp", None)
    row_spec = P("cp", "hp")
    any_spec = pl.BlockSpec(memory_space=pl.ANY)
    vmem_spec = pl.BlockSpec(memory_space=pltpu.VMEM)
    smem_spec = pl.BlockSpec(memory_space=pltpu.SMEM)
    dma = pltpu.SemaphoreType.DMA

    def device_fn(q_loc, k_loc, v_loc, o_loc, do_loc, lse_loc, cu_seqlens):
        n_tok, n_heads, head_dim = q_loc.shape
        seq_len = n_tok * n_dev
        score_scale = head_dim ** -0.5
        pair_shape = (2, n_heads, n_tok, head_dim)

        def wide(q_loc, k_loc, v_loc, o_loc, do_loc, lse_loc, cu_seqlens):
            bf16, f32 = jnp.bfloat16, jnp.float32
            per = n_heads // n_dev
            pos = jnp.arange(seq_len, dtype=jnp.int32).reshape(n_dev, n_tok)
            start_rows = jnp.max(jnp.where(cu_seqlens <= pos[..., None], cu_seqlens, 0), axis=-1)
            delta_loc = jnp.einsum("shd,shd->hs", do_loc, o_loc, preferred_element_type=f32)
            parts = [item.reshape(n_dev, per, n_tok) for item in (lse_loc.T, delta_loc)]
            stat = jnp.concatenate(parts + [jnp.zeros((n_dev, 8 - 2 * per, n_tok), f32)], axis=1)
            ops = jnp.stack([q_loc, k_loc, v_loc, do_loc]).transpose(0, 2, 1, 3)

            def heads_of(dev):
                return pl.ds(dev * per, per)

            def call(pairs, n_pairs, ident, out_shape, *args):
                return pl.pallas_call(functools.partial(swap_kernel, n_dev, pairs), out_shape=out_shape,
                                      in_specs=[any_spec] * len(args), out_specs=[any_spec] * len(out_shape),
                                      scratch_shapes=[dma((n_pairs, n_dev)), dma((n_pairs, n_dev)), dma((n_pairs,))],
                                      compiler_params=pltpu.CompilerParams(collective_id=ident, has_side_effects=True))(*args)

            def in_pairs(refs):
                ops_ref, stat_ref, got_ref, gstat_ref = refs
                return [(lambda d: ops_ref.at[:, heads_of(d)], lambda d: got_ref.at[d]), (lambda d: stat_ref.at[d], lambda d: gstat_ref.at[d])]

            def out_pairs(refs):
                grad_ref, back_ref = refs
                return [(lambda d: grad_ref.at[d], lambda d: back_ref.at[:, heads_of(d)])]

            got, gstat = call(in_pairs, 2, 1, (jax.ShapeDtypeStruct((n_dev, 4, per, n_tok, head_dim), bf16), jax.ShapeDtypeStruct((n_dev, 8, n_tok), f32)), ops, stat)
            grads = pl.pallas_call(
                functools.partial(head_kernel, score_scale),
                grid_spec=pltpu.PrefetchScalarGridSpec(
                    num_scalar_prefetch=1, grid=(per,),
                    in_specs=[pl.BlockSpec((n_dev, 4, 1, n_tok, head_dim), lambda h, s: (0, 0, h, 0, 0)), pl.BlockSpec((n_dev, 8, n_tok), lambda h, s: (0, 0, 0)), pl.BlockSpec((n_dev, n_tok), lambda h, s: (0, 0))],
                    out_specs=pl.BlockSpec((n_dev, 3, 1, n_tok, head_dim), lambda h, s: (0, 0, h, 0, 0)),
                    scratch_shapes=[pltpu.VMEM((n_dev, n_tok, head_dim), f32)] * 3),
                out_shape=jax.ShapeDtypeStruct((n_dev, 3, per, n_tok, head_dim), bf16), name="head_grads",
            )(start_rows[:, 0], got, gstat, start_rows)
            back, = call(out_pairs, 1, 2, (jax.ShapeDtypeStruct((3, n_heads, n_tok, head_dim), bf16),), grads)
            return tuple(back[n].transpose(1, 0, 2) for n in range(3))

        def near(q_loc, k_loc, v_loc, o_loc, do_loc, lse_loc, cu_seqlens):
            out_one = pltpu.VMEM((n_heads, n_tok, head_dim), q_loc.dtype)
            bf16, f32 = jnp.bfloat16, jnp.float32
            heads_out = pl.pallas_call(
                functools.partial(near_kernel, n_dev, score_scale),
                out_shape=(out_one, out_one, out_one),
                in_specs=[smem_spec] + [any_spec] * 5 + [vmem_spec], out_specs=(vmem_spec,) * 3,
                scratch_shapes=[pltpu.VMEM((n_heads // TILE_HEADS, 4, n_tok, TILE_HEADS, head_dim), bf16), pltpu.VMEM(q_loc.shape, bf16)]
                + [pltpu.VMEM(pair_shape, bf16)] * 3 + [pltpu.VMEM((5,) + pair_shape, bf16)]
                + [pltpu.VMEM((2 * n_heads, n_tok), f32), pltpu.VMEM((REACH, 2 * n_heads, n_tok), f32), pltpu.VMEM((8, n_tok), jnp.int32)]
                + [pltpu.VMEM((IN_FLIGHT, n_tok, head_dim), f32)] * 3
                + [dma((n_heads // TILE_HEADS, ROW_PARTS, 4)), dma, dma((REACH,)), dma((REACH,)), dma((n_heads,)), dma((n_heads,))]
                + [dma((n_heads, ROW_PARTS))] * 4 + [dma((n_heads,))] * 4,
                compiler_params=pltpu.CompilerParams(collective_id=0, has_side_effects=True, vmem_limit_bytes=50 * 1024 * 1024), name="near_grads",
            )(cu_seqlens, q_loc, k_loc, v_loc, o_loc, do_loc, lse_loc.T)
            return pl.pallas_call(
                token_major_kernel, out_shape=(pltpu.HBM(q_loc.shape, bf16),) * 3, in_specs=[vmem_spec] * 3, out_specs=(any_spec,) * 3,
                scratch_shapes=[pltpu.VMEM((3,) + q_loc.shape, bf16), dma((3, OUT_STEPS))],
                name="token_major", compiler_params=pltpu.CompilerParams(vmem_limit_bytes=20 * 1024 * 1024))(*heads_out)

        def branch_kernel(cu_ref, out_ref):
            first = 2 * n_tok

            def scan(n, seen):
                here = cu_ref[n]
                return tuple(jnp.where((here >= c * first) & (here <= (c + 1) * first), 1, flag) for c, flag in zip((1, 2), seen))

            seen = lax.fori_loop(0, cu_ref.shape[0], scan, (0, 0), unroll=True)
            out_ref[0] = 1 - seen[0] * seen[1]

        pick = pl.pallas_call(branch_kernel, out_shape=jax.ShapeDtypeStruct((1,), jnp.int32), in_specs=[smem_spec], out_specs=smem_spec, name="pick_branch")(cu_seqlens)[0]
        return lax.switch(pick, (near, wide), q_loc, k_loc, v_loc, o_loc, do_loc, lse_loc, cu_seqlens)

    return jax.shard_map(device_fn, mesh=mesh, in_specs=(head_spec, head_spec, head_spec, head_spec, head_spec, row_spec, P()), out_specs=(head_spec, head_spec, head_spec), check_vma=False)
```

```python
import functools

import jax
import jax.numpy as jnp
from jax import lax
from jax.experimental import pallas as pl
from jax.experimental.pallas import tpu as pltpu
from jax.sharding import PartitionSpec as P

REACH = 3
TILE_HEADS = 8
ROW_PARTS = 2
IN_FLIGHT = 4
OUT_STEPS = 2
LOG2E = 1.4426950408889634
MESH_ID = pl.DeviceIdType.MESH


def to_dev(idx):
    return {"cp": idx}


def greet_all(n_dev, me):
    barrier = pltpu.get_barrier_semaphore()
    for step in range(1, n_dev):
        pl.semaphore_signal(barrier, inc=1, device_id=to_dev(lax.rem(me + step, n_dev)), device_id_type=MESH_ID)


def await_all(n_dev):
    pl.semaphore_wait(pltpu.get_barrier_semaphore(), n_dev - 1)


def stat_copies(me, n_dev, stat_ref, swin_ref, send_sem, recv_sem):
    out = []
    for dist in range(1, REACH + 1):
        copy = pltpu.make_async_remote_copy(src_ref=stat_ref, dst_ref=swin_ref.at[dist - 1], send_sem=send_sem.at[dist - 1], recv_sem=recv_sem.at[dist - 1], device_id=to_dev(lax.rem(me + n_dev - dist, n_dev)), device_id_type=MESH_ID)
        out.append((dist, copy))
    return out


def nt_dot(a, b):
    return lax.dot_general(a, b, (((1,), (1,)), ((), ())), preferred_element_type=jnp.float32)


def nn_dot(a, b):
    return lax.dot_general(a, b, (((1,), (0,)), ((), ())), preferred_element_type=jnp.float32)


def tn_dot(a, b):
    return lax.dot_general(a, b, (((0,), (0,)), ((), ())), preferred_element_type=jnp.float32)


def block_terms(score_scale, k_blk, v_blk, q_blk, do_blk, lse_row, delta_row, start_row, k_base, q_base):
    s_t = nt_dot(k_blk, q_blk)
    dp_t = nt_dot(v_blk, do_blk)
    k_pos = k_base + lax.broadcasted_iota(jnp.int32, s_t.shape, 0)
    q_pos = q_base + lax.broadcasted_iota(jnp.int32, s_t.shape, 1)
    keep = (k_pos >= start_row) & (k_pos <= q_pos)
    p_t = jnp.where(keep, jnp.exp2(s_t * (score_scale * LOG2E) - lse_row * LOG2E), 0.0)
    ds_t = (p_t * (dp_t - delta_row)).astype(jnp.bfloat16)
    return p_t.astype(jnp.bfloat16), ds_t


def swap_kernel(n_dev, pairs, *refs):
    me = lax.axis_index("cp")
    views = pairs(refs[:-3])
    s_sem, r_sem, l_sem = refs[-3:]
    greet_all(n_dev, me)
    await_all(n_dev)

    def copies(mask):
        peer = me ^ mask
        return [pltpu.make_async_remote_copy(src_ref=src(peer), dst_ref=dst(me), send_sem=s_sem.at[n, mask], recv_sem=r_sem.at[n, mask], device_id=to_dev(peer), device_id_type=MESH_ID)
                for n, (src, dst) in enumerate(views)]

    order = [2, 4, 6, 3, 5, 7, 1]
    for mask in order:
        for copy in copies(mask):
            copy.start()
    for n, (src, dst) in enumerate(views):
        pltpu.make_async_copy(src(me), dst(me), l_sem.at[n]).start()
    for n, (src, dst) in enumerate(views):
        pltpu.make_async_copy(src(me), dst(me), l_sem.at[n]).wait()
    for mask in order:
        for copy in copies(mask):
            copy.wait()


def turn_kernel(*refs):
    n_out = len(refs) // 2 if len(refs) % 2 == 0 else 1
    srcs, dsts = refs[:len(refs) - n_out], refs[len(refs) - n_out:]
    for n, src in enumerate(srcs):
        if n_out == 1:
            dsts[0][n] = jnp.swapaxes(src[...], 0, 1)
        else:
            dsts[n][...] = jnp.swapaxes(src[0], 0, 1)


def head_kernel(score_scale, start_ref, got_ref, gstat_ref, rows_ref, out_ref, dq_acc, dk_acc, dv_acc):
    head = pl.program_id(0)
    n_dev, _, _, n_tok, _ = got_ref.shape
    terms = functools.partial(block_terms, score_scale)

    def shard(i, carry):
        q_blk, do_blk = got_ref[i, 0, 0], got_ref[i, 3, 0]
        lse_row, delta_row = gstat_ref[i, pl.ds(head, 1), :], gstat_ref[i, pl.ds(2 + head, 1), :]
        start_row = rows_ref[pl.ds(i, 1), :]

        def pair(j, first):
            k_blk, v_blk = got_ref[j, 1, 0], got_ref[j, 2, 0]
            p_t, ds_t = terms(k_blk, v_blk, q_blk, do_blk, lse_row, delta_row, start_row, j * n_tok, i * n_tok)
            dv, dk, dq = nn_dot(p_t, do_blk), nn_dot(ds_t, q_blk), tn_dot(ds_t, k_blk)
            if first:
                dv_acc[j], dk_acc[j], dq_acc[i] = dv, dk, dq
            else:
                dv_acc[j] += dv
                dk_acc[j] += dk
                dq_acc[i] += dq

        pair(i, True)
        lowest = start_ref[i] // n_tok
        lax.fori_loop(lowest, i, lambda j, c: (pair(j, False), c)[1], 0)
        return carry

    lax.fori_loop(0, n_dev, shard, 0)

    def write(i, carry):
        out_ref[i, 0, 0] = (dq_acc[i] * score_scale).astype(out_ref.dtype)
        out_ref[i, 1, 0] = (dk_acc[i] * score_scale).astype(out_ref.dtype)
        out_ref[i, 2, 0] = dv_acc[i].astype(out_ref.dtype)
        return carry

    lax.fori_loop(0, n_dev, write, 0)


def near_kernel(n_dev, score_scale, cu_ref, q_ref, k_ref, v_ref, o_ref, do_ref, lse_ref, dq_ref, dk_ref, dv_ref,
                raw, raw_o, qd, kv, pk, win, stat, swin, starts, dq_acc, dk_acc, dv_acc,
                ld_sem, o_sem, st_s, st_r, own_s, own_r, x_s, x_r, y_s, y_r, fx_s, fx_r, fy_s, fy_r):
    me = lax.axis_index("cp")
    core = lax.rem(me, 2)
    chip = me // 2
    chip_odd = lax.rem(chip, 2)
    n_tok, n_heads, _ = q_ref.shape
    part = n_tok // ROW_PARTS
    base = me * n_tok
    first_chip, last_chip = chip == 0, chip == n_dev // 2 - 1
    not_first, not_last = jnp.logical_not(first_chip), jnp.logical_not(last_chip)
    relays = first_chip | last_chip
    middle = jnp.logical_not(relays)
    x_dev, y_dev, mate = me + 2 - 4 * chip_odd, lax.rem(me + 4, n_dev), me + 1 - 2 * core
    x_dst = 1 + 2 * chip_odd
    x_slot = 3 - 2 * chip_odd
    y_slot = 4 - x_slot

    def remote(src, dst, s_sem, r_sem, dev):
        return pltpu.make_async_remote_copy(src_ref=src, dst_ref=dst, send_sem=s_sem, recv_sem=r_sem, device_id=to_dev(dev), device_id_type=MESH_ID)

    def block(slot, h, r):
        return win.at[slot, :, h, pl.ds(r * part, part)]

    def x_copy(h, r):
        return remote(pk.at[:, h, pl.ds(r * part, part)], block(x_dst, h, r), x_s.at[h, r], x_r.at[h, r], x_dev)

    def y_copy(h, r):
        return remote(block(x_slot, h, r), block(y_slot, h, r), y_s.at[h, r], y_r.at[h, r], y_dev)

    def fx_copy(h):
        return remote(win.at[x_slot, :, h], win.at[4 - 2 * core - 2 * chip_odd, :, h], fx_s.at[h], fx_r.at[h], mate)

    def fy_copy(h):
        return remote(win.at[y_slot, :, h], win.at[2 - 2 * core + 2 * chip_odd, :, h], fy_s.at[h], fy_r.at[h], mate)

    def own_kv(h):
        return remote(kv.at[:, h], win.at[0, :, h], own_s.at[h], own_r.at[h], mate)

    def own_qd(h):
        return remote(qd.at[:, h], win.at[4, :, h], own_s.at[h], own_r.at[h], mate)

    halves = n_heads // TILE_HEADS
    units = [(half, r) for half in range(halves) for r in range(ROW_PARTS)]

    def load(half, r, which):
        src = (q_ref, k_ref, do_ref, v_ref)[which]
        rows, heads = pl.ds(r * part, part), pl.ds(half * TILE_HEADS, TILE_HEADS)
        return pltpu.make_async_copy(src.at[rows, heads], raw.at[half, which, rows], ld_sem.at[half, r, which])

    for half, r in units[:1]:
        for which in range(4):
            load(half, r, which).start()
    greet_all(n_dev, me)
    for half, r in units[1:]:
        for which in range(4):
            load(half, r, which).start()
    load_o = pltpu.make_async_copy(o_ref, raw_o, o_sem)
    load_o.start()

    chip_pos = chip * 2 * n_tok

    def scan_cross(n, cross_end):
        return jnp.where((cu_ref[n] < chip_pos) & (cu_ref[n + 1] > chip_pos), cu_ref[n + 1], cross_end)

    n_docs = cu_ref.shape[0] - 1
    send_rows = lax.fori_loop(0, n_docs, scan_cross, 0, unroll=True) - base

    def find_starts():
        pos = base + n_tok * lax.broadcasted_iota(jnp.int32, starts.shape, 0) + lax.broadcasted_iota(jnp.int32, starts.shape, 1)

        def scan_docs(n, found):
            return jnp.where(cu_ref[n] <= pos, jnp.maximum(found, cu_ref[n]), found)

        found = lax.fori_loop(0, n_docs, scan_docs, jnp.zeros(starts.shape, jnp.int32))
        starts[...] = jnp.where(pos < n_dev * n_tok, found, n_dev * n_tok)

    row_ids = lax.broadcasted_iota(jnp.int32, (TILE_HEADS, part, q_ref.shape[2]), 1)
    stats = stat_copies(me, n_dev, stat, swin, st_s, st_r)

    def arrange(half, r):
        rows, heads = pl.ds(r * part, part), pl.ds(half * TILE_HEADS, TILE_HEADS)
        for pair in range(2):
            load(half, r, 2 * pair).wait()
            load(half, r, 2 * pair + 1).wait()
            q_side = jnp.swapaxes(raw[half, 2 * pair, rows], 0, 1)
            k_side = jnp.swapaxes(raw[half, 2 * pair + 1, rows], 0, 1)
            pk[pair, heads, rows] = jnp.where(row_ids < send_rows - r * part, q_side, k_side)
            qd[pair, heads, rows] = q_side
            kv[pair, heads, rows] = k_side

    def start_own(half):
        for h in range(half * TILE_HEADS, (half + 1) * TILE_HEADS):
            pl.when(core == 0)(own_kv(h).start)
            pl.when(core == 1)(own_qd(h).start)

    for r in range(ROW_PARTS):
        arrange(0, r)
        if r == 0:
            await_all(n_dev)
        x_copy(0, r).start()
    start_own(0)
    for half in range(1, halves):
        for r in range(ROW_PARTS):
            arrange(half, r)
        start_own(half)
    find_starts()
    load_o.wait()
    stat[0:n_heads, :] = lse_ref[...]
    for half in range(halves):
        delta = jnp.sum(raw[half, 2].astype(jnp.float32) * raw_o[:, half * TILE_HEADS:(half + 1) * TILE_HEADS, :].astype(jnp.float32), axis=-1)
        stat[n_heads + half * TILE_HEADS:n_heads + (half + 1) * TILE_HEADS, :] = delta.T
    for dist, copy in stats:
        pl.when(me >= dist)(copy.start)

    terms = functools.partial(block_terms, score_scale)

    def arrive(h):
        for r in range(ROW_PARTS):
            x_copy(h, r).wait_recv()
            pl.when(relays)(lambda: y_copy(h, r).start())
            pl.when(h + 1 < n_heads)(lambda: x_copy(h + 1, r).start())
        fx_copy(h).start()

    def arrive_y(h):
        for r in range(ROW_PARTS):
            y_copy(h, r).wait_recv()
        fy_copy(h).start()

    def mine(h):
        return qd[0, h], qd[1, h], kv[0, h], kv[1, h]

    def key_block(h, slot):
        q_blk, do_blk, _, _ = mine(h)
        k_far, v_far = win[slot, 0, h], win[slot, 1, h]
        _, ds_far = terms(k_far, v_far, q_blk, do_blk, stat[pl.ds(h, 1), :], stat[pl.ds(n_heads + h, 1), :], starts[0:1, :], base - (slot + 1) * n_tok, base)
        return tn_dot(ds_far, k_far)

    def query_block(h, slot):
        _, _, k_blk, v_blk = mine(h)
        dist = 5 - slot
        q_far, do_far = win[slot, 0, h], win[slot, 1, h]
        p_far, ds_far = terms(k_blk, v_blk, q_far, do_far, swin[dist - 1, pl.ds(h, 1), :], swin[dist - 1, pl.ds(n_heads + h, 1), :], starts[pl.ds(dist, 1), :], base, base + dist * n_tok)
        return nn_dot(ds_far, q_far), nn_dot(p_far, do_far)

    def key_blocks(h, slots):
        dq_acc[h % IN_FLIGHT] += sum(key_block(h, slot) for slot in slots)

    def query_blocks(h, slots):
        found = [query_block(h, slot) for slot in slots]
        dk_acc[h % IN_FLIGHT] += sum(item[0] for item in found)
        dv_acc[h % IN_FLIGHT] += sum(item[1] for item in found)

    def chip_part(h):
        q_blk, do_blk, k_blk, v_blk = mine(h)
        p_t, ds_t = terms(k_blk, v_blk, q_blk, do_blk, stat[pl.ds(h, 1), :], stat[pl.ds(n_heads + h, 1), :], starts[0:1, :], base, base)
        dv_acc[h % IN_FLIGHT] = nn_dot(p_t, do_blk)
        dk_acc[h % IN_FLIGHT] = nn_dot(ds_t, q_blk)
        dq_acc[h % IN_FLIGHT] = tn_dot(ds_t, k_blk)
        own_qd(h).wait_recv()
        pl.when(core == 1)(lambda: key_blocks(h, [0]))
        pl.when(core == 0)(lambda: query_blocks(h, [4]))

    def far_part(h, keys):
        pl.when(keys)(lambda: key_blocks(h, [1, 2 * core]))
        pl.when(jnp.logical_not(keys))(lambda: query_blocks(h, [3, 2 + 2 * core]))

    def x_part(h):
        fx_copy(h).wait_recv()
        far_part(h, chip_odd == 1)

    def y_part(h):
        fy_copy(h).wait_recv()
        far_part(h, chip_odd == 0)

    def finish(h):
        at = h % IN_FLIGHT
        dq_ref[h] = (dq_acc[at] * score_scale).astype(dq_ref.dtype)
        dk_ref[h] = (dk_acc[at] * score_scale).astype(dk_ref.dtype)
        dv_ref[h] = dv_acc[at].astype(dv_ref.dtype)

    for dist, copy in stats:
        pl.when(me + dist < n_dev)(copy.wait_recv)
    chip_part(0)

    def step(t, carry):
        pl.when(t < n_heads)(lambda: arrive(t))

        pl.when((t >= 1) & (t <= n_heads))(lambda: x_part(t - 1))
        pl.when((t >= 1) & (t <= n_heads) & middle)(lambda: arrive_y(t - 1))
        pl.when((t >= 2) & middle)(lambda: y_part(t - 2))
        pl.when(t >= 2)(lambda: finish(t - 2))
        pl.when(t < n_heads - 1)(lambda: chip_part(t + 1))
        return carry

    lax.fori_loop(0, n_heads + 2, step, 0)

    def drain(h, carry):
        own_kv(h).wait_send()
        fx_copy(h).wait_send()
        pl.when(middle)(lambda: fy_copy(h).wait_send())
        for r in range(ROW_PARTS):
            x_copy(h, r).wait_send()
            pl.when(relays)(lambda: y_copy(h, r).wait_send())
        return carry

    lax.fori_loop(0, n_heads, drain, 0)
    for dist, copy in stats:
        pl.when(me >= dist)(copy.wait_send)


def token_major_kernel(dq_ref, dk_ref, dv_ref, dq_out, dk_out, dv_out, rows_buf, out_sem):
    part = dq_ref.shape[1] // OUT_STEPS
    copies = []
    for r in range(OUT_STEPS):
        for which, (src, dst) in enumerate(((dq_ref, dq_out), (dk_ref, dk_out), (dv_ref, dv_out))):
            rows = pl.ds(r * part, part)
            rows_buf[which, rows] = jnp.swapaxes(src[:, rows], 0, 1)
            copies.append(pltpu.make_async_copy(rows_buf.at[which, rows], dst.at[rows], out_sem.at[which, r]))
            copies[-1].start()
    for copy in copies:
        copy.wait()


def solution(mesh):
    n_dev = mesh.shape["cp"]
    head_spec = P("cp", "hp", None)
    row_spec = P("cp", "hp")
    any_spec = pl.BlockSpec(memory_space=pl.ANY)
    vmem_spec = pl.BlockSpec(memory_space=pltpu.VMEM)
    smem_spec = pl.BlockSpec(memory_space=pltpu.SMEM)
    dma = pltpu.SemaphoreType.DMA

    def device_fn(q_loc, k_loc, v_loc, o_loc, do_loc, lse_loc, cu_seqlens):
        n_tok, n_heads, head_dim = q_loc.shape
        seq_len = n_tok * n_dev
        score_scale = head_dim ** -0.5
        pair_shape = (2, n_heads, n_tok, head_dim)

        def wide(q_loc, k_loc, v_loc, o_loc, do_loc, lse_loc, cu_seqlens):
            bf16, f32 = jnp.bfloat16, jnp.float32
            per = n_heads // n_dev
            pos = jnp.arange(seq_len, dtype=jnp.int32).reshape(n_dev, n_tok)
            start_rows = jnp.max(jnp.where(cu_seqlens <= pos[..., None], cu_seqlens, 0), axis=-1)
            delta_loc = jnp.einsum("shd,shd->hs", do_loc, o_loc, preferred_element_type=f32)
            parts = [item.reshape(n_dev, per, n_tok) for item in (lse_loc.T, delta_loc)]
            stat = jnp.concatenate(parts + [jnp.zeros((n_dev, 8 - 2 * per, n_tok), f32)], axis=1)
            rows = n_tok // OUT_STEPS
            row_blk = pl.BlockSpec((rows, n_heads, head_dim), lambda i: (i, 0, 0))
            ops = pl.pallas_call(turn_kernel, grid=(OUT_STEPS,), out_shape=jax.ShapeDtypeStruct((4, n_heads, n_tok, head_dim), bf16), in_specs=[row_blk] * 4,
                                 out_specs=pl.BlockSpec((4, n_heads, rows, head_dim), lambda i: (0, 0, i, 0)), name="turn_in")(q_loc, k_loc, v_loc, do_loc)

            def heads_of(dev):
                return pl.ds(dev * per, per)

            def call(pairs, n_pairs, ident, out_shape, *args):
                return pl.pallas_call(functools.partial(swap_kernel, n_dev, pairs), out_shape=out_shape,
                                      in_specs=[any_spec] * len(args), out_specs=[any_spec] * len(out_shape),
                                      scratch_shapes=[dma((n_pairs, n_dev)), dma((n_pairs, n_dev)), dma((n_pairs,))],
                                      compiler_params=pltpu.CompilerParams(collective_id=ident, has_side_effects=True))(*args)

            def in_pairs(refs):
                ops_ref, stat_ref, got_ref, gstat_ref = refs
                return [(lambda d: ops_ref.at[:, heads_of(d)], lambda d: got_ref.at[d]), (lambda d: stat_ref.at[d], lambda d: gstat_ref.at[d])]

            def out_pairs(refs):
                grad_ref, back_ref = refs
                return [(lambda d: grad_ref.at[d], lambda d: back_ref.at[:, heads_of(d)])]

            got, gstat = call(in_pairs, 2, 1, (jax.ShapeDtypeStruct((n_dev, 4, per, n_tok, head_dim), bf16), jax.ShapeDtypeStruct((n_dev, 8, n_tok), f32)), ops, stat)
            grads = pl.pallas_call(
                functools.partial(head_kernel, score_scale),
                grid_spec=pltpu.PrefetchScalarGridSpec(
                    num_scalar_prefetch=1, grid=(per,),
                    in_specs=[pl.BlockSpec((n_dev, 4, 1, n_tok, head_dim), lambda h, s: (0, 0, h, 0, 0)), pl.BlockSpec((n_dev, 8, n_tok), lambda h, s: (0, 0, 0)), pl.BlockSpec((n_dev, n_tok), lambda h, s: (0, 0))],
                    out_specs=pl.BlockSpec((n_dev, 3, 1, n_tok, head_dim), lambda h, s: (0, 0, h, 0, 0)),
                    scratch_shapes=[pltpu.VMEM((n_dev, n_tok, head_dim), f32)] * 3),
                out_shape=jax.ShapeDtypeStruct((n_dev, 3, per, n_tok, head_dim), bf16), name="head_grads",
            )(start_rows[:, 0], got, gstat, start_rows)
            back, = call(out_pairs, 1, 2, (jax.ShapeDtypeStruct((3, n_heads, n_tok, head_dim), bf16),), grads)
            head_blks = [pl.BlockSpec((1, n_heads, rows, head_dim), lambda i, n=n: (n, 0, i, 0)) for n in range(3)]
            return pl.pallas_call(turn_kernel, grid=(OUT_STEPS,), out_shape=(pltpu.HBM(q_loc.shape, bf16),) * 3, in_specs=head_blks, out_specs=[row_blk] * 3, name="turn_out")(back, back, back)

        def near(q_loc, k_loc, v_loc, o_loc, do_loc, lse_loc, cu_seqlens):
            out_one = pltpu.VMEM((n_heads, n_tok, head_dim), q_loc.dtype)
            bf16, f32 = jnp.bfloat16, jnp.float32
            heads_out = pl.pallas_call(
                functools.partial(near_kernel, n_dev, score_scale),
                out_shape=(out_one, out_one, out_one),
                in_specs=[smem_spec] + [any_spec] * 5 + [vmem_spec], out_specs=(vmem_spec,) * 3,
                scratch_shapes=[pltpu.VMEM((n_heads // TILE_HEADS, 4, n_tok, TILE_HEADS, head_dim), bf16), pltpu.VMEM(q_loc.shape, bf16)]
                + [pltpu.VMEM(pair_shape, bf16)] * 3 + [pltpu.VMEM((5,) + pair_shape, bf16)]
                + [pltpu.VMEM((2 * n_heads, n_tok), f32), pltpu.VMEM((REACH, 2 * n_heads, n_tok), f32), pltpu.VMEM((8, n_tok), jnp.int32)]
                + [pltpu.VMEM((IN_FLIGHT, n_tok, head_dim), f32)] * 3
                + [dma((n_heads // TILE_HEADS, ROW_PARTS, 4)), dma, dma((REACH,)), dma((REACH,)), dma((n_heads,)), dma((n_heads,))]
                + [dma((n_heads, ROW_PARTS))] * 4 + [dma((n_heads,))] * 4,
                compiler_params=pltpu.CompilerParams(collective_id=0, has_side_effects=True, vmem_limit_bytes=50 * 1024 * 1024), name="near_grads",
            )(cu_seqlens, q_loc, k_loc, v_loc, o_loc, do_loc, lse_loc.T)
            return pl.pallas_call(
                token_major_kernel, out_shape=(pltpu.HBM(q_loc.shape, bf16),) * 3, in_specs=[vmem_spec] * 3, out_specs=(any_spec,) * 3,
                scratch_shapes=[pltpu.VMEM((3,) + q_loc.shape, bf16), dma((3, OUT_STEPS))],
                name="token_major", compiler_params=pltpu.CompilerParams(vmem_limit_bytes=20 * 1024 * 1024))(*heads_out)

        def branch_kernel(cu_ref, out_ref):
            first = 2 * n_tok

            def scan(n, seen):
                here = cu_ref[n]
                return tuple(jnp.where((here >= c * first) & (here <= (c + 1) * first), 1, flag) for c, flag in zip((1, 2), seen))

            seen = lax.fori_loop(0, cu_ref.shape[0], scan, (0, 0), unroll=True)
            out_ref[0] = 1 - seen[0] * seen[1]

        pick = pl.pallas_call(branch_kernel, out_shape=jax.ShapeDtypeStruct((1,), jnp.int32), in_specs=[smem_spec], out_specs=smem_spec, name="pick_branch")(cu_seqlens)[0]
        return lax.switch(pick, (near, wide), q_loc, k_loc, v_loc, o_loc, do_loc, lse_loc, cu_seqlens)

    return jax.shard_map(device_fn, mesh=mesh, in_specs=(head_spec, head_spec, head_spec, head_spec, head_spec, row_spec, P()), out_specs=(head_spec, head_spec, head_spec), check_vma=False)
```

```python
import functools

import jax
import jax.numpy as jnp
from jax import lax
from jax.experimental import pallas as pl
from jax.experimental.pallas import tpu as pltpu
from jax.sharding import PartitionSpec as P

REACH = 3
TILE_HEADS = 8
ROW_PARTS = 2
IN_FLIGHT = 4
OUT_STEPS = 2
LOG2E = 1.4426950408889634
MESH_ID = pl.DeviceIdType.MESH


def to_dev(idx):
    return {"cp": idx}


def greet_all(n_dev, me):
    barrier = pltpu.get_barrier_semaphore()
    for step in range(1, n_dev):
        pl.semaphore_signal(barrier, inc=1, device_id=to_dev(lax.rem(me + step, n_dev)), device_id_type=MESH_ID)


def await_all(n_dev):
    pl.semaphore_wait(pltpu.get_barrier_semaphore(), n_dev - 1)


def stat_copies(me, n_dev, stat_ref, swin_ref, send_sem, recv_sem):
    out = []
    for dist in range(1, REACH + 1):
        copy = pltpu.make_async_remote_copy(src_ref=stat_ref, dst_ref=swin_ref.at[dist - 1], send_sem=send_sem.at[dist - 1], recv_sem=recv_sem.at[dist - 1], device_id=to_dev(lax.rem(me + n_dev - dist, n_dev)), device_id_type=MESH_ID)
        out.append((dist, copy))
    return out


def nt_dot(a, b):
    return lax.dot_general(a, b, (((1,), (1,)), ((), ())), preferred_element_type=jnp.float32)


def nn_dot(a, b):
    return lax.dot_general(a, b, (((1,), (0,)), ((), ())), preferred_element_type=jnp.float32)


def tn_dot(a, b):
    return lax.dot_general(a, b, (((0,), (0,)), ((), ())), preferred_element_type=jnp.float32)


def block_terms(score_scale, k_blk, v_blk, q_blk, do_blk, lse_row, delta_row, start_row, k_base, q_base):
    s_t = nt_dot(k_blk, q_blk)
    dp_t = nt_dot(v_blk, do_blk)
    k_pos = k_base + lax.broadcasted_iota(jnp.int32, s_t.shape, 0)
    q_pos = q_base + lax.broadcasted_iota(jnp.int32, s_t.shape, 1)
    keep = (k_pos >= start_row) & (k_pos <= q_pos)
    p_t = jnp.where(keep, jnp.exp2(s_t * (score_scale * LOG2E) - lse_row * LOG2E), 0.0)
    ds_t = (p_t * (dp_t - delta_row)).astype(jnp.bfloat16)
    return p_t.astype(jnp.bfloat16), ds_t


def swap_kernel(n_dev, pairs, *refs):
    me = lax.axis_index("cp")
    views = pairs(refs[:-3])
    s_sem, r_sem, l_sem = refs[-3:]
    greet_all(n_dev, me)
    await_all(n_dev)

    def copies(mask):
        peer = me ^ mask
        return [pltpu.make_async_remote_copy(src_ref=src(peer), dst_ref=dst(me), send_sem=s_sem.at[n, mask], recv_sem=r_sem.at[n, mask], device_id=to_dev(peer), device_id_type=MESH_ID)
                for n, (src, dst) in enumerate(views)]

    order = [2, 4, 6, 3, 5, 7, 1]
    for mask in order:
        for copy in copies(mask):
            copy.start()
    for n, (src, dst) in enumerate(views):
        pltpu.make_async_copy(src(me), dst(me), l_sem.at[n]).start()
    for n, (src, dst) in enumerate(views):
        pltpu.make_async_copy(src(me), dst(me), l_sem.at[n]).wait()
    for mask in order:
        for copy in copies(mask):
            copy.wait()


def turn_kernel(*refs):
    n_out = len(refs) // 2 if len(refs) % 2 == 0 else 1
    srcs, dsts = refs[:len(refs) - n_out], refs[len(refs) - n_out:]
    for n, src in enumerate(srcs):
        if n_out == 1:
            dsts[0][n] = jnp.swapaxes(src[...], 0, 1)
        else:
            dsts[n][...] = jnp.swapaxes(src[0], 0, 1)


def head_kernel(score_scale, start_ref, got_ref, gstat_ref, rows_ref, out_ref, dq_acc, dk_acc, dv_acc):
    head = pl.program_id(0)
    n_dev, _, _, n_tok, _ = got_ref.shape
    terms = functools.partial(block_terms, score_scale)

    def shard(i, carry):
        q_blk, do_blk = got_ref[i, 0, 0], got_ref[i, 3, 0]
        lse_row, delta_row = gstat_ref[i, pl.ds(head, 1), :], gstat_ref[i, pl.ds(2 + head, 1), :]
        start_row = rows_ref[pl.ds(i, 1), :]

        def pair(j, first):
            k_blk, v_blk = got_ref[j, 1, 0], got_ref[j, 2, 0]
            p_t, ds_t = terms(k_blk, v_blk, q_blk, do_blk, lse_row, delta_row, start_row, j * n_tok, i * n_tok)
            dv, dk, dq = nn_dot(p_t, do_blk), nn_dot(ds_t, q_blk), tn_dot(ds_t, k_blk)
            if first:
                dv_acc[j], dk_acc[j], dq_acc[i] = dv, dk, dq
            else:
                dv_acc[j] += dv
                dk_acc[j] += dk
                dq_acc[i] += dq

        pair(i, True)
        lowest = start_ref[i] // n_tok
        lax.fori_loop(lowest, i, lambda j, c: (pair(j, False), c)[1], 0)
        return carry

    lax.fori_loop(0, n_dev, shard, 0)

    def write(i, carry):
        out_ref[i, 0, 0] = (dq_acc[i] * score_scale).astype(out_ref.dtype)
        out_ref[i, 1, 0] = (dk_acc[i] * score_scale).astype(out_ref.dtype)
        out_ref[i, 2, 0] = dv_acc[i].astype(out_ref.dtype)
        return carry

    lax.fori_loop(0, n_dev, write, 0)


def near_kernel(n_dev, score_scale, cu_ref, q_ref, k_ref, v_ref, o_ref, do_ref, lse_ref, dq_ref, dk_ref, dv_ref,
                raw, raw_o, qd, kv, pk, win, stat, swin, starts, dq_acc, dk_acc, dv_acc,
                ld_sem, o_sem, st_s, st_r, own_s, own_r, x_s, x_r, y_s, y_r, fx_s, fx_r, fy_s, fy_r):
    me = lax.axis_index("cp")
    core = lax.rem(me, 2)
    chip = me // 2
    chip_odd = lax.rem(chip, 2)
    n_tok, n_heads, _ = q_ref.shape
    part = n_tok // ROW_PARTS
    base = me * n_tok
    first_chip, last_chip = chip == 0, chip == n_dev // 2 - 1
    not_first, not_last = jnp.logical_not(first_chip), jnp.logical_not(last_chip)
    relays = first_chip | last_chip
    middle = jnp.logical_not(relays)
    x_dev, y_dev, mate = me + 2 - 4 * chip_odd, lax.rem(me + 4, n_dev), me + 1 - 2 * core
    x_dst = 1 + 2 * chip_odd
    x_slot = 3 - 2 * chip_odd
    y_slot = 4 - x_slot

    def remote(src, dst, s_sem, r_sem, dev):
        return pltpu.make_async_remote_copy(src_ref=src, dst_ref=dst, send_sem=s_sem, recv_sem=r_sem, device_id=to_dev(dev), device_id_type=MESH_ID)

    def block(slot, h, r):
        return win.at[slot, :, h, pl.ds(r * part, part)]

    def x_copy(h, r):
        return remote(pk.at[:, h, pl.ds(r * part, part)], block(x_dst, h, r), x_s.at[h, r], x_r.at[h, r], x_dev)

    def y_copy(h, r):
        return remote(block(x_slot, h, r), block(y_slot, h, r), y_s.at[h, r], y_r.at[h, r], y_dev)

    def fx_copy(h):
        return remote(win.at[x_slot, :, h], win.at[4 - 2 * core - 2 * chip_odd, :, h], fx_s.at[h], fx_r.at[h], mate)

    def fy_copy(h):
        return remote(win.at[y_slot, :, h], win.at[2 - 2 * core + 2 * chip_odd, :, h], fy_s.at[h], fy_r.at[h], mate)

    def own_kv(h):
        return remote(kv.at[:, h], win.at[0, :, h], own_s.at[h], own_r.at[h], mate)

    def own_qd(h):
        return remote(qd.at[:, h], win.at[4, :, h], own_s.at[h], own_r.at[h], mate)

    halves = n_heads // TILE_HEADS
    units = [(half, r) for half in range(halves) for r in range(ROW_PARTS)]

    def load(half, r, which):
        src = (q_ref, k_ref, do_ref, v_ref)[which]
        rows, heads = pl.ds(r * part, part), pl.ds(half * TILE_HEADS, TILE_HEADS)
        return pltpu.make_async_copy(src.at[rows, heads], raw.at[half, which, rows], ld_sem.at[half, r, which])

    for half, r in units[:1]:
        for which in range(4):
            load(half, r, which).start()
    greet_all(n_dev, me)
    for half, r in units[1:]:
        for which in range(4):
            load(half, r, which).start()
    load_o = pltpu.make_async_copy(o_ref, raw_o, o_sem)
    load_o.start()

    chip_pos = chip * 2 * n_tok

    def scan_cross(n, cross_end):
        return jnp.where((cu_ref[n] < chip_pos) & (cu_ref[n + 1] > chip_pos), cu_ref[n + 1], cross_end)

    n_docs = cu_ref.shape[0] - 1
    send_rows = lax.fori_loop(0, n_docs, scan_cross, 0, unroll=True) - base

    def find_starts():
        pos = base + n_tok * lax.broadcasted_iota(jnp.int32, starts.shape, 0) + lax.broadcasted_iota(jnp.int32, starts.shape, 1)

        def scan_docs(n, found):
            return jnp.where(cu_ref[n] <= pos, jnp.maximum(found, cu_ref[n]), found)

        found = lax.fori_loop(0, n_docs, scan_docs, jnp.zeros(starts.shape, jnp.int32))
        starts[...] = jnp.where(pos < n_dev * n_tok, found, n_dev * n_tok)

    row_ids = lax.broadcasted_iota(jnp.int32, (TILE_HEADS, part, q_ref.shape[2]), 1)
    stats = stat_copies(me, n_dev, stat, swin, st_s, st_r)

    def arrange(half, r):
        rows, heads = pl.ds(r * part, part), pl.ds(half * TILE_HEADS, TILE_HEADS)
        for pair in range(2):
            load(half, r, 2 * pair).wait()
            load(half, r, 2 * pair + 1).wait()
            q_side = jnp.swapaxes(raw[half, 2 * pair, rows], 0, 1)
            k_side = jnp.swapaxes(raw[half, 2 * pair + 1, rows], 0, 1)
            pk[pair, heads, rows] = jnp.where(row_ids < send_rows - r * part, q_side, k_side)
            qd[pair, heads, rows] = q_side
            kv[pair, heads, rows] = k_side

    def start_own(half):
        for h in range(half * TILE_HEADS, (half + 1) * TILE_HEADS):
            pl.when(core == 0)(own_kv(h).start)
            pl.when(core == 1)(own_qd(h).start)

    for r in range(ROW_PARTS):
        arrange(0, r)
        if r == 0:
            await_all(n_dev)
        x_copy(0, r).start()
    start_own(0)
    for half in range(1, halves):
        for r in range(ROW_PARTS):
            arrange(half, r)
        start_own(half)
    find_starts()
    load_o.wait()
    stat[0:n_heads, :] = lse_ref[...]
    for half in range(halves):
        delta = jnp.sum(raw[half, 2].astype(jnp.float32) * raw_o[:, half * TILE_HEADS:(half + 1) * TILE_HEADS, :].astype(jnp.float32), axis=-1)
        stat[n_heads + half * TILE_HEADS:n_heads + (half + 1) * TILE_HEADS, :] = delta.T
    for dist, copy in stats:
        pl.when(me >= dist)(copy.start)

    terms = functools.partial(block_terms, score_scale)

    def arrive(h):
        for r in range(ROW_PARTS):
            x_copy(h, r).wait_recv()
            pl.when(relays)(lambda: y_copy(h, r).start())
            pl.when(h + 1 < n_heads)(lambda: x_copy(h + 1, r).start())
        fx_copy(h).start()

    def arrive_y(h):
        for r in range(ROW_PARTS):
            y_copy(h, r).wait_recv()
        fy_copy(h).start()

    def mine(h):
        return qd[0, h], qd[1, h], kv[0, h], kv[1, h]

    def key_block(h, slot):
        q_blk, do_blk, _, _ = mine(h)
        k_far, v_far = win[slot, 0, h], win[slot, 1, h]
        _, ds_far = terms(k_far, v_far, q_blk, do_blk, stat[pl.ds(h, 1), :], stat[pl.ds(n_heads + h, 1), :], starts[0:1, :], base - (slot + 1) * n_tok, base)
        return tn_dot(ds_far, k_far)

    def query_block(h, slot):
        _, _, k_blk, v_blk = mine(h)
        dist = 5 - slot
        q_far, do_far = win[slot, 0, h], win[slot, 1, h]
        p_far, ds_far = terms(k_blk, v_blk, q_far, do_far, swin[dist - 1, pl.ds(h, 1), :], swin[dist - 1, pl.ds(n_heads + h, 1), :], starts[pl.ds(dist, 1), :], base, base + dist * n_tok)
        return nn_dot(ds_far, q_far), nn_dot(p_far, do_far)

    def key_blocks(h, slots):
        dq_acc[h % IN_FLIGHT] += sum(key_block(h, slot) for slot in slots)

    def query_blocks(h, slots):
        found = [query_block(h, slot) for slot in slots]
        dk_acc[h % IN_FLIGHT] += sum(item[0] for item in found)
        dv_acc[h % IN_FLIGHT] += sum(item[1] for item in found)

    def chip_part(h):
        q_blk, do_blk, k_blk, v_blk = mine(h)
        p_t, ds_t = terms(k_blk, v_blk, q_blk, do_blk, stat[pl.ds(h, 1), :], stat[pl.ds(n_heads + h, 1), :], starts[0:1, :], base, base)
        dv_acc[h % IN_FLIGHT] = nn_dot(p_t, do_blk)
        dk_acc[h % IN_FLIGHT] = nn_dot(ds_t, q_blk)
        dq_acc[h % IN_FLIGHT] = tn_dot(ds_t, k_blk)
        own_qd(h).wait_recv()
        pl.when(core == 1)(lambda: key_blocks(h, [0]))
        pl.when(core == 0)(lambda: query_blocks(h, [4]))

    def far_part(h, keys, key_slots, query_slots):
        pl.when(keys)(lambda: key_blocks(h, key_slots))
        pl.when(jnp.logical_not(keys))(lambda: query_blocks(h, query_slots))

    def x_part(h):
        fx_copy(h).wait_recv()
        far_part(h, chip_odd == 1, [1, 2 * core], [3, 2 + 2 * core])

    def y_part(h):
        far_part(h, chip_odd == 0, [1], [3])
        fy_copy(h).wait_recv()
        far_part(h, chip_odd == 0, [2 * core], [2 + 2 * core])

    def finish(h):
        at = h % IN_FLIGHT
        dq_ref[h] = (dq_acc[at] * score_scale).astype(dq_ref.dtype)
        dk_ref[h] = (dk_acc[at] * score_scale).astype(dk_ref.dtype)
        dv_ref[h] = dv_acc[at].astype(dv_ref.dtype)

    for dist, copy in stats:
        pl.when(me + dist < n_dev)(copy.wait_recv)
    chip_part(0)

    def step(t, carry):
        pl.when(t < n_heads)(lambda: arrive(t))

        pl.when((t >= 1) & (t <= n_heads))(lambda: x_part(t - 1))
        pl.when((t >= 1) & (t <= n_heads) & middle)(lambda: arrive_y(t - 1))
        pl.when((t >= 2) & middle)(lambda: y_part(t - 2))
        pl.when(t >= 2)(lambda: finish(t - 2))
        pl.when(t < n_heads - 1)(lambda: chip_part(t + 1))
        return carry

    lax.fori_loop(0, n_heads + 2, step, 0)

    def drain(h, carry):
        own_kv(h).wait_send()
        fx_copy(h).wait_send()
        pl.when(middle)(lambda: fy_copy(h).wait_send())
        for r in range(ROW_PARTS):
            x_copy(h, r).wait_send()
            pl.when(relays)(lambda: y_copy(h, r).wait_send())
        return carry

    lax.fori_loop(0, n_heads, drain, 0)
    for dist, copy in stats:
        pl.when(me >= dist)(copy.wait_send)


def token_major_kernel(dq_ref, dk_ref, dv_ref, dq_out, dk_out, dv_out, rows_buf, out_sem):
    part = dq_ref.shape[1] // OUT_STEPS
    copies = []
    for r in range(OUT_STEPS):
        for which, (src, dst) in enumerate(((dq_ref, dq_out), (dk_ref, dk_out), (dv_ref, dv_out))):
            rows = pl.ds(r * part, part)
            rows_buf[which, rows] = jnp.swapaxes(src[:, rows], 0, 1)
            copies.append(pltpu.make_async_copy(rows_buf.at[which, rows], dst.at[rows], out_sem.at[which, r]))
            copies[-1].start()
    for copy in copies:
        copy.wait()


def solution(mesh):
    n_dev = mesh.shape["cp"]
    head_spec = P("cp", "hp", None)
    row_spec = P("cp", "hp")
    any_spec = pl.BlockSpec(memory_space=pl.ANY)
    vmem_spec = pl.BlockSpec(memory_space=pltpu.VMEM)
    smem_spec = pl.BlockSpec(memory_space=pltpu.SMEM)
    dma = pltpu.SemaphoreType.DMA

    def device_fn(q_loc, k_loc, v_loc, o_loc, do_loc, lse_loc, cu_seqlens):
        n_tok, n_heads, head_dim = q_loc.shape
        seq_len = n_tok * n_dev
        score_scale = head_dim ** -0.5
        pair_shape = (2, n_heads, n_tok, head_dim)

        def wide(q_loc, k_loc, v_loc, o_loc, do_loc, lse_loc, cu_seqlens):
            bf16, f32 = jnp.bfloat16, jnp.float32
            per = n_heads // n_dev
            pos = jnp.arange(seq_len, dtype=jnp.int32).reshape(n_dev, n_tok)
            start_rows = jnp.max(jnp.where(cu_seqlens <= pos[..., None], cu_seqlens, 0), axis=-1)
            delta_loc = jnp.einsum("shd,shd->hs", do_loc, o_loc, preferred_element_type=f32)
            parts = [item.reshape(n_dev, per, n_tok) for item in (lse_loc.T, delta_loc)]
            stat = jnp.concatenate(parts + [jnp.zeros((n_dev, 8 - 2 * per, n_tok), f32)], axis=1)
            rows = n_tok // OUT_STEPS
            row_blk = pl.BlockSpec((rows, n_heads, head_dim), lambda i: (i, 0, 0))
            ops = pl.pallas_call(turn_kernel, grid=(OUT_STEPS,), out_shape=jax.ShapeDtypeStruct((4, n_heads, n_tok, head_dim), bf16), in_specs=[row_blk] * 4,
                                 out_specs=pl.BlockSpec((4, n_heads, rows, head_dim), lambda i: (0, 0, i, 0)), name="turn_in")(q_loc, k_loc, v_loc, do_loc)

            def heads_of(dev):
                return pl.ds(dev * per, per)

            def call(pairs, n_pairs, ident, out_shape, *args):
                return pl.pallas_call(functools.partial(swap_kernel, n_dev, pairs), out_shape=out_shape,
                                      in_specs=[any_spec] * len(args), out_specs=[any_spec] * len(out_shape),
                                      scratch_shapes=[dma((n_pairs, n_dev)), dma((n_pairs, n_dev)), dma((n_pairs,))],
                                      compiler_params=pltpu.CompilerParams(collective_id=ident, has_side_effects=True))(*args)

            def in_pairs(refs):
                ops_ref, stat_ref, got_ref, gstat_ref = refs
                return [(lambda d: ops_ref.at[:, heads_of(d)], lambda d: got_ref.at[d]), (lambda d: stat_ref.at[d], lambda d: gstat_ref.at[d])]

            def out_pairs(refs):
                grad_ref, back_ref = refs
                return [(lambda d: grad_ref.at[d], lambda d: back_ref.at[:, heads_of(d)])]

            got, gstat = call(in_pairs, 2, 1, (jax.ShapeDtypeStruct((n_dev, 4, per, n_tok, head_dim), bf16), jax.ShapeDtypeStruct((n_dev, 8, n_tok), f32)), ops, stat)
            grads = pl.pallas_call(
                functools.partial(head_kernel, score_scale),
                grid_spec=pltpu.PrefetchScalarGridSpec(
                    num_scalar_prefetch=1, grid=(per,),
                    in_specs=[pl.BlockSpec((n_dev, 4, 1, n_tok, head_dim), lambda h, s: (0, 0, h, 0, 0)), pl.BlockSpec((n_dev, 8, n_tok), lambda h, s: (0, 0, 0)), pl.BlockSpec((n_dev, n_tok), lambda h, s: (0, 0))],
                    out_specs=pl.BlockSpec((n_dev, 3, 1, n_tok, head_dim), lambda h, s: (0, 0, h, 0, 0)),
                    scratch_shapes=[pltpu.VMEM((n_dev, n_tok, head_dim), f32)] * 3),
                out_shape=jax.ShapeDtypeStruct((n_dev, 3, per, n_tok, head_dim), bf16), name="head_grads",
            )(start_rows[:, 0], got, gstat, start_rows)
            back, = call(out_pairs, 1, 2, (jax.ShapeDtypeStruct((3, n_heads, n_tok, head_dim), bf16),), grads)
            head_blks = [pl.BlockSpec((1, n_heads, rows, head_dim), lambda i, n=n: (n, 0, i, 0)) for n in range(3)]
            return pl.pallas_call(turn_kernel, grid=(OUT_STEPS,), out_shape=(pltpu.HBM(q_loc.shape, bf16),) * 3, in_specs=head_blks, out_specs=[row_blk] * 3, name="turn_out")(back, back, back)

        def near(q_loc, k_loc, v_loc, o_loc, do_loc, lse_loc, cu_seqlens):
            out_one = pltpu.VMEM((n_heads, n_tok, head_dim), q_loc.dtype)
            bf16, f32 = jnp.bfloat16, jnp.float32
            heads_out = pl.pallas_call(
                functools.partial(near_kernel, n_dev, score_scale),
                out_shape=(out_one, out_one, out_one),
                in_specs=[smem_spec] + [any_spec] * 5 + [vmem_spec], out_specs=(vmem_spec,) * 3,
                scratch_shapes=[pltpu.VMEM((n_heads // TILE_HEADS, 4, n_tok, TILE_HEADS, head_dim), bf16), pltpu.VMEM(q_loc.shape, bf16)]
                + [pltpu.VMEM(pair_shape, bf16)] * 3 + [pltpu.VMEM((5,) + pair_shape, bf16)]
                + [pltpu.VMEM((2 * n_heads, n_tok), f32), pltpu.VMEM((REACH, 2 * n_heads, n_tok), f32), pltpu.VMEM((8, n_tok), jnp.int32)]
                + [pltpu.VMEM((IN_FLIGHT, n_tok, head_dim), f32)] * 3
                + [dma((n_heads // TILE_HEADS, ROW_PARTS, 4)), dma, dma((REACH,)), dma((REACH,)), dma((n_heads,)), dma((n_heads,))]
                + [dma((n_heads, ROW_PARTS))] * 4 + [dma((n_heads,))] * 4,
                compiler_params=pltpu.CompilerParams(collective_id=0, has_side_effects=True, vmem_limit_bytes=50 * 1024 * 1024), name="near_grads",
            )(cu_seqlens, q_loc, k_loc, v_loc, o_loc, do_loc, lse_loc.T)
            return pl.pallas_call(
                token_major_kernel, out_shape=(pltpu.HBM(q_loc.shape, bf16),) * 3, in_specs=[vmem_spec] * 3, out_specs=(any_spec,) * 3,
                scratch_shapes=[pltpu.VMEM((3,) + q_loc.shape, bf16), dma((3, OUT_STEPS))],
                name="token_major", compiler_params=pltpu.CompilerParams(vmem_limit_bytes=20 * 1024 * 1024))(*heads_out)

        def branch_kernel(cu_ref, out_ref):
            first = 2 * n_tok

            def scan(n, seen):
                here = cu_ref[n]
                return tuple(jnp.where((here >= c * first) & (here <= (c + 1) * first), 1, flag) for c, flag in zip((1, 2), seen))

            seen = lax.fori_loop(0, cu_ref.shape[0], scan, (0, 0), unroll=True)
            out_ref[0] = 1 - seen[0] * seen[1]

        pick = pl.pallas_call(branch_kernel, out_shape=jax.ShapeDtypeStruct((1,), jnp.int32), in_specs=[smem_spec], out_specs=smem_spec, name="pick_branch")(cu_seqlens)[0]
        return lax.switch(pick, (near, wide), q_loc, k_loc, v_loc, o_loc, do_loc, lse_loc, cu_seqlens)

    return jax.shard_map(device_fn, mesh=mesh, in_specs=(head_spec, head_spec, head_spec, head_spec, head_spec, row_spec, P()), out_specs=(head_spec, head_spec, head_spec), check_vma=False)
```

```python
import functools

import jax
import jax.numpy as jnp
from jax import lax
from jax.experimental import pallas as pl
from jax.experimental.pallas import tpu as pltpu
from jax.sharding import PartitionSpec as P

REACH = 3
TILE_HEADS = 8
ROW_PARTS = 2
IN_FLIGHT = 4
OUT_STEPS = 2
OUT_PIECES = 4
LOG2E = 1.4426950408889634
MESH_ID = pl.DeviceIdType.MESH


def to_dev(idx):
    return {"cp": idx}


def greet_all(n_dev, me):
    barrier = pltpu.get_barrier_semaphore()
    for step in range(1, n_dev):
        pl.semaphore_signal(barrier, inc=1, device_id=to_dev(lax.rem(me + step, n_dev)), device_id_type=MESH_ID)


def await_all(n_dev):
    pl.semaphore_wait(pltpu.get_barrier_semaphore(), n_dev - 1)


def stat_copies(me, n_dev, stat_ref, swin_ref, send_sem, recv_sem):
    out = []
    for dist in range(1, REACH + 1):
        copy = pltpu.make_async_remote_copy(src_ref=stat_ref, dst_ref=swin_ref.at[dist - 1], send_sem=send_sem.at[dist - 1], recv_sem=recv_sem.at[dist - 1], device_id=to_dev(lax.rem(me + n_dev - dist, n_dev)), device_id_type=MESH_ID)
        out.append((dist, copy))
    return out


def nt_dot(a, b):
    return lax.dot_general(a, b, (((1,), (1,)), ((), ())), preferred_element_type=jnp.float32)


def nn_dot(a, b):
    return lax.dot_general(a, b, (((1,), (0,)), ((), ())), preferred_element_type=jnp.float32)


def tn_dot(a, b):
    return lax.dot_general(a, b, (((0,), (0,)), ((), ())), preferred_element_type=jnp.float32)


def block_terms(score_scale, k_blk, v_blk, q_blk, do_blk, lse_row, delta_row, start_row, k_base, q_base):
    s_t = nt_dot(k_blk, q_blk)
    dp_t = nt_dot(v_blk, do_blk)
    k_pos = k_base + lax.broadcasted_iota(jnp.int32, s_t.shape, 0)
    q_pos = q_base + lax.broadcasted_iota(jnp.int32, s_t.shape, 1)
    keep = (k_pos >= start_row) & (k_pos <= q_pos)
    p_t = jnp.where(keep, jnp.exp2(s_t * (score_scale * LOG2E) - lse_row * LOG2E), 0.0)
    ds_t = (p_t * (dp_t - delta_row)).astype(jnp.bfloat16)
    return p_t.astype(jnp.bfloat16), ds_t


def swap_kernel(n_dev, pairs, *refs):
    me = lax.axis_index("cp")
    views = pairs(refs[:-3])
    s_sem, r_sem, l_sem = refs[-3:]
    greet_all(n_dev, me)
    await_all(n_dev)

    def copies(mask):
        peer = me ^ mask
        return [pltpu.make_async_remote_copy(src_ref=src(peer), dst_ref=dst(me), send_sem=s_sem.at[n, mask], recv_sem=r_sem.at[n, mask], device_id=to_dev(peer), device_id_type=MESH_ID)
                for n, (src, dst) in enumerate(views)]

    order = [2, 4, 6, 3, 5, 7, 1]
    for mask in order:
        for copy in copies(mask):
            copy.start()
    for n, (src, dst) in enumerate(views):
        pltpu.make_async_copy(src(me), dst(me), l_sem.at[n]).start()
    for n, (src, dst) in enumerate(views):
        pltpu.make_async_copy(src(me), dst(me), l_sem.at[n]).wait()
    for mask in order:
        for copy in copies(mask):
            copy.wait()


def turn_kernel(*refs):
    n_out = len(refs) // 2 if len(refs) % 2 == 0 else 1
    srcs, dsts = refs[:len(refs) - n_out], refs[len(refs) - n_out:]
    for n, src in enumerate(srcs):
        if n_out == 1:
            dsts[0][n] = jnp.swapaxes(src[...], 0, 1)
        else:
            dsts[n][...] = jnp.swapaxes(src[0], 0, 1)


def head_kernel(score_scale, start_ref, got_ref, gstat_ref, rows_ref, out_ref, dq_acc, dk_acc, dv_acc):
    head = pl.program_id(0)
    n_dev, _, _, n_tok, _ = got_ref.shape
    terms = functools.partial(block_terms, score_scale)

    def shard(i, carry):
        q_blk, do_blk = got_ref[i, 0, 0], got_ref[i, 3, 0]
        lse_row, delta_row = gstat_ref[i, pl.ds(head, 1), :], gstat_ref[i, pl.ds(2 + head, 1), :]
        start_row = rows_ref[pl.ds(i, 1), :]

        def pair(j, first):
            k_blk, v_blk = got_ref[j, 1, 0], got_ref[j, 2, 0]
            p_t, ds_t = terms(k_blk, v_blk, q_blk, do_blk, lse_row, delta_row, start_row, j * n_tok, i * n_tok)
            dv, dk, dq = nn_dot(p_t, do_blk), nn_dot(ds_t, q_blk), tn_dot(ds_t, k_blk)
            if first:
                dv_acc[j], dk_acc[j], dq_acc[i] = dv, dk, dq
            else:
                dv_acc[j] += dv
                dk_acc[j] += dk
                dq_acc[i] += dq

        pair(i, True)
        lowest = start_ref[i] // n_tok
        lax.fori_loop(lowest, i, lambda j, c: (pair(j, False), c)[1], 0)
        return carry

    lax.fori_loop(0, n_dev, shard, 0)

    def write(i, carry):
        out_ref[i, 0, 0] = (dq_acc[i] * score_scale).astype(out_ref.dtype)
        out_ref[i, 1, 0] = (dk_acc[i] * score_scale).astype(out_ref.dtype)
        out_ref[i, 2, 0] = dv_acc[i].astype(out_ref.dtype)
        return carry

    lax.fori_loop(0, n_dev, write, 0)


def near_kernel(n_dev, score_scale, cu_ref, q_ref, k_ref, v_ref, o_ref, do_ref, lse_ref, dq_ref, dk_ref, dv_ref,
                raw, raw_o, qd, kv, pk, win, stat, swin, starts, dq_acc, dk_acc, dv_acc,
                ld_sem, o_sem, st_s, st_r, own_s, own_r, x_s, x_r, y_s, y_r, fx_s, fx_r, fy_s, fy_r):
    me = lax.axis_index("cp")
    core = lax.rem(me, 2)
    chip = me // 2
    chip_odd = lax.rem(chip, 2)
    n_tok, n_heads, _ = q_ref.shape
    part = n_tok // ROW_PARTS
    base = me * n_tok
    first_chip, last_chip = chip == 0, chip == n_dev // 2 - 1
    not_first, not_last = jnp.logical_not(first_chip), jnp.logical_not(last_chip)
    relays = first_chip | last_chip
    middle = jnp.logical_not(relays)
    x_dev, y_dev, mate = me + 2 - 4 * chip_odd, lax.rem(me + 4, n_dev), me + 1 - 2 * core
    x_dst = 1 + 2 * chip_odd
    x_slot = 3 - 2 * chip_odd
    y_slot = 4 - x_slot

    def remote(src, dst, s_sem, r_sem, dev):
        return pltpu.make_async_remote_copy(src_ref=src, dst_ref=dst, send_sem=s_sem, recv_sem=r_sem, device_id=to_dev(dev), device_id_type=MESH_ID)

    def block(slot, h, r):
        return win.at[slot, :, h, pl.ds(r * part, part)]

    def x_copy(h, r):
        return remote(pk.at[:, h, pl.ds(r * part, part)], block(x_dst, h, r), x_s.at[h, r], x_r.at[h, r], x_dev)

    def y_copy(h, r):
        return remote(block(x_slot, h, r), block(y_slot, h, r), y_s.at[h, r], y_r.at[h, r], y_dev)

    def fx_copy(h):
        return remote(win.at[x_slot, :, h], win.at[4 - 2 * core - 2 * chip_odd, :, h], fx_s.at[h], fx_r.at[h], mate)

    def fy_copy(h):
        return remote(win.at[y_slot, :, h], win.at[2 - 2 * core + 2 * chip_odd, :, h], fy_s.at[h], fy_r.at[h], mate)

    def own_kv(h):
        return remote(kv.at[:, h], win.at[0, :, h], own_s.at[h], own_r.at[h], mate)

    def own_qd(h):
        return remote(qd.at[:, h], win.at[4, :, h], own_s.at[h], own_r.at[h], mate)

    halves = n_heads // TILE_HEADS
    units = [(half, r) for half in range(halves) for r in range(ROW_PARTS)]

    def load(half, r, which):
        src = (q_ref, k_ref, do_ref, v_ref)[which]
        rows, heads = pl.ds(r * part, part), pl.ds(half * TILE_HEADS, TILE_HEADS)
        return pltpu.make_async_copy(src.at[rows, heads], raw.at[half, which, rows], ld_sem.at[half, r, which])

    for half, r in units[:1]:
        for which in range(4):
            load(half, r, which).start()
    greet_all(n_dev, me)
    for half, r in units[1:]:
        for which in range(4):
            load(half, r, which).start()
    load_o = pltpu.make_async_copy(o_ref, raw_o, o_sem)
    load_o.start()

    chip_pos = chip * 2 * n_tok

    def scan_cross(n, cross_end):
        return jnp.where((cu_ref[n] < chip_pos) & (cu_ref[n + 1] > chip_pos), cu_ref[n + 1], cross_end)

    n_docs = cu_ref.shape[0] - 1
    send_rows = lax.fori_loop(0, n_docs, scan_cross, 0, unroll=True) - base

    def find_starts():
        pos = base + n_tok * lax.broadcasted_iota(jnp.int32, starts.shape, 0) + lax.broadcasted_iota(jnp.int32, starts.shape, 1)

        def scan_docs(n, found):
            return jnp.where(cu_ref[n] <= pos, jnp.maximum(found, cu_ref[n]), found)

        found = lax.fori_loop(0, n_docs, scan_docs, jnp.zeros(starts.shape, jnp.int32))
        starts[...] = jnp.where(pos < n_dev * n_tok, found, n_dev * n_tok)

    row_ids = lax.broadcasted_iota(jnp.int32, (TILE_HEADS, part, q_ref.shape[2]), 1)
    stats = stat_copies(me, n_dev, stat, swin, st_s, st_r)

    def arrange(half, r):
        rows, heads = pl.ds(r * part, part), pl.ds(half * TILE_HEADS, TILE_HEADS)
        for pair in range(2):
            load(half, r, 2 * pair).wait()
            load(half, r, 2 * pair + 1).wait()
            q_side = jnp.swapaxes(raw[half, 2 * pair, rows], 0, 1)
            k_side = jnp.swapaxes(raw[half, 2 * pair + 1, rows], 0, 1)
            pk[pair, heads, rows] = jnp.where(row_ids < send_rows - r * part, q_side, k_side)
            qd[pair, heads, rows] = q_side
            kv[pair, heads, rows] = k_side

    def start_own(half):
        for h in range(half * TILE_HEADS, (half + 1) * TILE_HEADS):
            pl.when(core == 0)(own_kv(h).start)
            pl.when(core == 1)(own_qd(h).start)

    for r in range(ROW_PARTS):
        arrange(0, r)
        if r == 0:
            await_all(n_dev)
        x_copy(0, r).start()
    start_own(0)
    for half in range(1, halves):
        for r in range(ROW_PARTS):
            arrange(half, r)
        start_own(half)
    find_starts()
    load_o.wait()
    stat[0:n_heads, :] = lse_ref[...]
    for half in range(halves):
        delta = jnp.sum(raw[half, 2].astype(jnp.float32) * raw_o[:, half * TILE_HEADS:(half + 1) * TILE_HEADS, :].astype(jnp.float32), axis=-1)
        stat[n_heads + half * TILE_HEADS:n_heads + (half + 1) * TILE_HEADS, :] = delta.T
    for dist, copy in stats:
        pl.when(me >= dist)(copy.start)

    terms = functools.partial(block_terms, score_scale)

    def arrive(h):
        for r in range(ROW_PARTS):
            x_copy(h, r).wait_recv()
            pl.when(relays)(lambda: y_copy(h, r).start())
            pl.when(h + 1 < n_heads)(lambda: x_copy(h + 1, r).start())
        fx_copy(h).start()

    def arrive_y(h):
        for r in range(ROW_PARTS):
            y_copy(h, r).wait_recv()
        fy_copy(h).start()

    def mine(h):
        return qd[0, h], qd[1, h], kv[0, h], kv[1, h]

    def key_block(h, slot):
        q_blk, do_blk, _, _ = mine(h)
        k_far, v_far = win[slot, 0, h], win[slot, 1, h]
        _, ds_far = terms(k_far, v_far, q_blk, do_blk, stat[pl.ds(h, 1), :], stat[pl.ds(n_heads + h, 1), :], starts[0:1, :], base - (slot + 1) * n_tok, base)
        return tn_dot(ds_far, k_far)

    def query_block(h, slot):
        _, _, k_blk, v_blk = mine(h)
        dist = 5 - slot
        q_far, do_far = win[slot, 0, h], win[slot, 1, h]
        p_far, ds_far = terms(k_blk, v_blk, q_far, do_far, swin[dist - 1, pl.ds(h, 1), :], swin[dist - 1, pl.ds(n_heads + h, 1), :], starts[pl.ds(dist, 1), :], base, base + dist * n_tok)
        return nn_dot(ds_far, q_far), nn_dot(p_far, do_far)

    def key_blocks(h, slots):
        dq_acc[h % IN_FLIGHT] += sum(key_block(h, slot) for slot in slots)

    def query_blocks(h, slots):
        found = [query_block(h, slot) for slot in slots]
        dk_acc[h % IN_FLIGHT] += sum(item[0] for item in found)
        dv_acc[h % IN_FLIGHT] += sum(item[1] for item in found)

    def chip_part(h):
        q_blk, do_blk, k_blk, v_blk = mine(h)
        p_t, ds_t = terms(k_blk, v_blk, q_blk, do_blk, stat[pl.ds(h, 1), :], stat[pl.ds(n_heads + h, 1), :], starts[0:1, :], base, base)
        dv_acc[h % IN_FLIGHT] = nn_dot(p_t, do_blk)
        dk_acc[h % IN_FLIGHT] = nn_dot(ds_t, q_blk)
        dq_acc[h % IN_FLIGHT] = tn_dot(ds_t, k_blk)
        own_qd(h).wait_recv()
        pl.when(core == 1)(lambda: key_blocks(h, [0]))
        pl.when(core == 0)(lambda: query_blocks(h, [4]))

    def far_part(h, keys, key_slots, query_slots):
        pl.when(keys)(lambda: key_blocks(h, key_slots))
        pl.when(jnp.logical_not(keys))(lambda: query_blocks(h, query_slots))

    def x_part(h):
        fx_copy(h).wait_recv()
        far_part(h, chip_odd == 1, [1, 2 * core], [3, 2 + 2 * core])

    def y_part(h):
        far_part(h, chip_odd == 0, [1], [3])
        fy_copy(h).wait_recv()
        far_part(h, chip_odd == 0, [2 * core], [2 + 2 * core])

    def finish(h):
        at = h % IN_FLIGHT
        dq_ref[h] = (dq_acc[at] * score_scale).astype(dq_ref.dtype)
        dk_ref[h] = (dk_acc[at] * score_scale).astype(dk_ref.dtype)
        dv_ref[h] = dv_acc[at].astype(dv_ref.dtype)

    for dist, copy in stats:
        pl.when(me + dist < n_dev)(copy.wait_recv)
    chip_part(0)

    def step(t, carry):
        pl.when(t < n_heads)(lambda: arrive(t))

        pl.when((t >= 1) & (t <= n_heads))(lambda: x_part(t - 1))
        pl.when((t >= 1) & (t <= n_heads) & middle)(lambda: arrive_y(t - 1))
        pl.when((t >= 2) & middle)(lambda: y_part(t - 2))
        pl.when(t >= 2)(lambda: finish(t - 2))
        pl.when(t < n_heads - 1)(lambda: chip_part(t + 1))
        return carry

    lax.fori_loop(0, n_heads + 2, step, 0)

    def drain(h, carry):
        own_kv(h).wait_send()
        fx_copy(h).wait_send()
        pl.when(middle)(lambda: fy_copy(h).wait_send())
        for r in range(ROW_PARTS):
            x_copy(h, r).wait_send()
            pl.when(relays)(lambda: y_copy(h, r).wait_send())
        return carry

    lax.fori_loop(0, n_heads, drain, 0)
    for dist, copy in stats:
        pl.when(me >= dist)(copy.wait_send)


def token_major_kernel(dq_ref, dk_ref, dv_ref, dq_out, dk_out, dv_out, rows_buf, out_sem):
    part = dq_ref.shape[1] // OUT_PIECES
    copies = []
    for r in range(OUT_PIECES):
        for which, (src, dst) in enumerate(((dq_ref, dq_out), (dk_ref, dk_out), (dv_ref, dv_out))):
            rows = pl.ds(r * part, part)
            rows_buf[which, rows] = jnp.swapaxes(src[:, rows], 0, 1)
            copies.append(pltpu.make_async_copy(rows_buf.at[which, rows], dst.at[rows], out_sem.at[which, r]))
            copies[-1].start()
    for copy in copies:
        copy.wait()


def solution(mesh):
    n_dev = mesh.shape["cp"]
    head_spec = P("cp", "hp", None)
    row_spec = P("cp", "hp")
    any_spec = pl.BlockSpec(memory_space=pl.ANY)
    vmem_spec = pl.BlockSpec(memory_space=pltpu.VMEM)
    smem_spec = pl.BlockSpec(memory_space=pltpu.SMEM)
    dma = pltpu.SemaphoreType.DMA

    def device_fn(q_loc, k_loc, v_loc, o_loc, do_loc, lse_loc, cu_seqlens):
        n_tok, n_heads, head_dim = q_loc.shape
        seq_len = n_tok * n_dev
        score_scale = head_dim ** -0.5
        pair_shape = (2, n_heads, n_tok, head_dim)

        def wide(q_loc, k_loc, v_loc, o_loc, do_loc, lse_loc, cu_seqlens):
            bf16, f32 = jnp.bfloat16, jnp.float32
            per = n_heads // n_dev
            pos = jnp.arange(seq_len, dtype=jnp.int32).reshape(n_dev, n_tok)
            start_rows = jnp.max(jnp.where(cu_seqlens <= pos[..., None], cu_seqlens, 0), axis=-1)
            delta_loc = jnp.einsum("shd,shd->hs", do_loc, o_loc, preferred_element_type=f32)
            parts = [item.reshape(n_dev, per, n_tok) for item in (lse_loc.T, delta_loc)]
            stat = jnp.concatenate(parts + [jnp.zeros((n_dev, 8 - 2 * per, n_tok), f32)], axis=1)
            rows = n_tok // OUT_STEPS
            row_blk = pl.BlockSpec((rows, n_heads, head_dim), lambda i: (i, 0, 0))
            ops = pl.pallas_call(turn_kernel, grid=(OUT_STEPS,), out_shape=jax.ShapeDtypeStruct((4, n_heads, n_tok, head_dim), bf16), in_specs=[row_blk] * 4,
                                 out_specs=pl.BlockSpec((4, n_heads, rows, head_dim), lambda i: (0, 0, i, 0)), name="turn_in")(q_loc, k_loc, v_loc, do_loc)

            def heads_of(dev):
                return pl.ds(dev * per, per)

            def call(pairs, n_pairs, ident, out_shape, *args):
                return pl.pallas_call(functools.partial(swap_kernel, n_dev, pairs), out_shape=out_shape,
                                      in_specs=[any_spec] * len(args), out_specs=[any_spec] * len(out_shape),
                                      scratch_shapes=[dma((n_pairs, n_dev)), dma((n_pairs, n_dev)), dma((n_pairs,))],
                                      compiler_params=pltpu.CompilerParams(collective_id=ident, has_side_effects=True))(*args)

            def in_pairs(refs):
                ops_ref, stat_ref, got_ref, gstat_ref = refs
                return [(lambda d: ops_ref.at[:, heads_of(d)], lambda d: got_ref.at[d]), (lambda d: stat_ref.at[d], lambda d: gstat_ref.at[d])]

            def out_pairs(refs):
                grad_ref, back_ref = refs
                return [(lambda d: grad_ref.at[d], lambda d: back_ref.at[:, heads_of(d)])]

            got, gstat = call(in_pairs, 2, 1, (jax.ShapeDtypeStruct((n_dev, 4, per, n_tok, head_dim), bf16), jax.ShapeDtypeStruct((n_dev, 8, n_tok), f32)), ops, stat)
            grads = pl.pallas_call(
                functools.partial(head_kernel, score_scale),
                grid_spec=pltpu.PrefetchScalarGridSpec(
                    num_scalar_prefetch=1, grid=(per,),
                    in_specs=[pl.BlockSpec((n_dev, 4, 1, n_tok, head_dim), lambda h, s: (0, 0, h, 0, 0)), pl.BlockSpec((n_dev, 8, n_tok), lambda h, s: (0, 0, 0)), pl.BlockSpec((n_dev, n_tok), lambda h, s: (0, 0))],
                    out_specs=pl.BlockSpec((n_dev, 3, 1, n_tok, head_dim), lambda h, s: (0, 0, h, 0, 0)),
                    scratch_shapes=[pltpu.VMEM((n_dev, n_tok, head_dim), f32)] * 3),
                out_shape=jax.ShapeDtypeStruct((n_dev, 3, per, n_tok, head_dim), bf16), name="head_grads",
            )(start_rows[:, 0], got, gstat, start_rows)
            back, = call(out_pairs, 1, 2, (jax.ShapeDtypeStruct((3, n_heads, n_tok, head_dim), bf16),), grads)
            head_blks = [pl.BlockSpec((1, n_heads, rows, head_dim), lambda i, n=n: (n, 0, i, 0)) for n in range(3)]
            return pl.pallas_call(turn_kernel, grid=(OUT_STEPS,), out_shape=(pltpu.HBM(q_loc.shape, bf16),) * 3, in_specs=head_blks, out_specs=[row_blk] * 3, name="turn_out")(back, back, back)

        def near(q_loc, k_loc, v_loc, o_loc, do_loc, lse_loc, cu_seqlens):
            out_one = pltpu.VMEM((n_heads, n_tok, head_dim), q_loc.dtype)
            bf16, f32 = jnp.bfloat16, jnp.float32
            heads_out = pl.pallas_call(
                functools.partial(near_kernel, n_dev, score_scale),
                out_shape=(out_one, out_one, out_one),
                in_specs=[smem_spec] + [any_spec] * 5 + [vmem_spec], out_specs=(vmem_spec,) * 3,
                scratch_shapes=[pltpu.VMEM((n_heads // TILE_HEADS, 4, n_tok, TILE_HEADS, head_dim), bf16), pltpu.VMEM(q_loc.shape, bf16)]
                + [pltpu.VMEM(pair_shape, bf16)] * 3 + [pltpu.VMEM((5,) + pair_shape, bf16)]
                + [pltpu.VMEM((2 * n_heads, n_tok), f32), pltpu.VMEM((REACH, 2 * n_heads, n_tok), f32), pltpu.VMEM((8, n_tok), jnp.int32)]
                + [pltpu.VMEM((IN_FLIGHT, n_tok, head_dim), f32)] * 3
                + [dma((n_heads // TILE_HEADS, ROW_PARTS, 4)), dma, dma((REACH,)), dma((REACH,)), dma((n_heads,)), dma((n_heads,))]
                + [dma((n_heads, ROW_PARTS))] * 4 + [dma((n_heads,))] * 4,
                compiler_params=pltpu.CompilerParams(collective_id=0, has_side_effects=True, vmem_limit_bytes=50 * 1024 * 1024), name="near_grads",
            )(cu_seqlens, q_loc, k_loc, v_loc, o_loc, do_loc, lse_loc.T)
            return pl.pallas_call(
                token_major_kernel, out_shape=(pltpu.HBM(q_loc.shape, bf16),) * 3, in_specs=[vmem_spec] * 3, out_specs=(any_spec,) * 3,
                scratch_shapes=[pltpu.VMEM((3,) + q_loc.shape, bf16), dma((3, OUT_PIECES))],
                name="token_major", compiler_params=pltpu.CompilerParams(vmem_limit_bytes=20 * 1024 * 1024))(*heads_out)

        def branch_kernel(cu_ref, out_ref):
            first = 2 * n_tok

            def scan(n, seen):
                here = cu_ref[n]
                return tuple(jnp.where((here >= c * first) & (here <= (c + 1) * first), 1, flag) for c, flag in zip((1, 2), seen))

            seen = lax.fori_loop(0, cu_ref.shape[0], scan, (0, 0), unroll=True)
            out_ref[0] = 1 - seen[0] * seen[1]

        pick = pl.pallas_call(branch_kernel, out_shape=jax.ShapeDtypeStruct((1,), jnp.int32), in_specs=[smem_spec], out_specs=smem_spec, name="pick_branch")(cu_seqlens)[0]
        return lax.switch(pick, (near, wide), q_loc, k_loc, v_loc, o_loc, do_loc, lse_loc, cu_seqlens)

    return jax.shard_map(device_fn, mesh=mesh, in_specs=(head_spec, head_spec, head_spec, head_spec, head_spec, row_spec, P()), out_specs=(head_spec, head_spec, head_spec), check_vma=False)
```
